8 devices in a mesh: fsdp: 8 (over z, y, x, core).
Axes of the slice: x: 2, y: 2, z: 1, core: 2. Of those that a mesh axis runs over, the one named last changes fastest.
Arguments:
- grad_mat: bfloat16 [8, 29818880], P('fsdp')
- grad_vec: bfloat16 [8, 6144], P('fsdp')
- master_mat: float32 [29818880], P('fsdp')
- moment_mat: float32 [29818880], P('fsdp')
- second_mat: float32 [29818880], P('fsdp')
- master_vec: float32 [6144], P('fsdp')
- moment_vec: float32 [6144], P('fsdp')
- second_vec: float32 [6144], P('fsdp')
Outputs:
- output 1: float32 [29818880], P('fsdp')
- output 2: float32 [29818880], P('fsdp')
- output 3: float32 [29818880], P('fsdp')
- output 4: float32 [6144], P('fsdp')
- output 5: float32 [6144], P('fsdp')
- output 6: float32 [6144], P('fsdp')
- output 7: bfloat16 [29818880], replicated
- output 8: bfloat16 [6144], replicated
All inputs are finite; a program needn't handle non-finite values.
Results may differ from the reference program's by a relative error of at most 0.001.
Values are sent between devices in bfloat16 or wider.
A program may use at most 1 GiB of HBM per device.

```python
import jax
import jax.numpy as jnp
from jax import lax

D = 896
HEADS = 14
KV_HEADS = 2
HEAD = 64
FF = 4864
LAYERS = 2
GROUP = 8
NM_PAD = 29818880
NV_PAD = 6144
STEP = 4

Q_OUT = HEADS * HEAD
KV_OUT = KV_HEADS * HEAD
MAT_COUNT = LAYERS * (2 * D * Q_OUT + 2 * D * KV_OUT + 3 * D * FF)
VEC_COUNT = LAYERS * (Q_OUT + 2 * KV_OUT + 2 * D)
GRAD_UNIT = (MAT_COUNT + VEC_COUNT) ** -0.5
TARGET_NORM = 3.0
LEARN_RATE = 1e-3
BETA_ONE = 0.9
BETA_TWO = 0.999
ADAM_EPS = 1e-8
DECAY = 0.01
NORM_EPS = 1e-6
FIX_ONE = 1.0 - BETA_ONE ** STEP
FIX_TWO = 1.0 - BETA_TWO ** STEP


def pad_flat(flat, total):
    return jnp.pad(flat, (0, total - flat.shape[0]))


def layer_draw(key, pieces):
    sub_keys = jax.random.split(key, len(pieces))
    drawn = [jax.random.normal(sub_key, (LAYERS, length), jnp.float32) * scale + offset
             for sub_key, (length, scale, offset) in zip(sub_keys, pieces)]
    return jnp.concatenate(drawn, axis=1).reshape(-1)


def grad_rows(key, total, valid):
    keep = jnp.arange(total) < valid
    scale = TARGET_NORM * GRAD_UNIT * GROUP ** -0.5

    def one_row(row):
        noise = jax.random.normal(jax.random.fold_in(key, row), (total,), jnp.float32)
        return jnp.where(keep, noise * scale, 0.0).astype(jnp.bfloat16)

    return lax.map(one_row, jnp.arange(GROUP))


def moment_draw(key, total, valid):
    keep = jnp.arange(total) < valid
    noise = jax.random.normal(key, (total,), jnp.float32)
    return jnp.where(keep, 0.1 * GRAD_UNIT * noise, 0.0)


def second_draw(key, total, valid):
    keep = jnp.arange(total) < valid
    noise = jax.random.normal(key, (total,), jnp.float32)
    return jnp.where(keep, 0.003 * GRAD_UNIT ** 2 * (noise * noise + 0.5), 0.0)


def setup_inputs(seed: int = 0) -> dict:
    keys = jax.random.split(jax.random.key(seed), 8)
    mat_pieces = [(D * Q_OUT, D ** -0.5, 0.0), (D * KV_OUT, D ** -0.5, 0.0), (D * KV_OUT, D ** -0.5, 0.0),
                  (Q_OUT * D, Q_OUT ** -0.5, 0.0), (D * FF, D ** -0.5, 0.0), (D * FF, D ** -0.5, 0.0),
                  (FF * D, FF ** -0.5, 0.0)]
    vec_pieces = [(Q_OUT, 0.5, 0.0), (KV_OUT, 0.5, 0.0), (KV_OUT, 0.5, 0.0), (D, 0.2, 1.0), (D, 0.2, 1.0)]
    return {
        'grad_mat': grad_rows(keys[0], NM_PAD, MAT_COUNT),
        'grad_vec': grad_rows(keys[1], NV_PAD, VEC_COUNT),
        'master_mat': pad_flat(layer_draw(keys[2], mat_pieces), NM_PAD),
        'moment_mat': moment_draw(keys[3], NM_PAD, MAT_COUNT),
        'second_mat': second_draw(keys[4], NM_PAD, MAT_COUNT),
        'master_vec': pad_flat(layer_draw(keys[5], vec_pieces), NV_PAD),
        'moment_vec': moment_draw(keys[6], NV_PAD, VEC_COUNT),
        'second_vec': second_draw(keys[7], NV_PAD, VEC_COUNT),
    }


def row_total(grad_block):
    def add_row(running, row_vals):
        return running + row_vals.astype(jnp.float32), None

    total, _ = lax.scan(add_row, jnp.zeros(grad_block.shape[1:], jnp.float32), grad_block)
    return total


def adam_update(grad_sum, clip_coef, master, moment, second, decay):
    clip_grad = clip_coef * grad_sum
    new_moment = BETA_ONE * moment + (1.0 - BETA_ONE) * clip_grad
    new_second = BETA_TWO * second + (1.0 - BETA_TWO) * clip_grad * clip_grad
    step_dir = (new_moment / FIX_ONE) / (jnp.sqrt(new_second / FIX_TWO) + ADAM_EPS)
    new_master = master - LEARN_RATE * (step_dir + decay * master)
    return new_master, new_moment, new_second


def reference(grad_mat, grad_vec, master_mat, moment_mat, second_mat, master_vec, moment_vec, second_vec):
    sum_mat = row_total(grad_mat)
    sum_vec = row_total(grad_vec)
    total_norm = jnp.sqrt(jnp.sum(sum_mat * sum_mat) + jnp.sum(sum_vec * sum_vec))
    clip_coef = jnp.minimum(1.0, 1.0 / (total_norm + NORM_EPS))
    mat_out = adam_update(sum_mat, clip_coef, master_mat, moment_mat, second_mat, DECAY)
    vec_out = adam_update(sum_vec, clip_coef, master_vec, moment_vec, second_vec, 0.0)
    return (mat_out[0], mat_out[1], mat_out[2], vec_out[0], vec_out[1], vec_out[2],
            mat_out[0].astype(jnp.bfloat16), vec_out[0].astype(jnp.bfloat16))
```

```python
import functools

import jax
import jax.numpy as jnp
from jax import lax
from jax.experimental import pallas as pl
from jax.experimental.pallas import tpu as pltpu
from jax.sharding import PartitionSpec as P

STEP = 4
LEARN_RATE = 1e-3
BETA_ONE = 0.9
BETA_TWO = 0.999
ADAM_EPS = 1e-8
DECAY = 0.01
NORM_EPS = 1e-6
FIX_ONE = 1.0 - BETA_ONE ** STEP
FIX_TWO = 1.0 - BETA_TWO ** STEP

MESH = pl.DeviceIdType.MESH
LANES = 128
TILE = 1024


def adam_update(grad_sum, clip_coef, master, moment, second, decay):
    clip_grad = clip_coef * grad_sum
    new_moment = BETA_ONE * moment + (1.0 - BETA_ONE) * clip_grad
    new_second = BETA_TWO * second + (1.0 - BETA_TWO) * clip_grad * clip_grad
    step_dir = (new_moment / FIX_ONE) / (jnp.sqrt(new_second / FIX_TWO) + ADAM_EPS)
    new_master = master - LEARN_RATE * (step_dir + decay * master)
    return new_master, new_moment, new_second


def block_len(n, most):
    tiles = n // TILE
    return max(d for d in range(1, most // TILE + 1) if tiles % d == 0) * TILE


PIECES = {'diag': (0, 2), 'x_b': (2, 1), 'y_a': (3, 1), 'x_a': (4, 1), 'y_b': (5, 1), 'mine': (6, 2)}


def reduce_kernel(share, half, steps, g, gv, pv, mv, sv,
                  total, sib_land, leaf_land, four_land, direct_land, square_out, vec_out, vec_state,
                  raw_own, raw_sib, leaf_st, direct_st, four_st, leaf_in, fin_in, out_st, acc, sq_land, vec_land,
                  sib_send, sib_recv, leaf_send, leaf_recv, four_send, four_recv, direct_send, direct_recv,
                  own_sem, sibin_sem, leafin_sem, fin_sem, out_sem, sq_send, sq_recv, vec_send, vec_recv, local_sem):
    me = lax.axis_index('fsdp')
    core = lax.rem(me, 2)
    x_pos = lax.rem(me // 2, 2)
    y_pos = me // 4
    sib = me + 1 - 2 * core
    x_dev = me + 2 - 4 * x_pos
    y_dev = me + 4 - 8 * y_pos
    g_dev = y_dev + 2 - 4 * x_pos
    sib_delta = 1 - 2 * core
    dests = (g_dev, x_dev, y_dev, me)
    rows = half // LANES
    n_dev = 8

    barrier = pltpu.get_barrier_semaphore()
    for k in range(1, n_dev):
        pl.semaphore_signal(barrier, inc=1, device_id=(lax.rem(me + k, n_dev),), device_id_type=MESH)
    pl.semaphore_wait(barrier, n_dev - 1)

    def sib_copy(j, t):
        src = pl.multiple_of((dests[j] + sib_delta) * share + t * 2 * half, TILE)
        dst = pl.multiple_of(j * share + t * 2 * half, TILE)
        return pltpu.make_async_remote_copy(
            src_ref=g.at[:, pl.ds(src, 2 * half)], dst_ref=sib_land.at[:, pl.ds(dst, 2 * half)],
            send_sem=sib_send, recv_sem=sib_recv.at[j, t], device_id=(sib,), device_id_type=MESH)

    def raw_copies(piece, t, slot):
        place, width = PIECES[piece]
        j = {'diag': 0, 'x_b': 1, 'x_a': 1, 'y_a': 2, 'y_b': 2, 'mine': 3}[piece]
        skip = half if piece in ('x_b', 'y_b') else 0
        n = width * half
        here = pl.ds(place * half, n)
        index = list(PIECES).index(piece)
        src = pl.multiple_of(dests[j] * share + t * 2 * half + skip, TILE)
        land = pl.multiple_of(j * share + t * 2 * half + skip, TILE)
        return (pltpu.make_async_copy(g.at[:, pl.ds(src, n)], raw_own.at[slot, :, here], own_sem.at[slot, index]),
                pltpu.make_async_copy(sib_land.at[:, pl.ds(land, n)], raw_sib.at[slot, :, here],
                                      sibin_sem.at[slot, index]))

    def land_rows(t, part):
        return pl.ds(pl.multiple_of(t * 2 * rows + part * rows, 8), rows)

    def remote(stage, slot, part, land, t, send, recv, target):
        return pltpu.make_async_remote_copy(
            src_ref=stage.at[slot, pl.ds(part * rows, rows), :], dst_ref=land.at[land_rows(t, part), :],
            send_sem=send.at[slot, part], recv_sem=recv.at[part, t], device_id=(target,), device_id_type=MESH)

    def leaf_copy(t, slot, part):
        return remote(leaf_st, slot, part, leaf_land, t, leaf_send, leaf_recv, (y_dev, x_dev)[part])

    def direct_copy(t, slot, part):
        return remote(direct_st, slot, part, direct_land, t, direct_send, direct_recv, (y_dev, x_dev)[part])

    def four_copy(t, slot, part):
        return remote(four_st, slot, part, four_land, t, four_send, four_recv, (x_dev, y_dev)[part])

    def leaf_load(t, part):
        return pltpu.make_async_copy(leaf_land.at[land_rows(t, part), :], leaf_in.at[pl.ds(part * rows, rows), :],
                                     leafin_sem.at[part])

    def fin_load(land, which, t):
        both = pl.ds(pl.multiple_of(t * 2 * rows, 8), 2 * rows)
        return pltpu.make_async_copy(land.at[both, :], fin_in.at[which], fin_sem.at[which])

    def out_copy(t, slot):
        both = pl.ds(pl.multiple_of(t * 2 * rows, 8), 2 * rows)
        return pltpu.make_async_copy(out_st.at[slot], total.at[both, :], out_sem.at[slot])

    blk = block_len(half, 16 * TILE)
    blk_rows = blk // LANES

    def pair(slot, place, i):
        at = pl.ds(pl.multiple_of(place * half + i * blk, TILE), blk)
        own = raw_own[slot, :, at].astype(jnp.float32).reshape(blk_rows, LANES)
        other = raw_sib[slot, :, at].astype(jnp.float32).reshape(blk_rows, LANES)
        return own + other

    def block_rows(i, part=0):
        return pl.ds(pl.multiple_of(part * rows + i * blk_rows, 8), blk_rows)

    def store_pair(slot, place, stage, part):
        @pl.loop(0, half // blk)
        def _(i):
            stage[slot, block_rows(i, part), :] = pair(slot, place, i)

    def wait_raw(piece, t, slot):
        for copy in raw_copies(piece, t, slot):
            copy.wait()

    vec_srcs = (gv, pv, mv, sv)

    def vec_copies(k):
        target = lax.rem(me + k, n_dev)
        out = []
        for i, src in enumerate(vec_srcs):
            dst = vec_land.at[me] if i == 0 else vec_state.at[i - 1, me]
            out.append(pltpu.make_async_remote_copy(
                src_ref=src, dst_ref=dst, send_sem=vec_send.at[k - 1, i], recv_sem=vec_recv.at[k - 1, i],
                device_id=(target,), device_id_type=MESH))
        return out

    def send_sib(t):
        for j in range(4):
            sib_copy(j, t).start()

    def fetch(t):
        slot = lax.rem(t, 2)

        @pl.when(t < steps)
        def _():
            for j in range(3):
                sib_copy(j, t).wait_recv()
            for piece in ('diag', 'x_b', 'y_a'):
                for copy in raw_copies(piece, t, slot):
                    copy.start()

        @pl.when(jnp.logical_and(t >= 1, t <= steps))
        def _():
            for piece in ('x_a', 'y_b'):
                for copy in raw_copies(piece, t - 1, slot):
                    copy.start()

        @pl.when(jnp.logical_and(t >= 2, t <= steps + 1))
        def _():
            sib_copy(3, t - 2).wait_recv()
            for copy in raw_copies('mine', t - 2, slot):
                copy.start()

    send_sib(0)
    send_sib(1)
    acc[...] = jnp.zeros_like(acc)
    fetch(0)

    @pl.loop(0, steps + 2)
    def _(t):
        slot = lax.rem(t, 2)
        before = 1 - slot

        @pl.when(t + 2 < steps)
        def _():
            send_sib(t + 2)

        fetch(t + 1)

        @pl.when(t < steps)
        def _():
            wait_raw('diag', t, slot)
            for part in range(2):
                @pl.when(t >= 2)
                def _():
                    leaf_copy(t - 2, slot, part).wait_send()
                store_pair(slot, part, leaf_st, part)
                leaf_copy(t, slot, part).start()
            for part, piece, place in ((1, 'x_b', 2), (0, 'y_a', 3)):
                wait_raw(piece, t, slot)

                @pl.when(t >= 2)
                def _():
                    direct_copy(t - 2, slot, part).wait_send()
                store_pair(slot, place, direct_st, part)
                direct_copy(t, slot, part).start()

        @pl.when(t == 0)
        def _():
            for k in range(1, n_dev):
                for copy in vec_copies(k):
                    copy.start()

        @pl.when(jnp.logical_and(t >= 1, t <= steps))
        def _():
            for part in range(2):
                leaf_copy(t - 1, before, part).wait_recv()
                leaf_load(t - 1, part).start()
            for part, piece, place in ((0, 'x_a', 4), (1, 'y_b', 5)):
                wait_raw(piece, t - 1, slot)

                @pl.when(t >= 3)
                def _():
                    four_copy(t - 3, before, part).wait_send()
                leaf_load(t - 1, part).wait()

                @pl.loop(0, half // blk)
                def _(i):
                    at = block_rows(i, part)
                    four_st[before, at, :] = leaf_in[at, :] + pair(slot, place, i)
                four_copy(t - 1, before, part).start()

        @pl.when(t >= 2)
        def _():
            for part in range(2):
                four_copy(t - 2, slot, part).wait_recv()
                direct_copy(t - 2, slot, part).wait_recv()
            fin_load(four_land, 0, t - 2).start()
            fin_load(direct_land, 1, t - 2).start()
            wait_raw('mine', t - 2, slot)

            @pl.when(t >= 4)
            def _():
                out_copy(t - 4, slot).wait()
            fin_load(four_land, 0, t - 2).wait()
            fin_load(direct_land, 1, t - 2).wait()

            @pl.loop(0, 2 * half // blk)
            def _(i):
                at = block_rows(i)
                whole = (fin_in[0, at, :] + fin_in[1, at, :]) + pair(slot, 6, i)
                out_st[slot, at, :] = whole
                acc[...] += jnp.sum((whole * whole).reshape(blk_rows // 8, 8, LANES), axis=0)
            out_copy(t - 2, slot).start()

    def square_copy(k):
        target = lax.rem(me + k, n_dev)
        return pltpu.make_async_remote_copy(
            src_ref=acc, dst_ref=sq_land.at[me], send_sem=sq_send.at[k - 1], recv_sem=sq_recv.at[k - 1],
            device_id=(target,), device_id_type=MESH)

    for k in range(1, n_dev):
        square_copy(k).start()
    sq_land[me] = acc[...]

    own = [pltpu.make_async_copy(src, vec_land.at[me] if i == 0 else vec_state.at[i - 1, me], local_sem.at[i])
           for i, src in enumerate(vec_srcs)]
    for copy in own:
        copy.start()
    for copy in own:
        copy.wait()
    for k in range(1, n_dev):
        for copy in vec_copies(k):
            copy.wait()
    vec_rows = vec_out.shape[0]
    vec_total = vec_land[0].astype(jnp.float32)
    for d in range(1, n_dev):
        vec_total += vec_land[d].astype(jnp.float32)
    vec_total = vec_total.reshape(vec_rows, LANES)
    vec_out[...] = vec_total
    vec_square = jnp.sum((vec_total * vec_total).reshape(vec_rows // 8, 8, LANES), axis=0)
    for t in (steps - 2, steps - 1):
        slot = t % 2
        out_copy(t, slot).wait()
        for part in range(2):
            leaf_copy(t, slot, part).wait_send()
            direct_copy(t, slot, part).wait_send()
            four_copy(t, slot, part).wait_send()
    pltpu.make_async_remote_copy(
        src_ref=g.at[:, pl.ds(0, 4 * share)], dst_ref=sib_land, send_sem=sib_send, recv_sem=sib_recv.at[0, 0],
        device_id=(sib,), device_id_type=MESH).wait_send()
    for k in range(1, n_dev):
        square_copy(k).wait()
    square = sq_land[0]
    for d in range(1, n_dev):
        square += sq_land[d]
    square_out[...] = square + vec_square


def reduce_call(g, gv, pv, mv, sv, share, steps):
    half = share // (2 * steps)
    rows = half // LANES
    share_rows = share // LANES
    dma = pltpu.SemaphoreType.DMA
    f32, bf16 = jnp.float32, jnp.bfloat16
    vec_rows = gv.shape[1] // LANES
    own_rows = pv.shape[0]
    any_spec = pl.BlockSpec(memory_space=pltpu.HBM)
    vmem = pl.BlockSpec(memory_space=pltpu.VMEM)
    return pl.pallas_call(
        functools.partial(reduce_kernel, share, half, steps),
        out_shape=(jax.ShapeDtypeStruct((share_rows, LANES), f32),
                   jax.ShapeDtypeStruct((1, 4 * share), bf16),
                   jax.ShapeDtypeStruct((share_rows, LANES), f32),
                   jax.ShapeDtypeStruct((share_rows, LANES), f32),
                   jax.ShapeDtypeStruct((share_rows, LANES), f32),
                   jax.ShapeDtypeStruct((8, LANES), f32),
                   jax.ShapeDtypeStruct((vec_rows, LANES), f32),
                   jax.ShapeDtypeStruct((3, 8, own_rows, LANES), f32)),
        in_specs=[any_spec] + [vmem] * 4,
        out_specs=(any_spec,) * 5 + (vmem,) * 3,
        scratch_shapes=[
            pltpu.VMEM((2, 1, 8 * half), bf16),
            pltpu.VMEM((2, 1, 8 * half), bf16),
            pltpu.VMEM((2, 2 * rows, LANES), f32),
            pltpu.VMEM((2, 2 * rows, LANES), f32),
            pltpu.VMEM((2, 2 * rows, LANES), f32),
            pltpu.VMEM((2 * rows, LANES), f32),
            pltpu.VMEM((2, 2 * rows, LANES), f32),
            pltpu.VMEM((2, 2 * rows, LANES), f32),
            pltpu.VMEM((8, LANES), f32),
            pltpu.VMEM((8, 8, LANES), f32),
            pltpu.VMEM((8, 1, gv.shape[1]), bf16),
            dma(()), dma((4, steps)),
            dma((2, 2)), dma((2, steps)), dma((2, 2)), dma((2, steps)), dma((2, 2)), dma((2, steps)),
            dma((2, 6)), dma((2, 6)), dma((2,)), dma((2,)), dma((2,)),
            dma((7,)), dma((7,)), dma((7, 4)), dma((7, 4)), dma((4,)),
        ],
        compiler_params=pltpu.CompilerParams(collective_id=0, has_side_effects=True, vmem_limit_bytes=60 * 2**20),
        name='reduce_share',
    )(g, gv, pv, mv, sv)


STEPS = 14


def solution(mesh):
    def local_step(grad_mat, grad_vec, master_mat, moment_mat, second_mat, master_vec, moment_vec, second_vec):
        share = master_mat.shape[0]
        own_rows = master_vec.shape[0] // LANES
        vecs = [v.reshape(own_rows, LANES) for v in (master_vec, moment_vec, second_vec)]
        total, _, _, _, _, square, vec_sum, vec_state = reduce_call(grad_mat, grad_vec, *vecs, share, STEPS)
        total_norm = jnp.sqrt(jnp.sum(square))
        clip_coef = jnp.minimum(1.0, 1.0 / (total_norm + NORM_EPS))
        new_mat = adam_update(total.reshape(-1), clip_coef, master_mat, moment_mat, second_mat, DECAY)
        weights_mat = lax.all_gather(new_mat[0].astype(jnp.bfloat16), 'fsdp', tiled=True)
        vec_state = vec_state.reshape(3, -1)
        vec_new = adam_update(vec_sum.reshape(-1), clip_coef, vec_state[0], vec_state[1], vec_state[2], 0.0)
        at = lax.axis_index('fsdp') * master_vec.shape[0]
        new_vec = tuple(lax.dynamic_slice(v, (at,), master_vec.shape) for v in vec_new)
        return new_mat + new_vec + (weights_mat, vec_new[0].astype(jnp.bfloat16))

    row_spec = P('fsdp', None)
    flat_spec = P('fsdp')
    whole_spec = P()
    return jax.shard_map(local_step, mesh=mesh,
                         in_specs=(row_spec, row_spec) + (flat_spec,) * 6,
                         out_specs=(flat_spec,) * 6 + (whole_spec, whole_spec),
                         check_vma=False)
```

```python
import functools

import jax
import jax.numpy as jnp
from jax import lax
from jax.experimental import pallas as pl
from jax.experimental.pallas import tpu as pltpu
from jax.sharding import PartitionSpec as P

STEP = 4
LEARN_RATE = 1e-3
BETA_ONE = 0.9
BETA_TWO = 0.999
ADAM_EPS = 1e-8
DECAY = 0.01
NORM_EPS = 1e-6
FIX_ONE = 1.0 - BETA_ONE ** STEP
FIX_TWO = 1.0 - BETA_TWO ** STEP

MESH = pl.DeviceIdType.MESH
LANES = 128
TILE = 1024


def adam_update(grad_sum, clip_coef, master, moment, second, decay):
    clip_grad = clip_coef * grad_sum
    new_moment = BETA_ONE * moment + (1.0 - BETA_ONE) * clip_grad
    new_second = BETA_TWO * second + (1.0 - BETA_TWO) * clip_grad * clip_grad
    step_dir = (new_moment * (LEARN_RATE / FIX_ONE)) / (jnp.sqrt(new_second * (1.0 / FIX_TWO)) + ADAM_EPS)
    new_master = master - (step_dir + (LEARN_RATE * decay) * master)
    return new_master, new_moment, new_second


def block_len(n, most):
    tiles = n // TILE
    return max(d for d in range(1, most // TILE + 1) if tiles % d == 0) * TILE


PIECES = {'diag': (0, 2), 'x_b': (2, 1), 'y_a': (3, 1), 'x_a': (4, 1), 'y_b': (5, 1), 'mine': (6, 2)}


def step_kernel(share, half, steps, w_steps, w_late, g, gv, p_mat, m_mat, s_mat, pv, mv, sv,
                total, gathered, late_a, late_b, sib_land, leaf_land, four_land, direct_land, coef_out, vec_new, vec_w,
                raw_own, raw_sib, leaf_st, direct_st, four_st, leaf_in, fin_in, out_st, acc, sq_land, vec_land,
                  sib_send, sib_recv, leaf_send, leaf_recv, four_send, four_recv, direct_send, direct_recv,
                  own_sem, sibin_sem, leafin_sem, fin_sem, out_sem, sq_send, sq_recv, vec_send, vec_recv, local_sem,
                state_in, own_w, state_sem, own_send, own_recv, own_sib_recv, keep_sem, late_sem,
                fwd_send, fwd_recv, fsib_send, fsib_recv):
    me = lax.axis_index('fsdp')
    core = lax.rem(me, 2)
    x_pos = lax.rem(me // 2, 2)
    y_pos = me // 4
    sib = me + 1 - 2 * core
    x_dev = me + 2 - 4 * x_pos
    y_dev = me + 4 - 8 * y_pos
    g_dev = y_dev + 2 - 4 * x_pos
    sib_delta = 1 - 2 * core
    dests = (g_dev, x_dev, y_dev, me)
    rows = half // LANES
    n_dev = 8

    def sib_copy(j, t):
        src = pl.multiple_of((dests[j] + sib_delta) * share + t * 2 * half, TILE)
        dst = pl.multiple_of(j * share + t * 2 * half, TILE)
        return pltpu.make_async_remote_copy(
            src_ref=g.at[:, pl.ds(src, 2 * half)], dst_ref=sib_land.at[:, pl.ds(dst, 2 * half)],
            send_sem=sib_send, recv_sem=sib_recv.at[j, t], device_id=(sib,), device_id_type=MESH)

    def raw_copy(piece, t, slot, which):
        place, width = PIECES[piece]
        j = {'diag': 0, 'x_b': 1, 'x_a': 1, 'y_a': 2, 'y_b': 2, 'mine': 3}[piece]
        skip = half if piece in ('x_b', 'y_b') else 0
        n = width * half
        here = pl.ds(place * half, n)
        index = list(PIECES).index(piece)
        src = pl.multiple_of(dests[j] * share + t * 2 * half + skip, TILE)
        land = pl.multiple_of(j * share + t * 2 * half + skip, TILE)
        if which == 0:
            return pltpu.make_async_copy(g.at[:, pl.ds(src, n)], raw_own.at[slot, :, here], own_sem.at[slot, index])
        return pltpu.make_async_copy(sib_land.at[:, pl.ds(land, n)], raw_sib.at[slot, :, here],
                                     sibin_sem.at[slot, index])

    def land_rows(t, part):
        return pl.ds(pl.multiple_of(t * 2 * rows + part * rows, 8), rows)

    def remote(stage, slot, part, land, t, send, recv, target):
        return pltpu.make_async_remote_copy(
            src_ref=stage.at[slot, pl.ds(part * rows, rows), :], dst_ref=land.at[land_rows(t, part), :],
            send_sem=send.at[slot, part], recv_sem=recv.at[part, t], device_id=(target,), device_id_type=MESH)

    def leaf_copy(t, slot, part):
        return remote(leaf_st, slot, part, leaf_land, t, leaf_send, leaf_recv, (y_dev, x_dev)[part])

    def direct_copy(t, slot, part):
        return remote(direct_st, slot, part, direct_land, t, direct_send, direct_recv, (y_dev, x_dev)[part])

    def four_copy(t, slot, part):
        return remote(four_st, slot, part, four_land, t, four_send, four_recv, (x_dev, y_dev)[part])

    def leaf_load(t, part):
        return pltpu.make_async_copy(leaf_land.at[land_rows(t, part), :], leaf_in.at[pl.ds(part * rows, rows), :],
                                     leafin_sem.at[part])

    def fin_load(land, which, t):
        both = pl.ds(pl.multiple_of(t * 2 * rows, 8), 2 * rows)
        return pltpu.make_async_copy(land.at[both, :], fin_in.at[which], fin_sem.at[which])

    def out_copy(t, slot):
        both = pl.ds(pl.multiple_of(t * 2 * rows, 8), 2 * rows)
        return pltpu.make_async_copy(out_st.at[slot], total.at[both, :], out_sem.at[slot])

    blk = block_len(half, 16 * TILE)
    blk_rows = blk // LANES

    def pair(slot, place, i):
        at = pl.ds(pl.multiple_of(place * half + i * blk, TILE), blk)
        own = raw_own[slot, :, at].astype(jnp.float32).reshape(blk_rows, LANES)
        other = raw_sib[slot, :, at].astype(jnp.float32).reshape(blk_rows, LANES)
        return own + other

    def block_rows(i, part=0):
        return pl.ds(pl.multiple_of(part * rows + i * blk_rows, 8), blk_rows)

    def store_pair(slot, place, stage, part):
        @pl.loop(0, half // blk)
        def _(i):
            stage[slot, block_rows(i, part), :] = pair(slot, place, i)

    def wait_raw(piece, t, slot):
        for which in range(2):
            raw_copy(piece, t, slot, which).wait()

    def row_copy(k):
        return pltpu.make_async_remote_copy(
            src_ref=gv, dst_ref=vec_land.at[me], send_sem=vec_send.at[k - 1, 0], recv_sem=vec_recv.at[k - 1, 0],
            device_id=(lax.rem(me + k, n_dev),), device_id_type=MESH)

    def new_copy(k):
        return pltpu.make_async_remote_copy(
            src_ref=vec_new.at[0], dst_ref=vec_w.at[me], send_sem=vec_send.at[k - 1, 1], recv_sem=vec_recv.at[k - 1, 1],
            device_id=(lax.rem(me + k, n_dev),), device_id_type=MESH)

    def send_sib(t):
        for j in range(4):
            sib_copy(j, t).start()

    def fetch(t, which):
        slot = lax.rem(t, 2)

        @pl.when(t < steps)
        def _():
            for j, piece in enumerate(('diag', 'x_b', 'y_a')):
                if which == 1:
                    sib_copy(j, t).wait_recv()
                raw_copy(piece, t, slot, which).start()

        @pl.when(jnp.logical_and(t >= 1, t <= steps))
        def _():
            for piece in ('x_a', 'y_b'):
                raw_copy(piece, t - 1, slot, which).start()

        @pl.when(jnp.logical_and(t >= 2, t <= steps + 1))
        def _():
            if which == 1:
                sib_copy(3, t - 2).wait_recv()
            raw_copy('mine', t - 2, slot, which).start()

    barrier = pltpu.get_barrier_semaphore()
    for k in range(1, n_dev):
        pl.semaphore_signal(barrier, inc=1, device_id=(lax.rem(me + k, n_dev),), device_id_type=MESH)
    fetch(jnp.int32(0), 0)
    pl.semaphore_wait(barrier, n_dev - 1)
    send_sib(0)
    send_sib(1)
    acc[...] = jnp.zeros_like(acc)
    fetch(jnp.int32(0), 1)

    @pl.loop(0, steps + 2)
    def _(t):
        slot = lax.rem(t, 2)
        before = 1 - slot

        @pl.when(t + 2 < steps)
        def _():
            send_sib(t + 2)

        fetch(t + 1, 0)
        fetch(t + 1, 1)

        @pl.when(t < steps)
        def _():
            wait_raw('diag', t, slot)
            for part in range(2):
                @pl.when(t >= 2)
                def _():
                    leaf_copy(t - 2, slot, part).wait_send()
                store_pair(slot, part, leaf_st, part)
                leaf_copy(t, slot, part).start()
            for part, piece, place in ((1, 'x_b', 2), (0, 'y_a', 3)):
                wait_raw(piece, t, slot)

                @pl.when(t >= 2)
                def _():
                    direct_copy(t - 2, slot, part).wait_send()
                store_pair(slot, place, direct_st, part)
                direct_copy(t, slot, part).start()

        @pl.when(t == 0)
        def _():
            for k in range(1, n_dev):
                row_copy(k).start()

        @pl.when(jnp.logical_and(t >= 1, t <= steps))
        def _():
            for part in range(2):
                leaf_copy(t - 1, before, part).wait_recv()
                leaf_load(t - 1, part).start()
            for part, piece, place in ((0, 'x_a', 4), (1, 'y_b', 5)):
                wait_raw(piece, t - 1, slot)

                @pl.when(t >= 3)
                def _():
                    four_copy(t - 3, before, part).wait_send()
                leaf_load(t - 1, part).wait()

                @pl.loop(0, half // blk)
                def _(i):
                    at = block_rows(i, part)
                    four_st[before, at, :] = leaf_in[at, :] + pair(slot, place, i)
                four_copy(t - 1, before, part).start()

        @pl.when(t >= 2)
        def _():
            for part in range(2):
                four_copy(t - 2, slot, part).wait_recv()
                direct_copy(t - 2, slot, part).wait_recv()
            fin_load(four_land, 0, t - 2).start()
            fin_load(direct_land, 1, t - 2).start()
            wait_raw('mine', t - 2, slot)

            @pl.when(t >= 4)
            def _():
                out_copy(t - 4, slot).wait()
            fin_load(four_land, 0, t - 2).wait()
            fin_load(direct_land, 1, t - 2).wait()

            @pl.loop(0, 2 * half // blk)
            def _(i):
                at = block_rows(i)
                whole = (fin_in[0, at, :] + fin_in[1, at, :]) + pair(slot, 6, i)
                out_st[slot, at, :] = whole
                acc[...] += jnp.sum((whole * whole).reshape(blk_rows // 8, 8, LANES), axis=0)
            out_copy(t - 2, slot).start()

    for t in (steps - 2, steps - 1):
        out_copy(t, t % 2).wait()

    def square_copy(k):
        target = lax.rem(me + k, n_dev)
        return pltpu.make_async_remote_copy(
            src_ref=acc, dst_ref=sq_land.at[me], send_sem=sq_send.at[k - 1], recv_sem=sq_recv.at[k - 1],
            device_id=(target,), device_id_type=MESH)

    for k in range(1, n_dev):
        square_copy(k).start()
    sq_land[me] = acc[...]
    own_row = pltpu.make_async_copy(gv, vec_land.at[me], local_sem)
    own_row.start()

    share_rows = share // LANES
    half_rows = share_rows // 2
    w_rows = half_rows // w_steps

    def inside(part, t, n=1):
        return pl.ds(pl.multiple_of(part * half_rows + t * w_rows, 16), n * w_rows)

    def place(dev, part, t):
        return pl.ds(pl.multiple_of(dev * share_rows + part * half_rows + t * w_rows, 16), w_rows)

    def state_copies(t, slot):
        return [pltpu.make_async_copy(src.at[inside(part, t), :], state_in.at[slot, i, part], state_sem.at[slot, i, part])
                for i, src in enumerate((total, p_mat, m_mat, s_mat)) for part in range(2)]

    def own_copy(to, part, t):
        target = (x_dev, y_dev, sib)[to]
        recv = own_sib_recv if to == 2 else own_recv.at[to, part, t]
        return pltpu.make_async_remote_copy(
            src_ref=own_w.at[inside(part, t), :], dst_ref=gathered.at[place(me, part, t), :],
            send_sem=own_send.at[to], recv_sem=recv, device_id=(target,), device_id_type=MESH)

    def keep_copy(part, t):
        return pltpu.make_async_copy(own_w.at[inside(part, t), :], gathered.at[place(me, part, t), :], keep_sem)

    def late_copy(part):
        return pltpu.make_async_copy(own_w.at[inside(part, w_steps - w_late, w_late), :], (late_a, late_b)[part],
                                     late_sem.at[part])

    def forward(part, t):
        rows_at = place((x_dev, y_dev)[part], part, t)
        return pltpu.make_async_remote_copy(
            src_ref=gathered.at[rows_at, :], dst_ref=gathered.at[rows_at, :],
            send_sem=fwd_send.at[part], recv_sem=fwd_recv.at[part, t],
            device_id=((y_dev, x_dev)[part],), device_id_type=MESH)

    def to_sib(dev, part, t):
        rows_at = place(dev, part, t)
        return pltpu.make_async_remote_copy(
            src_ref=gathered.at[rows_at, :], dst_ref=gathered.at[rows_at, :],
            send_sem=fsib_send, recv_sem=fsib_recv, device_id=(sib,), device_id_type=MESH)

    def all_rows(n, send, recv):
        return pltpu.make_async_remote_copy(
            src_ref=gathered.at[pl.ds(0, n * w_rows), :], dst_ref=gathered.at[pl.ds(0, n * w_rows), :],
            send_sem=send, recv_sem=recv, device_id=(sib,), device_id_type=MESH)

    for copy in state_copies(0, 0):
        copy.start()

    own_row.wait()
    for k in range(1, n_dev):
        row_copy(k).wait()
    vec_total = vec_land[0].astype(jnp.float32)
    for d in range(1, n_dev):
        vec_total += vec_land[d].astype(jnp.float32)
    vec_rows = gv.shape[1] // LANES
    vec_total = vec_total.reshape(vec_rows, LANES)
    square = jnp.sum((vec_total * vec_total).reshape(vec_rows // 8, 8, LANES), axis=0)
    own_rows = pv.shape[0]
    mine = pl.ds(pl.multiple_of(me * own_rows * LANES, LANES), own_rows * LANES)
    vec_sum = vec_land[0, :, mine].astype(jnp.float32)
    for d in range(1, n_dev):
        vec_sum += vec_land[d, :, mine].astype(jnp.float32)
    vec_sum = vec_sum.reshape(own_rows, LANES)
    for k in range(1, n_dev):
        square_copy(k).wait()
    for d in range(n_dev):
        square += sq_land[d]
    norm = jnp.sqrt(jnp.sum(jnp.sum(square, axis=0, keepdims=True), axis=1, keepdims=True))
    coef = jnp.minimum(1.0, 1.0 / (norm + NORM_EPS))
    coef_out[...] = jnp.broadcast_to(coef, coef_out.shape)

    w_tiles = w_rows // 16
    w_blk = 16 * max(d for d in range(1, 9) if w_tiles % d == 0)

    def update(slot, part, t):
        @pl.loop(0, w_rows // w_blk)
        def _(i):
            at = pl.ds(pl.multiple_of(i * w_blk, 16), w_blk)
            grad, master, moment, second = (state_in[slot, k, part, at, :] for k in range(4))
            new = adam_update(grad, coef_out[0:1, :], master, moment, second, DECAY)[0]
            out = pl.ds(pl.multiple_of(part * half_rows + t * w_rows + i * w_blk, 16), w_blk)
            own_w[out, :] = new.astype(jnp.bfloat16)

    early = w_steps - w_late

    @pl.loop(0, w_steps + LAG + 2)
    def _(u):
        slot = lax.rem(u, 2)

        @pl.when(u + 1 < w_steps)
        def _():
            for copy in state_copies(u + 1, 1 - slot):
                copy.start()

        @pl.when(u < w_steps)
        def _():
            for copy in state_copies(u, slot):
                copy.wait()
            for part in range(2):
                update(slot, part, u)
                own_copy(part, part, u).start()

                @pl.when(u < early)
                def _():
                    own_copy(1 - part, part, u).start()
                own_copy(2, part, u).start()
                keep_copy(part, u).start()

        @pl.when(jnp.logical_and(u >= LAG, u < w_steps + LAG))
        def _():
            t = u - LAG
            for part in range(2):
                own_copy(part, part, t).wait_recv()
                forward(part, t).start()
                to_sib((x_dev, y_dev)[part], part, t).start()

            @pl.when(t < early)
            def _():
                for part in range(2):
                    own_copy(1 - part, part, t).wait_recv()
                    to_sib((y_dev, x_dev)[part], part, t).start()

        @pl.when(u >= LAG + 2)
        def _():
            t = u - LAG - 2
            for part in range(2):
                forward(part, t).wait_recv()
                to_sib(g_dev, part, t).start()

        @pl.when(u == 1)
        def _():
            new = adam_update(vec_sum, coef_out[0:1, :], pv[...], mv[...], sv[...], 0.0)
            for i in range(3):
                vec_new[i] = new[i]
            vec_w[me] = new[0]
            for k in range(1, n_dev):
                new_copy(k).start()

        @pl.when(u == w_steps - 1)
        def _():
            for part in range(2):
                late_copy(part).start()

    for k in range(1, n_dev):
        new_copy(k).wait()

    for t in (steps - 2, steps - 1):
        slot = t % 2
        for part in range(2):
            leaf_copy(t, slot, part).wait_send()
            direct_copy(t, slot, part).wait_send()
            four_copy(t, slot, part).wait_send()
    pltpu.make_async_remote_copy(
        src_ref=g.at[:, pl.ds(0, 4 * share)], dst_ref=sib_land, send_sem=sib_send, recv_sem=sib_recv.at[0, 0],
        device_id=(sib,), device_id_type=MESH).wait_send()
    for part in range(2):
        late_copy(part).wait()
        all_rows(w_steps + early, own_send.at[part], fsib_recv).wait_send()
        all_rows(w_steps, fwd_send.at[part], fsib_recv).wait_send()
    all_rows(2 * w_steps, own_send.at[2], own_sib_recv).wait()
    all_rows(4 * w_steps + 2 * early, fsib_send, fsib_recv).wait()
    pltpu.make_async_copy(own_w, gathered.at[pl.ds(0, share_rows), :], keep_sem).wait()


def step_call(g, gv, p_mat, m_mat, s_mat, pv, mv, sv, share, steps, w_steps, w_late):
    half = share // (2 * steps)
    rows = half // LANES
    share_rows = share // LANES
    w_rows = share_rows // (2 * w_steps)
    dma = pltpu.SemaphoreType.DMA
    f32, bf16 = jnp.float32, jnp.bfloat16
    own_rows = pv.shape[0]
    hbm = pl.BlockSpec(memory_space=pltpu.HBM)
    vmem = pl.BlockSpec(memory_space=pltpu.VMEM)
    return pl.pallas_call(
        functools.partial(step_kernel, share, half, steps, w_steps, w_late),
        out_shape=(jax.ShapeDtypeStruct((share_rows, LANES), f32),
                   jax.ShapeDtypeStruct((8 * share_rows, LANES), bf16),
                   jax.ShapeDtypeStruct((w_late * w_rows, LANES), bf16),
                   jax.ShapeDtypeStruct((w_late * w_rows, LANES), bf16),
                   jax.ShapeDtypeStruct((1, 4 * share), bf16),
                   jax.ShapeDtypeStruct((share_rows, LANES), f32),
                   jax.ShapeDtypeStruct((share_rows, LANES), f32),
                   jax.ShapeDtypeStruct((share_rows, LANES), f32),
                   jax.ShapeDtypeStruct((8, LANES), f32),
                   jax.ShapeDtypeStruct((3, own_rows, LANES), f32),
                   jax.ShapeDtypeStruct((8, own_rows, LANES), f32)),
        in_specs=[hbm, vmem, hbm, hbm, hbm, vmem, vmem, vmem],
        out_specs=(hbm,) * 8 + (vmem,) * 3,
        scratch_shapes=[
            pltpu.VMEM((2, 1, 8 * half), bf16),
            pltpu.VMEM((2, 1, 8 * half), bf16),
            pltpu.VMEM((2, 2 * rows, LANES), f32),
            pltpu.VMEM((2, 2 * rows, LANES), f32),
            pltpu.VMEM((2, 2 * rows, LANES), f32),
            pltpu.VMEM((2 * rows, LANES), f32),
            pltpu.VMEM((2, 2 * rows, LANES), f32),
            pltpu.VMEM((2, 2 * rows, LANES), f32),
            pltpu.VMEM((8, LANES), f32),
            pltpu.VMEM((8, 8, LANES), f32),
            pltpu.VMEM((8, 1, gv.shape[1]), bf16),
            dma(()), dma((4, steps)),
            dma((2, 2)), dma((2, steps)), dma((2, 2)), dma((2, steps)), dma((2, 2)), dma((2, steps)),
            dma((2, 6)), dma((2, 6)), dma((2,)), dma((2,)), dma((2,)),
            dma((7,)), dma((7,)), dma((7, 2)), dma((7, 2)), dma(()),
            pltpu.VMEM((2, 4, 2, w_rows, LANES), f32),
            pltpu.VMEM((share_rows, LANES), bf16),
            dma((2, 4, 2)), dma((3,)), dma((2, 2, w_steps)), dma(()), dma(()), dma((2,)),
            dma((2,)), dma((2, w_steps)), dma(()), dma(()),
        ],
        compiler_params=pltpu.CompilerParams(collective_id=0, has_side_effects=True, vmem_limit_bytes=60 * 2**20),
        name='reduce_update_gather',
    )(g, gv, p_mat, m_mat, s_mat, pv, mv, sv)


def update_kernel(coef, grad, master, moment, second, vec_new, vec_w, new_p, new_m, new_s, vec_p, vec_m, vec_s, w_vec,
                  rows):
    new_p[...], new_m[...], new_s[...] = adam_update(grad[...], coef[0:1, :], master[...], moment[...], second[...], DECAY)

    @pl.when(pl.program_id(0) == 0)
    def _():
        vec_p[...], vec_m[...], vec_s[...] = vec_new[0], vec_new[1], vec_new[2]
        n = vec_w.shape[1]
        for d in range(vec_w.shape[0]):
            rows[pl.ds(d * n, n), :] = vec_w[d]
        w_vec[...] = rows[...].astype(jnp.bfloat16)


def update_call(coef, grad, master, moment, second, vec_new, vec_w, block):
    n = grad.shape[0]
    own_rows = vec_new.shape[1]
    f32 = jnp.float32
    tile = pl.BlockSpec((block, LANES), lambda i: (i, 0))

    def whole(shape):
        return pl.BlockSpec(shape, lambda i: (0,) * len(shape))

    small = jax.ShapeDtypeStruct((own_rows, LANES), f32)
    return pl.pallas_call(
        update_kernel,
        grid=(n // block,),
        out_shape=(jax.ShapeDtypeStruct(grad.shape, f32),) * 3 + (small,) * 3 + (
            jax.ShapeDtypeStruct((8 * own_rows, LANES), jnp.bfloat16),),
        in_specs=[whole((8, LANES))] + [tile] * 4 + [whole(vec_new.shape), whole(vec_w.shape)],
        out_specs=(tile,) * 3 + (whole((own_rows, LANES)),) * 3 + (whole((8 * own_rows, LANES)),),
        scratch_shapes=[pltpu.VMEM((8 * own_rows, LANES), f32)],
        compiler_params=pltpu.CompilerParams(vmem_limit_bytes=40 * 2**20),
        cost_estimate=pl.CostEstimate(flops=n * LANES * 200, bytes_accessed=n * LANES * 28, transcendentals=0),
        name='update',
    )(coef, grad, master, moment, second, vec_new, vec_w)


def copy_kernel(moves, blocks, *refs):
    n_src = 1 + max(move[0] for move in moves(0))
    srcs, out, buf, in_sem, out_sem = refs[:n_src], refs[-4], refs[-3], refs[-2], refs[-1]
    me = lax.axis_index('fsdp')
    todo = []
    for which, src_row, dst_row, n in moves(me):
        size = n // blocks(n)
        for i in range(blocks(n)):
            todo.append((srcs[which], src_row + i * size, dst_row + i * size, size))
    slots = buf.shape[0]

    def take(k):
        src, src_row, _, size = todo[k]
        return pltpu.make_async_copy(src.at[pl.ds(pl.multiple_of(src_row, 16), size), :],
                                     buf.at[k % slots, pl.ds(0, size), :], in_sem.at[k % slots])

    def give(k):
        _, _, dst_row, size = todo[k]
        return pltpu.make_async_copy(buf.at[k % slots, pl.ds(0, size), :],
                                     out.at[pl.ds(pl.multiple_of(dst_row, 16), size), :], out_sem.at[k % slots])

    ahead = slots // 2
    for k in range(min(ahead, len(todo))):
        take(k).start()
    for k in range(len(todo)):
        take(k).wait()
        give(k).start()
        if k + ahead < len(todo):
            if k + ahead >= slots:
                give(k + ahead - slots).wait()
            take(k + ahead).start()
    for k in range(max(0, len(todo) - slots), len(todo)):
        give(k).wait()


def copy_call(name, moves, srcs, out_rows, into=None, slots=12, most=4160):
    def blocks(n):
        return next(d for d in range(1, n // 16 + 1) if (n // 16) % d == 0 and n // d <= most)

    hbm = pl.BlockSpec(memory_space=pltpu.HBM)
    args = list(srcs) + ([into] if into is not None else [])
    size = sum(move[3] for move in moves(0)) * LANES * 2
    return pl.pallas_call(
        functools.partial(copy_kernel, moves, blocks),
        out_shape=jax.ShapeDtypeStruct((out_rows, LANES), jnp.bfloat16),
        in_specs=[hbm] * len(args),
        out_specs=hbm,
        scratch_shapes=[pltpu.VMEM((slots, most, LANES), jnp.bfloat16),
                        pltpu.SemaphoreType.DMA((slots,)), pltpu.SemaphoreType.DMA((slots,))],
        input_output_aliases={len(srcs): 0} if into is not None else {},
        compiler_params=pltpu.CompilerParams(vmem_limit_bytes=32 * 2**20),
        cost_estimate=pl.CostEstimate(flops=size * 6, bytes_accessed=2 * size, transcendentals=0),
        name=name,
    )(*args)


def block_rows_of(n):
    return 16 * max(d for d in range(1, 190) if (n // 16) % d == 0)


STEPS = 28
W_STEPS = 14
W_LATE = 10
LAG = 3


def neighbours(me):
    core, x_pos, y_pos = lax.rem(me, 2), lax.rem(me // 2, 2), me // 4
    return me + 1 - 2 * core, me + 2 - 4 * x_pos, me + 4 - 8 * y_pos


def solution(mesh):
    hop_x = [(d, d ^ 2) for d in range(8)]
    hop_y = [(d, d ^ 4) for d in range(8)]
    hop_core = [(d, d ^ 1) for d in range(8)]

    def local_step(grad_mat, grad_vec, master_mat, moment_mat, second_mat, master_vec, moment_vec, second_vec):
        share = master_mat.shape[0]
        share_rows = share // LANES
        half_rows = share_rows // 2
        late = W_LATE * (half_rows // W_STEPS)
        early = half_rows - late
        own_rows = master_vec.shape[0] // LANES
        mats = [v.reshape(share_rows, LANES) for v in (master_mat, moment_mat, second_mat)]
        vecs = [v.reshape(own_rows, LANES) for v in (master_vec, moment_vec, second_vec)]
        total, gathered, late_a, late_b, _, _, _, _, coef, vec_new, vec_w = step_call(
            grad_mat, grad_vec, *mats, *vecs, share, STEPS, W_STEPS, W_LATE)

        from_x = lax.ppermute(late_b, 'fsdp', hop_x)
        from_y = lax.ppermute(late_a, 'fsdp', hop_y)

        def whole_moves(me):
            sib, x_dev, y_dev = neighbours(me)
            g_dev = x_dev + y_dev - me
            flip = sib - me
            return [(0, dev * share_rows, dev * share_rows, share_rows) for dev in (me, sib, g_dev, g_dev + flip)]

        def early_moves(me):
            sib, x_dev, y_dev = neighbours(me)
            flip = sib - me
            moves = []
            for dev in (x_dev, x_dev + flip):
                moves.append((0, dev * share_rows, dev * share_rows, half_rows + early))
            for dev in (y_dev, y_dev + flip):
                moves.append((0, dev * share_rows, dev * share_rows, early))
                moves.append((0, dev * share_rows + half_rows, dev * share_rows + half_rows, half_rows))
            return moves + [(1, 0, x_dev * share_rows + half_rows + early, late),
                            (2, 0, y_dev * share_rows + early, late)]

        def late_moves(me):
            sib, x_dev, y_dev = neighbours(me)
            flip = sib - me
            return [(0, 0, (x_dev + flip) * share_rows + half_rows + early, late),
                    (1, 0, (y_dev + flip) * share_rows + early, late)]

        *new, weights_vec = update_call(coef, total, *mats, vec_new, vec_w, block_rows_of(share_rows))
        weights = copy_call('collect_whole', whole_moves, (gathered,), 8 * share_rows)
        from_x, from_y, weights, *new = lax.optimization_barrier((from_x, from_y, weights, *new))
        sib_x = lax.ppermute(from_x, 'fsdp', hop_core)
        sib_y = lax.ppermute(from_y, 'fsdp', hop_core)
        weights = copy_call('collect_early', early_moves, (gathered, from_x, from_y), 8 * share_rows, into=weights)
        weights = copy_call('collect_late', late_moves, (sib_x, sib_y), 8 * share_rows, into=weights)
        return tuple(v.reshape(-1) for v in (*new, weights, weights_vec))

    row_spec = P('fsdp', None)
    flat_spec = P('fsdp')
    whole_spec = P()
    return jax.shard_map(local_step, mesh=mesh,
                         in_specs=(row_spec, row_spec) + (flat_spec,) * 6,
                         out_specs=(flat_spec,) * 6 + (whole_spec, whole_spec),
                         check_vma=False)
```

```python
import functools

import jax
import jax.numpy as jnp
from jax import lax
from jax.experimental import pallas as pl
from jax.experimental.pallas import tpu as pltpu
from jax.sharding import PartitionSpec as P

STEP = 4
LEARN_RATE = 1e-3
BETA_ONE = 0.9
BETA_TWO = 0.999
ADAM_EPS = 1e-8
DECAY = 0.01
NORM_EPS = 1e-6
FIX_ONE = 1.0 - BETA_ONE ** STEP
FIX_TWO = 1.0 - BETA_TWO ** STEP

MESH = pl.DeviceIdType.MESH
LANES = 128
TILE = 1024


def adam_update(grad_sum, clip_coef, master, moment, second, decay):
    clip_grad = clip_coef * grad_sum
    new_moment = BETA_ONE * moment + (1.0 - BETA_ONE) * clip_grad
    new_second = BETA_TWO * second + (1.0 - BETA_TWO) * clip_grad * clip_grad
    step_dir = (new_moment * (LEARN_RATE / FIX_ONE)) / (jnp.sqrt(new_second * (1.0 / FIX_TWO)) + ADAM_EPS)
    new_master = master - (step_dir + (LEARN_RATE * decay) * master)
    return new_master, new_moment, new_second


def block_len(n, most):
    tiles = n // TILE
    return max(d for d in range(1, most // TILE + 1) if tiles % d == 0) * TILE


PIECES = {'diag': (0, 2), 'x_b': (2, 1), 'y_a': (3, 1), 'x_a': (4, 1), 'y_b': (5, 1), 'mine': (6, 2)}


def step_kernel(share, half, steps, w_steps, w_late, g, gv, p_mat, m_mat, s_mat, pv, mv, sv,
                total, gathered, late_a, late_b, last_a, last_b, sib_land, leaf_land, four_land, direct_land, coef_out, vec_new, vec_w,
                raw_own, raw_sib, leaf_st, direct_st, four_st, leaf_in, fin_in, out_st, acc, sq_land, vec_land,
                  sib_send, sib_recv, leaf_send, leaf_recv, four_send, four_recv, direct_send, direct_recv,
                  own_sem, sibin_sem, leafin_sem, fin_sem, out_sem, sq_send, sq_recv, vec_send, vec_recv, local_sem,
                state_in, own_w, state_sem, own_send, own_recv, own_sib_recv, keep_sem, late_sem,
                fwd_send, fwd_recv, fsib_send, fsib_recv):
    me = lax.axis_index('fsdp')
    core = lax.rem(me, 2)
    x_pos = lax.rem(me // 2, 2)
    y_pos = me // 4
    sib = me + 1 - 2 * core
    x_dev = me + 2 - 4 * x_pos
    y_dev = me + 4 - 8 * y_pos
    g_dev = y_dev + 2 - 4 * x_pos
    sib_delta = 1 - 2 * core
    dests = (g_dev, x_dev, y_dev, me)
    rows = half // LANES
    n_dev = 8

    def sib_copy(j, t):
        src = pl.multiple_of((dests[j] + sib_delta) * share + t * 2 * half, TILE)
        dst = pl.multiple_of(j * share + t * 2 * half, TILE)
        return pltpu.make_async_remote_copy(
            src_ref=g.at[:, pl.ds(src, 2 * half)], dst_ref=sib_land.at[:, pl.ds(dst, 2 * half)],
            send_sem=sib_send, recv_sem=sib_recv.at[j, t], device_id=(sib,), device_id_type=MESH)

    def raw_copy(piece, t, slot, which):
        place, width = PIECES[piece]
        j = {'diag': 0, 'x_b': 1, 'x_a': 1, 'y_a': 2, 'y_b': 2, 'mine': 3}[piece]
        skip = half if piece in ('x_b', 'y_b') else 0
        n = width * half
        here = pl.ds(place * half, n)
        index = list(PIECES).index(piece)
        src = pl.multiple_of(dests[j] * share + t * 2 * half + skip, TILE)
        land = pl.multiple_of(j * share + t * 2 * half + skip, TILE)
        if which == 0:
            return pltpu.make_async_copy(g.at[:, pl.ds(src, n)], raw_own.at[slot, :, here], own_sem.at[slot, index])
        return pltpu.make_async_copy(sib_land.at[:, pl.ds(land, n)], raw_sib.at[slot, :, here],
                                     sibin_sem.at[slot, index])

    def land_rows(t, part):
        return pl.ds(pl.multiple_of(t * 2 * rows + part * rows, 8), rows)

    def remote(stage, slot, part, land, t, send, recv, target):
        return pltpu.make_async_remote_copy(
            src_ref=stage.at[slot, pl.ds(part * rows, rows), :], dst_ref=land.at[land_rows(t, part), :],
            send_sem=send.at[slot, part], recv_sem=recv.at[part, t], device_id=(target,), device_id_type=MESH)

    def leaf_copy(t, slot, part):
        return remote(leaf_st, slot, part, leaf_land, t, leaf_send, leaf_recv, (y_dev, x_dev)[part])

    def direct_copy(t, slot, part):
        return remote(direct_st, slot, part, direct_land, t, direct_send, direct_recv, (y_dev, x_dev)[part])

    def four_copy(t, slot, part):
        return remote(four_st, slot, part, four_land, t, four_send, four_recv, (x_dev, y_dev)[part])

    def leaf_load(t, part):
        return pltpu.make_async_copy(leaf_land.at[land_rows(t, part), :], leaf_in.at[pl.ds(part * rows, rows), :],
                                     leafin_sem.at[part])

    def fin_load(land, which, t):
        both = pl.ds(pl.multiple_of(t * 2 * rows, 8), 2 * rows)
        return pltpu.make_async_copy(land.at[both, :], fin_in.at[which], fin_sem.at[which])

    def out_copy(t, slot):
        both = pl.ds(pl.multiple_of(t * 2 * rows, 8), 2 * rows)
        return pltpu.make_async_copy(out_st.at[slot], total.at[both, :], out_sem.at[slot])

    blk = block_len(half, 16 * TILE)
    blk_rows = blk // LANES

    def pair(slot, place, i):
        at = pl.ds(pl.multiple_of(place * half + i * blk, TILE), blk)
        own = raw_own[slot, :, at].astype(jnp.float32).reshape(blk_rows, LANES)
        other = raw_sib[slot, :, at].astype(jnp.float32).reshape(blk_rows, LANES)
        return own + other

    def block_rows(i, part=0):
        return pl.ds(pl.multiple_of(part * rows + i * blk_rows, 8), blk_rows)

    def store_pair(slot, place, stage, part):
        @pl.loop(0, half // blk)
        def _(i):
            stage[slot, block_rows(i, part), :] = pair(slot, place, i)

    def wait_raw(piece, t, slot):
        for which in range(2):
            raw_copy(piece, t, slot, which).wait()

    def row_copy(k):
        return pltpu.make_async_remote_copy(
            src_ref=gv, dst_ref=vec_land.at[me], send_sem=vec_send.at[k - 1, 0], recv_sem=vec_recv.at[k - 1, 0],
            device_id=(lax.rem(me + k, n_dev),), device_id_type=MESH)

    def new_copy(k):
        return pltpu.make_async_remote_copy(
            src_ref=vec_new.at[0], dst_ref=vec_w.at[me], send_sem=vec_send.at[k - 1, 1], recv_sem=vec_recv.at[k - 1, 1],
            device_id=(lax.rem(me + k, n_dev),), device_id_type=MESH)

    def send_sib(t):
        for j in range(4):
            sib_copy(j, t).start()

    def fetch(t, which):
        slot = lax.rem(t, 2)

        @pl.when(t < steps)
        def _():
            for j, piece in enumerate(('diag', 'x_b', 'y_a')):
                if which == 1:
                    sib_copy(j, t).wait_recv()
                raw_copy(piece, t, slot, which).start()

        @pl.when(jnp.logical_and(t >= 1, t <= steps))
        def _():
            for piece in ('x_a', 'y_b'):
                raw_copy(piece, t - 1, slot, which).start()

        @pl.when(jnp.logical_and(t >= 2, t <= steps + 1))
        def _():
            if which == 1:
                sib_copy(3, t - 2).wait_recv()
            raw_copy('mine', t - 2, slot, which).start()

    barrier = pltpu.get_barrier_semaphore()
    for k in range(1, n_dev):
        pl.semaphore_signal(barrier, inc=1, device_id=(lax.rem(me + k, n_dev),), device_id_type=MESH)
    fetch(jnp.int32(0), 0)
    pl.semaphore_wait(barrier, n_dev - 1)
    send_sib(0)
    send_sib(1)
    acc[...] = jnp.zeros_like(acc)
    fetch(jnp.int32(0), 1)

    @pl.loop(0, steps + 2)
    def _(t):
        slot = lax.rem(t, 2)
        before = 1 - slot

        @pl.when(t + 2 < steps)
        def _():
            send_sib(t + 2)

        fetch(t + 1, 0)
        fetch(t + 1, 1)

        @pl.when(t < steps)
        def _():
            wait_raw('diag', t, slot)
            for part in range(2):
                @pl.when(t >= 2)
                def _():
                    leaf_copy(t - 2, slot, part).wait_send()
                store_pair(slot, part, leaf_st, part)
                leaf_copy(t, slot, part).start()
            for part, piece, place in ((1, 'x_b', 2), (0, 'y_a', 3)):
                wait_raw(piece, t, slot)

                @pl.when(t >= 2)
                def _():
                    direct_copy(t - 2, slot, part).wait_send()
                store_pair(slot, place, direct_st, part)
                direct_copy(t, slot, part).start()

        @pl.when(t == 0)
        def _():
            for k in range(1, n_dev):
                row_copy(k).start()

        @pl.when(jnp.logical_and(t >= 1, t <= steps))
        def _():
            for part in range(2):
                leaf_copy(t - 1, before, part).wait_recv()
                leaf_load(t - 1, part).start()
            for part, piece, place in ((0, 'x_a', 4), (1, 'y_b', 5)):
                wait_raw(piece, t - 1, slot)

                @pl.when(t >= 3)
                def _():
                    four_copy(t - 3, before, part).wait_send()
                leaf_load(t - 1, part).wait()

                @pl.loop(0, half // blk)
                def _(i):
                    at = block_rows(i, part)
                    four_st[before, at, :] = leaf_in[at, :] + pair(slot, place, i)
                four_copy(t - 1, before, part).start()

        @pl.when(t >= 2)
        def _():
            for part in range(2):
                four_copy(t - 2, slot, part).wait_recv()
                direct_copy(t - 2, slot, part).wait_recv()
            fin_load(four_land, 0, t - 2).start()
            fin_load(direct_land, 1, t - 2).start()
            wait_raw('mine', t - 2, slot)

            @pl.when(t >= 4)
            def _():
                out_copy(t - 4, slot).wait()
            fin_load(four_land, 0, t - 2).wait()
            fin_load(direct_land, 1, t - 2).wait()

            @pl.loop(0, 2 * half // blk)
            def _(i):
                at = block_rows(i)
                whole = (fin_in[0, at, :] + fin_in[1, at, :]) + pair(slot, 6, i)
                out_st[slot, at, :] = whole
                acc[...] += jnp.sum((whole * whole).reshape(blk_rows // 8, 8, LANES), axis=0)
            out_copy(t - 2, slot).start()

    def square_copy(k):
        target = lax.rem(me + k, n_dev)
        return pltpu.make_async_remote_copy(
            src_ref=acc, dst_ref=sq_land.at[me], send_sem=sq_send.at[k - 1], recv_sem=sq_recv.at[k - 1],
            device_id=(target,), device_id_type=MESH)

    for k in range(1, n_dev):
        square_copy(k).start()
    sq_land[me] = acc[...]
    for t in (steps - 2, steps - 1):
        out_copy(t, t % 2).wait()
    own_row = pltpu.make_async_copy(gv, vec_land.at[me], local_sem)
    own_row.start()

    share_rows = share // LANES
    half_rows = share_rows // 2
    w_rows = half_rows // w_steps

    def inside(part, t, n=1):
        return pl.ds(pl.multiple_of(part * half_rows + t * w_rows, 16), n * w_rows)

    def place(dev, part, t):
        return pl.ds(pl.multiple_of(dev * share_rows + part * half_rows + t * w_rows, 16), w_rows)

    def state_copies(t, slot):
        return [pltpu.make_async_copy(src.at[inside(part, t), :], state_in.at[slot, i, part], state_sem.at[slot, i, part])
                for i, src in enumerate((total, p_mat, m_mat, s_mat)) for part in range(2)]

    def own_copy(to, part, t):
        target = (x_dev, y_dev, sib)[to]
        recv = own_sib_recv if to == 2 else own_recv.at[to, part, t]
        return pltpu.make_async_remote_copy(
            src_ref=own_w.at[inside(part, t), :], dst_ref=gathered.at[place(me, part, t), :],
            send_sem=own_send.at[to], recv_sem=recv, device_id=(target,), device_id_type=MESH)

    def keep_copy(part, t):
        return pltpu.make_async_copy(own_w.at[inside(part, t), :], gathered.at[place(me, part, t), :], keep_sem)

    def late_copy(group, part):
        start = w_steps - sum(w_late[group:])
        return pltpu.make_async_copy(own_w.at[inside(part, start, w_late[group]), :],
                                     ((late_a, late_b), (last_a, last_b))[group][part], late_sem.at[group, part])

    def forward(part, t):
        rows_at = place((x_dev, y_dev)[part], part, t)
        return pltpu.make_async_remote_copy(
            src_ref=gathered.at[rows_at, :], dst_ref=gathered.at[rows_at, :],
            send_sem=fwd_send.at[part], recv_sem=fwd_recv.at[part, t],
            device_id=((y_dev, x_dev)[part],), device_id_type=MESH)

    def to_sib(dev, part, t):
        rows_at = place(dev, part, t)
        return pltpu.make_async_remote_copy(
            src_ref=gathered.at[rows_at, :], dst_ref=gathered.at[rows_at, :],
            send_sem=fsib_send, recv_sem=fsib_recv, device_id=(sib,), device_id_type=MESH)

    def all_rows(n, send, recv):
        return pltpu.make_async_remote_copy(
            src_ref=gathered.at[pl.ds(0, n * w_rows), :], dst_ref=gathered.at[pl.ds(0, n * w_rows), :],
            send_sem=send, recv_sem=recv, device_id=(sib,), device_id_type=MESH)

    for copy in state_copies(0, 0):
        copy.start()

    own_row.wait()
    for k in range(1, n_dev):
        row_copy(k).wait()
    vec_total = vec_land[0].astype(jnp.float32)
    for d in range(1, n_dev):
        vec_total += vec_land[d].astype(jnp.float32)
    vec_rows = gv.shape[1] // LANES
    vec_total = vec_total.reshape(vec_rows, LANES)
    square = jnp.sum((vec_total * vec_total).reshape(vec_rows // 8, 8, LANES), axis=0)
    own_rows = pv.shape[0]
    mine = pl.ds(pl.multiple_of(me * own_rows * LANES, LANES), own_rows * LANES)
    vec_sum = vec_land[0, :, mine].astype(jnp.float32)
    for d in range(1, n_dev):
        vec_sum += vec_land[d, :, mine].astype(jnp.float32)
    vec_sum = vec_sum.reshape(own_rows, LANES)
    for k in range(1, n_dev):
        square_copy(k).wait()
    for d in range(n_dev):
        square += sq_land[d]
    norm = jnp.sqrt(jnp.sum(jnp.sum(square, axis=0, keepdims=True), axis=1, keepdims=True))
    coef = jnp.minimum(1.0, 1.0 / (norm + NORM_EPS))
    coef_out[...] = jnp.broadcast_to(coef, coef_out.shape)

    w_tiles = w_rows // 16
    w_blk = 16 * max(d for d in range(1, 9) if w_tiles % d == 0)

    def update(slot, part, t):
        @pl.loop(0, w_rows // w_blk)
        def _(i):
            at = pl.ds(pl.multiple_of(i * w_blk, 16), w_blk)
            grad, master, moment, second = (state_in[slot, k, part, at, :] for k in range(4))
            new = adam_update(grad, coef_out[0:1, :], master, moment, second, DECAY)[0]
            out = pl.ds(pl.multiple_of(part * half_rows + t * w_rows + i * w_blk, 16), w_blk)
            own_w[out, :] = new.astype(jnp.bfloat16)

    early = w_steps - sum(w_late)

    @pl.loop(0, w_steps + LAG + 2)
    def _(u):
        slot = lax.rem(u, 2)

        @pl.when(u + 1 < w_steps)
        def _():
            for copy in state_copies(u + 1, 1 - slot):
                copy.start()

        @pl.when(u < w_steps)
        def _():
            for copy in state_copies(u, slot):
                copy.wait()
            for part in range(2):
                update(slot, part, u)
                own_copy(part, part, u).start()

                @pl.when(u < early)
                def _():
                    own_copy(1 - part, part, u).start()
                own_copy(2, part, u).start()
                keep_copy(part, u).start()

        @pl.when(jnp.logical_and(u >= LAG, u < w_steps + LAG))
        def _():
            t = u - LAG
            for part in range(2):
                own_copy(part, part, t).wait_recv()
                forward(part, t).start()
                to_sib((x_dev, y_dev)[part], part, t).start()

            @pl.when(t < early)
            def _():
                for part in range(2):
                    own_copy(1 - part, part, t).wait_recv()
                    to_sib((y_dev, x_dev)[part], part, t).start()

        @pl.when(u >= LAG + 2)
        def _():
            t = u - LAG - 2
            for part in range(2):
                forward(part, t).wait_recv()
                to_sib(g_dev, part, t).start()

        @pl.when(u == 1)
        def _():
            new = adam_update(vec_sum, coef_out[0:1, :], pv[...], mv[...], sv[...], 0.0)
            for i in range(3):
                vec_new[i] = new[i]
            vec_w[me] = new[0]
            for k in range(1, n_dev):
                new_copy(k).start()

        @pl.when(u == w_steps - 1)
        def _():
            for group in range(2):
                for part in range(2):
                    late_copy(group, part).start()

    for k in range(1, n_dev):
        new_copy(k).wait()

    for t in (steps - 2, steps - 1):
        slot = t % 2
        for part in range(2):
            leaf_copy(t, slot, part).wait_send()
            direct_copy(t, slot, part).wait_send()
            four_copy(t, slot, part).wait_send()
    pltpu.make_async_remote_copy(
        src_ref=g.at[:, pl.ds(0, 4 * share)], dst_ref=sib_land, send_sem=sib_send, recv_sem=sib_recv.at[0, 0],
        device_id=(sib,), device_id_type=MESH).wait_send()
    for part in range(2):
        late_copy(0, part).wait()
        late_copy(1, part).wait()
        all_rows(w_steps + early, own_send.at[part], fsib_recv).wait_send()
        all_rows(w_steps, fwd_send.at[part], fsib_recv).wait_send()
    all_rows(2 * w_steps, own_send.at[2], own_sib_recv).wait()
    all_rows(4 * w_steps + 2 * early, fsib_send, fsib_recv).wait()
    pltpu.make_async_copy(own_w, gathered.at[pl.ds(0, share_rows), :], keep_sem).wait()


def step_call(g, gv, p_mat, m_mat, s_mat, pv, mv, sv, share, steps, w_steps, w_late):
    half = share // (2 * steps)
    rows = half // LANES
    share_rows = share // LANES
    w_rows = share_rows // (2 * w_steps)
    dma = pltpu.SemaphoreType.DMA
    f32, bf16 = jnp.float32, jnp.bfloat16
    own_rows = pv.shape[0]
    hbm = pl.BlockSpec(memory_space=pltpu.HBM)
    vmem = pl.BlockSpec(memory_space=pltpu.VMEM)
    return pl.pallas_call(
        functools.partial(step_kernel, share, half, steps, w_steps, w_late),
        out_shape=(jax.ShapeDtypeStruct((share_rows, LANES), f32),
                   jax.ShapeDtypeStruct((8 * share_rows, LANES), bf16),
                   jax.ShapeDtypeStruct((w_late[0] * w_rows, LANES), bf16),
                   jax.ShapeDtypeStruct((w_late[0] * w_rows, LANES), bf16),
                   jax.ShapeDtypeStruct((w_late[1] * w_rows, LANES), bf16),
                   jax.ShapeDtypeStruct((w_late[1] * w_rows, LANES), bf16),
                   jax.ShapeDtypeStruct((1, 4 * share), bf16),
                   jax.ShapeDtypeStruct((share_rows, LANES), f32),
                   jax.ShapeDtypeStruct((share_rows, LANES), f32),
                   jax.ShapeDtypeStruct((share_rows, LANES), f32),
                   jax.ShapeDtypeStruct((8, LANES), f32),
                   jax.ShapeDtypeStruct((3, own_rows, LANES), f32),
                   jax.ShapeDtypeStruct((8, own_rows, LANES), f32)),
        in_specs=[hbm, vmem, hbm, hbm, hbm, vmem, vmem, vmem],
        out_specs=(hbm,) * 10 + (vmem,) * 3,
        scratch_shapes=[
            pltpu.VMEM((2, 1, 8 * half), bf16),
            pltpu.VMEM((2, 1, 8 * half), bf16),
            pltpu.VMEM((2, 2 * rows, LANES), f32),
            pltpu.VMEM((2, 2 * rows, LANES), f32),
            pltpu.VMEM((2, 2 * rows, LANES), f32),
            pltpu.VMEM((2 * rows, LANES), f32),
            pltpu.VMEM((2, 2 * rows, LANES), f32),
            pltpu.VMEM((2, 2 * rows, LANES), f32),
            pltpu.VMEM((8, LANES), f32),
            pltpu.VMEM((8, 8, LANES), f32),
            pltpu.VMEM((8, 1, gv.shape[1]), bf16),
            dma(()), dma((4, steps)),
            dma((2, 2)), dma((2, steps)), dma((2, 2)), dma((2, steps)), dma((2, 2)), dma((2, steps)),
            dma((2, 6)), dma((2, 6)), dma((2,)), dma((2,)), dma((2,)),
            dma((7,)), dma((7,)), dma((7, 2)), dma((7, 2)), dma(()),
            pltpu.VMEM((2, 4, 2, w_rows, LANES), f32),
            pltpu.VMEM((share_rows, LANES), bf16),
            dma((2, 4, 2)), dma((3,)), dma((2, 2, w_steps)), dma(()), dma(()), dma((2, 2)),
            dma((2,)), dma((2, w_steps)), dma(()), dma(()),
        ],
        compiler_params=pltpu.CompilerParams(collective_id=0, has_side_effects=True, vmem_limit_bytes=60 * 2**20),
        name='reduce_update_gather',
    )(g, gv, p_mat, m_mat, s_mat, pv, mv, sv)


def update_kernel(coef, grad, master, moment, second, vec_new, vec_w, new_p, new_m, new_s, vec_p, vec_m, vec_s, w_vec,
                  rows):
    new_p[...], new_m[...], new_s[...] = adam_update(grad[...], coef[0:1, :], master[...], moment[...], second[...], DECAY)

    @pl.when(pl.program_id(0) == 0)
    def _():
        vec_p[...], vec_m[...], vec_s[...] = vec_new[0], vec_new[1], vec_new[2]
        n = vec_w.shape[1]
        for d in range(vec_w.shape[0]):
            rows[pl.ds(d * n, n), :] = vec_w[d]
        w_vec[...] = rows[...].astype(jnp.bfloat16)


def update_call(coef, grad, master, moment, second, vec_new, vec_w, block):
    n = grad.shape[0]
    own_rows = vec_new.shape[1]
    f32 = jnp.float32
    tile = pl.BlockSpec((block, LANES), lambda i: (i, 0))

    def whole(shape):
        return pl.BlockSpec(shape, lambda i: (0,) * len(shape))

    small = jax.ShapeDtypeStruct((own_rows, LANES), f32)
    return pl.pallas_call(
        update_kernel,
        grid=(n // block,),
        out_shape=(jax.ShapeDtypeStruct(grad.shape, f32),) * 3 + (small,) * 3 + (
            jax.ShapeDtypeStruct((8 * own_rows, LANES), jnp.bfloat16),),
        in_specs=[whole((8, LANES))] + [tile] * 4 + [whole(vec_new.shape), whole(vec_w.shape)],
        out_specs=(tile,) * 3 + (whole((own_rows, LANES)),) * 3 + (whole((8 * own_rows, LANES)),),
        scratch_shapes=[pltpu.VMEM((8 * own_rows, LANES), f32)],
        compiler_params=pltpu.CompilerParams(vmem_limit_bytes=40 * 2**20),
        cost_estimate=pl.CostEstimate(flops=n * LANES * 200, bytes_accessed=n * LANES * 28, transcendentals=0),
        name='update',
    )(coef, grad, master, moment, second, vec_new, vec_w)


def copy_kernel(moves, blocks, *refs):
    n_src = 1 + max(move[0] for move in moves(0))
    srcs, out, buf, in_sem, out_sem = refs[:n_src], refs[-4], refs[-3], refs[-2], refs[-1]
    me = lax.axis_index('fsdp')
    todo = []
    for which, src_row, dst_row, n in moves(me):
        size = n // blocks(n)
        for i in range(blocks(n)):
            todo.append((srcs[which], src_row + i * size, dst_row + i * size, size))
    slots = buf.shape[0]

    def take(k):
        src, src_row, _, size = todo[k]
        return pltpu.make_async_copy(src.at[pl.ds(pl.multiple_of(src_row, 16), size), :],
                                     buf.at[k % slots, pl.ds(0, size), :], in_sem.at[k % slots])

    def give(k):
        _, _, dst_row, size = todo[k]
        return pltpu.make_async_copy(buf.at[k % slots, pl.ds(0, size), :],
                                     out.at[pl.ds(pl.multiple_of(dst_row, 16), size), :], out_sem.at[k % slots])

    ahead = slots // 2
    for k in range(min(ahead, len(todo))):
        take(k).start()
    for k in range(len(todo)):
        take(k).wait()
        give(k).start()
        if k + ahead < len(todo):
            if k + ahead >= slots:
                give(k + ahead - slots).wait()
            take(k + ahead).start()
    for k in range(max(0, len(todo) - slots), len(todo)):
        give(k).wait()


def copy_call(name, moves, srcs, out_rows, into=None, slots=12, most=4160):
    def blocks(n):
        return next(d for d in range(1, n // 16 + 1) if (n // 16) % d == 0 and n // d <= most)

    hbm = pl.BlockSpec(memory_space=pltpu.HBM)
    args = list(srcs) + ([into] if into is not None else [])
    size = sum(move[3] for move in moves(0)) * LANES * 2
    return pl.pallas_call(
        functools.partial(copy_kernel, moves, blocks),
        out_shape=jax.ShapeDtypeStruct((out_rows, LANES), jnp.bfloat16),
        in_specs=[hbm] * len(args),
        out_specs=hbm,
        scratch_shapes=[pltpu.VMEM((slots, most, LANES), jnp.bfloat16),
                        pltpu.SemaphoreType.DMA((slots,)), pltpu.SemaphoreType.DMA((slots,))],
        input_output_aliases={len(srcs): 0} if into is not None else {},
        compiler_params=pltpu.CompilerParams(vmem_limit_bytes=32 * 2**20),
        cost_estimate=pl.CostEstimate(flops=size * 6, bytes_accessed=2 * size, transcendentals=0),
        name=name,
    )(*args)


def block_rows_of(n):
    return 16 * max(d for d in range(1, 190) if (n // 16) % d == 0)


STEPS = 28
W_STEPS = 14
W_LATE = (10, 2)
LAG = 3


def neighbours(me):
    core, x_pos, y_pos = lax.rem(me, 2), lax.rem(me // 2, 2), me // 4
    return me + 1 - 2 * core, me + 2 - 4 * x_pos, me + 4 - 8 * y_pos


def solution(mesh):
    hop_x = [(d, d ^ 2) for d in range(8)]
    hop_y = [(d, d ^ 4) for d in range(8)]
    hop_core = [(d, d ^ 1) for d in range(8)]

    def local_step(grad_mat, grad_vec, master_mat, moment_mat, second_mat, master_vec, moment_vec, second_vec):
        share = master_mat.shape[0]
        share_rows = share // LANES
        half_rows = share_rows // 2
        late, last = (n * (half_rows // W_STEPS) for n in W_LATE)
        early = half_rows - late - last
        own_rows = master_vec.shape[0] // LANES
        mats = [v.reshape(share_rows, LANES) for v in (master_mat, moment_mat, second_mat)]
        vecs = [v.reshape(own_rows, LANES) for v in (master_vec, moment_vec, second_vec)]
        total, gathered, late_a, late_b, last_a, last_b, _, _, _, _, coef, vec_new, vec_w = step_call(
            grad_mat, grad_vec, *mats, *vecs, share, STEPS, W_STEPS, W_LATE)

        late_x = lax.ppermute(late_b, 'fsdp', hop_x)
        late_y = lax.ppermute(late_a, 'fsdp', hop_y)
        last_x = lax.ppermute(last_b, 'fsdp', hop_x)
        last_y = lax.ppermute(last_a, 'fsdp', hop_y)

        def whole_moves(me):
            sib, x_dev, y_dev = neighbours(me)
            g_dev = x_dev + y_dev - me
            flip = sib - me
            return [(0, dev * share_rows, dev * share_rows, share_rows) for dev in (me, sib, g_dev, g_dev + flip)]

        def early_moves(me):
            sib, x_dev, y_dev = neighbours(me)
            flip = sib - me
            moves = []
            for dev in (x_dev, x_dev + flip):
                moves.append((0, dev * share_rows, dev * share_rows, half_rows + early))
            for dev in (y_dev, y_dev + flip):
                moves.append((0, dev * share_rows, dev * share_rows, early))
                moves.append((0, dev * share_rows + half_rows, dev * share_rows + half_rows, half_rows))
            return moves

        def late_rows(x_dev, y_dev):
            return [(0, 0, x_dev * share_rows + half_rows + early, late),
                    (1, 0, y_dev * share_rows + early, late),
                    (2, 0, x_dev * share_rows + half_rows + early + late, last),
                    (3, 0, y_dev * share_rows + early + late, last)]

        def own_late_moves(me):
            _, x_dev, y_dev = neighbours(me)
            return late_rows(x_dev, y_dev)

        def sib_late_moves(me):
            sib, x_dev, y_dev = neighbours(me)
            return late_rows(x_dev + sib - me, y_dev + sib - me)

        *new, weights_vec = update_call(coef, total, *mats, vec_new, vec_w, block_rows_of(share_rows))
        weights = copy_call('collect_whole', whole_moves, (gathered,), 8 * share_rows)
        late_x, late_y, weights, *new = lax.optimization_barrier((late_x, late_y, weights, *new))
        sib_late_x = lax.ppermute(late_x, 'fsdp', hop_core)
        sib_late_y = lax.ppermute(late_y, 'fsdp', hop_core)
        weights = copy_call('collect_early', early_moves, (gathered,), 8 * share_rows, into=weights)
        last_x, last_y, weights = lax.optimization_barrier((last_x, last_y, weights))
        sib_last_x = lax.ppermute(last_x, 'fsdp', hop_core)
        sib_last_y = lax.ppermute(last_y, 'fsdp', hop_core)
        weights = copy_call('collect_late', own_late_moves, (late_x, late_y, last_x, last_y), 8 * share_rows, into=weights)
        weights = copy_call('collect_last', sib_late_moves, (sib_late_x, sib_late_y, sib_last_x, sib_last_y),
                            8 * share_rows, into=weights)
        return tuple(v.reshape(-1) for v in (*new, weights, weights_vec))

    row_spec = P('fsdp', None)
    flat_spec = P('fsdp')
    whole_spec = P()
    return jax.shard_map(local_step, mesh=mesh,
                         in_specs=(row_spec, row_spec) + (flat_spec,) * 6,
                         out_specs=(flat_spec,) * 6 + (whole_spec, whole_spec),
                         check_vma=False)
```

```python
import functools

import jax
import jax.numpy as jnp
from jax import lax
from jax.experimental import pallas as pl
from jax.experimental.pallas import tpu as pltpu
from jax.sharding import PartitionSpec as P


STEP = 4
LEARN_RATE = 1e-3
BETA_ONE = 0.9
BETA_TWO = 0.999
ADAM_EPS = 1e-8
DECAY = 0.01
NORM_EPS = 1e-6
FIX_ONE = 1.0 - BETA_ONE ** STEP
FIX_TWO = 1.0 - BETA_TWO ** STEP

MESH = pl.DeviceIdType.MESH
LANES = 128
TILE = 1024


def adam_update(grad_sum, clip_coef, master, moment, second, decay):
    clip_grad = clip_coef * grad_sum
    new_moment = BETA_ONE * moment + (1.0 - BETA_ONE) * clip_grad
    new_second = BETA_TWO * second + (1.0 - BETA_TWO) * clip_grad * clip_grad
    step_dir = (new_moment * (LEARN_RATE / FIX_ONE)) / (jnp.sqrt(new_second * (1.0 / FIX_TWO)) + ADAM_EPS)
    new_master = master - (step_dir + (LEARN_RATE * decay) * master)
    return new_master, new_moment, new_second


def block_len(n, most):
    tiles = n // TILE
    return max(d for d in range(1, most // TILE + 1) if tiles % d == 0) * TILE


PIECES = {'diag': (0, 2), 'x_b': (2, 1), 'y_a': (3, 1), 'x_a': (4, 1), 'y_b': (5, 1), 'mine': (6, 2)}


def step_kernel(share, half, steps, w_steps, w_late, g, gv, p_mat, m_mat, s_mat, pv, mv, sv,
                total, gathered, late_a, late_b, last_a, last_b, sib_land, leaf_land, four_land, direct_land, coef_out, vec_new, vec_w,
                raw_own, raw_sib, leaf_st, direct_st, four_st, leaf_in, fin_in, out_st, acc, sq_land, vec_land,
                  sib_send, sib_recv, leaf_send, leaf_recv, four_send, four_recv, direct_send, direct_recv,
                  own_sem, sibin_sem, leafin_sem, fin_sem, out_sem, sq_send, sq_recv, vec_send, vec_recv, local_sem,
                state_in, own_w, state_sem, own_send, own_recv, own_sib_recv, keep_sem, late_sem,
                fwd_send, fwd_recv, fsib_send, fsib_recv):
    me = lax.axis_index('fsdp')
    core = lax.rem(me, 2)
    x_pos = lax.rem(me // 2, 2)
    y_pos = me // 4
    sib = me + 1 - 2 * core
    x_dev = me + 2 - 4 * x_pos
    y_dev = me + 4 - 8 * y_pos
    g_dev = y_dev + 2 - 4 * x_pos
    sib_delta = 1 - 2 * core
    dests = (g_dev, x_dev, y_dev, me)
    rows = half // LANES
    n_dev = 8

    def sib_copy(j, t):
        src = pl.multiple_of((dests[j] + sib_delta) * share + t * 2 * half, TILE)
        dst = pl.multiple_of(j * share + t * 2 * half, TILE)
        return pltpu.make_async_remote_copy(
            src_ref=g.at[:, pl.ds(src, 2 * half)], dst_ref=sib_land.at[:, pl.ds(dst, 2 * half)],
            send_sem=sib_send, recv_sem=sib_recv.at[j, t], device_id=(sib,), device_id_type=MESH)

    def raw_copy(piece, t, slot, which):
        place, width = PIECES[piece]
        j = {'diag': 0, 'x_b': 1, 'x_a': 1, 'y_a': 2, 'y_b': 2, 'mine': 3}[piece]
        skip = half if piece in ('x_b', 'y_b') else 0
        n = width * half
        here = pl.ds(place * half, n)
        index = list(PIECES).index(piece)
        src = pl.multiple_of(dests[j] * share + t * 2 * half + skip, TILE)
        land = pl.multiple_of(j * share + t * 2 * half + skip, TILE)
        if which == 0:
            return pltpu.make_async_copy(g.at[:, pl.ds(src, n)], raw_own.at[slot, :, here], own_sem.at[slot, index])
        return pltpu.make_async_copy(sib_land.at[:, pl.ds(land, n)], raw_sib.at[slot, :, here],
                                     sibin_sem.at[slot, index])

    def land_rows(t, part):
        return pl.ds(pl.multiple_of(t * 2 * rows + part * rows, 8), rows)

    def remote(stage, slot, part, land, t, send, recv, target):
        return pltpu.make_async_remote_copy(
            src_ref=stage.at[slot, pl.ds(part * rows, rows), :], dst_ref=land.at[land_rows(t, part), :],
            send_sem=send.at[slot, part], recv_sem=recv.at[part, t], device_id=(target,), device_id_type=MESH)

    def leaf_copy(t, slot, part):
        return remote(leaf_st, slot, part, leaf_land, t, leaf_send, leaf_recv, (y_dev, x_dev)[part])

    def direct_copy(t, slot, part):
        return remote(direct_st, slot, part, direct_land, t, direct_send, direct_recv, (y_dev, x_dev)[part])

    def four_copy(t, slot, part):
        return remote(four_st, slot, part, four_land, t, four_send, four_recv, (x_dev, y_dev)[part])

    def leaf_load(t, part):
        return pltpu.make_async_copy(leaf_land.at[land_rows(t, part), :], leaf_in.at[pl.ds(part * rows, rows), :],
                                     leafin_sem.at[part])

    def fin_load(land, which, t):
        both = pl.ds(pl.multiple_of(t * 2 * rows, 8), 2 * rows)
        return pltpu.make_async_copy(land.at[both, :], fin_in.at[which], fin_sem.at[which])

    def out_copy(t, slot):
        both = pl.ds(pl.multiple_of(t * 2 * rows, 8), 2 * rows)
        return pltpu.make_async_copy(out_st.at[slot], total.at[both, :], out_sem.at[slot])

    blk = block_len(half, 16 * TILE)
    blk_rows = blk // LANES

    def pair(slot, place, i):
        at = pl.ds(pl.multiple_of(place * half + i * blk, TILE), blk)
        own = raw_own[slot, :, at].astype(jnp.float32).reshape(blk_rows, LANES)
        other = raw_sib[slot, :, at].astype(jnp.float32).reshape(blk_rows, LANES)
        return own + other

    def block_rows(i, part=0):
        return pl.ds(pl.multiple_of(part * rows + i * blk_rows, 8), blk_rows)

    def store_pair(slot, place, stage, part):
        @pl.loop(0, half // blk)
        def _(i):
            stage[slot, block_rows(i, part), :] = pair(slot, place, i)

    def wait_raw(piece, t, slot):
        for which in range(2):
            raw_copy(piece, t, slot, which).wait()

    def row_copy(k):
        return pltpu.make_async_remote_copy(
            src_ref=gv, dst_ref=vec_land.at[me], send_sem=vec_send.at[k - 1, 0], recv_sem=vec_recv.at[k - 1, 0],
            device_id=(lax.rem(me + k, n_dev),), device_id_type=MESH)

    def new_copy(k):
        return pltpu.make_async_remote_copy(
            src_ref=vec_new.at[0], dst_ref=vec_w.at[me], send_sem=vec_send.at[k - 1, 1], recv_sem=vec_recv.at[k - 1, 1],
            device_id=(lax.rem(me + k, n_dev),), device_id_type=MESH)

    def send_sib(t):
        @pl.when(t < steps)
        def _():
            for j in range(3):
                sib_copy(j, t).start()

        @pl.when(t >= 1)
        def _():
            sib_copy(3, t - 1).start()

    def fetch(t, which):
        slot = lax.rem(t, 2)

        @pl.when(t < steps)
        def _():
            for j, piece in enumerate(('diag', 'x_b', 'y_a')):
                if which == 1:
                    sib_copy(j, t).wait_recv()
                raw_copy(piece, t, slot, which).start()

        @pl.when(jnp.logical_and(t >= 1, t <= steps))
        def _():
            for piece in ('x_a', 'y_b'):
                raw_copy(piece, t - 1, slot, which).start()

        @pl.when(jnp.logical_and(t >= 2, t <= steps + 1))
        def _():
            if which == 1:
                sib_copy(3, t - 2).wait_recv()
            raw_copy('mine', t - 2, slot, which).start()

    barrier = pltpu.get_barrier_semaphore()
    for k in range(1, n_dev):
        pl.semaphore_signal(barrier, inc=1, device_id=(lax.rem(me + k, n_dev),), device_id_type=MESH)
    fetch(jnp.int32(0), 0)
    pl.semaphore_wait(barrier, n_dev - 1)
    send_sib(jnp.int32(0))
    acc[...] = jnp.zeros_like(acc)
    fetch(jnp.int32(0), 1)
    send_sib(jnp.int32(1))

    @pl.loop(0, steps + 2)
    def _(t):
        slot = lax.rem(t, 2)
        before = 1 - slot

        @pl.when(t + 2 <= steps)
        def _():
            send_sib(t + 2)

        fetch(t + 1, 0)

        @pl.when(t < steps)
        def _():
            wait_raw('diag', t, slot)
            for part in range(2):
                @pl.when(t >= 2)
                def _():
                    leaf_copy(t - 2, slot, part).wait_send()

                store_pair(slot, part, leaf_st, part)
                leaf_copy(t, slot, part).start()
            for part, piece, place in ((1, 'x_b', 2), (0, 'y_a', 3)):
                wait_raw(piece, t, slot)

                @pl.when(t >= 2)
                def _():
                    direct_copy(t - 2, slot, part).wait_send()

                store_pair(slot, place, direct_st, part)
                direct_copy(t, slot, part).start()

        fetch(t + 1, 1)

        @pl.when(t == 0)
        def _():
            for k in range(1, n_dev):
                row_copy(k).start()

        @pl.when(jnp.logical_and(t >= 1, t <= steps))
        def _():
            for part in range(2):
                leaf_copy(t - 1, before, part).wait_recv()
                leaf_load(t - 1, part).start()
            for part, piece, place in ((0, 'x_a', 4), (1, 'y_b', 5)):
                wait_raw(piece, t - 1, slot)

                @pl.when(t >= 3)
                def _():
                    four_copy(t - 3, before, part).wait_send()

                leaf_load(t - 1, part).wait()

                @pl.loop(0, half // blk)
                def _(i):
                    at = block_rows(i, part)
                    four_st[before, at, :] = leaf_in[at, :] + pair(slot, place, i)

                four_copy(t - 1, before, part).start()

        @pl.when(t >= 2)
        def _():
            for part in range(2):
                four_copy(t - 2, slot, part).wait_recv()
                direct_copy(t - 2, slot, part).wait_recv()
            fin_load(four_land, 0, t - 2).start()
            fin_load(direct_land, 1, t - 2).start()
            wait_raw('mine', t - 2, slot)

            @pl.when(t >= 4)
            def _():
                out_copy(t - 4, slot).wait()

            fin_load(four_land, 0, t - 2).wait()
            fin_load(direct_land, 1, t - 2).wait()

            @pl.loop(0, 2 * half // blk)
            def _(i):
                at = block_rows(i)
                whole = (fin_in[0, at, :] + fin_in[1, at, :]) + pair(slot, 6, i)
                out_st[slot, at, :] = whole
                acc[...] += jnp.sum((whole * whole).reshape(blk_rows // 8, 8, LANES), axis=0)

            out_copy(t - 2, slot).start()

    def square_copy(k):
        target = lax.rem(me + k, n_dev)
        return pltpu.make_async_remote_copy(
            src_ref=acc, dst_ref=sq_land.at[me], send_sem=sq_send.at[k - 1], recv_sem=sq_recv.at[k - 1],
            device_id=(target,), device_id_type=MESH)

    for k in range(1, n_dev):
        square_copy(k).start()
    sq_land[me] = acc[...]
    for t in (steps - 2, steps - 1):
        out_copy(t, t % 2).wait()
    own_row = pltpu.make_async_copy(gv, vec_land.at[me], local_sem)
    own_row.start()

    share_rows = share // LANES
    half_rows = share_rows // 2
    w_rows = half_rows // w_steps

    def inside(part, t, n=1):
        return pl.ds(pl.multiple_of(part * half_rows + t * w_rows, 16), n * w_rows)

    def place(dev, part, t):
        return pl.ds(pl.multiple_of(dev * share_rows + part * half_rows + t * w_rows, 16), w_rows)

    def state_copies(t, slot):
        return [pltpu.make_async_copy(src.at[inside(part, t), :], state_in.at[slot, i, part], state_sem.at[slot, i, part])
                for i, src in enumerate((total, p_mat, m_mat, s_mat)) for part in range(2)]

    def own_copy(to, part, t):
        target = (x_dev, y_dev, sib)[to]
        recv = own_sib_recv if to == 2 else own_recv.at[to, part, t]
        return pltpu.make_async_remote_copy(
            src_ref=own_w.at[inside(part, t), :], dst_ref=gathered.at[place(me, part, t), :],
            send_sem=own_send.at[to], recv_sem=recv, device_id=(target,), device_id_type=MESH)

    def keep_copy(part, t):
        return pltpu.make_async_copy(own_w.at[inside(part, t), :], gathered.at[place(me, part, t), :], keep_sem)

    def late_copy(group, part):
        start = w_steps - sum(w_late[group:])
        return pltpu.make_async_copy(own_w.at[inside(part, start, w_late[group]), :],
                                     ((late_a, late_b), (last_a, last_b))[group][part], late_sem.at[group, part])

    def forward(part, t):
        rows_at = place((x_dev, y_dev)[part], part, t)
        return pltpu.make_async_remote_copy(
            src_ref=gathered.at[rows_at, :], dst_ref=gathered.at[rows_at, :],
            send_sem=fwd_send.at[part], recv_sem=fwd_recv.at[part, t],
            device_id=((y_dev, x_dev)[part],), device_id_type=MESH)

    def to_sib(dev, part, t):
        rows_at = place(dev, part, t)
        return pltpu.make_async_remote_copy(
            src_ref=gathered.at[rows_at, :], dst_ref=gathered.at[rows_at, :],
            send_sem=fsib_send, recv_sem=fsib_recv, device_id=(sib,), device_id_type=MESH)

    def all_rows(n, send, recv):
        return pltpu.make_async_remote_copy(
            src_ref=gathered.at[pl.ds(0, n * w_rows), :], dst_ref=gathered.at[pl.ds(0, n * w_rows), :],
            send_sem=send, recv_sem=recv, device_id=(sib,), device_id_type=MESH)

    for copy in state_copies(0, 0):
        copy.start()

    own_row.wait()
    for k in range(1, n_dev):
        row_copy(k).wait()
    vec_total = vec_land[0].astype(jnp.float32)
    for d in range(1, n_dev):
        vec_total += vec_land[d].astype(jnp.float32)
    vec_rows = gv.shape[1] // LANES
    vec_total = vec_total.reshape(vec_rows, LANES)
    square = jnp.sum((vec_total * vec_total).reshape(vec_rows // 8, 8, LANES), axis=0)
    own_rows = pv.shape[0]
    mine = pl.ds(pl.multiple_of(me * own_rows * LANES, LANES), own_rows * LANES)
    vec_sum = vec_land[0, :, mine].astype(jnp.float32)
    for d in range(1, n_dev):
        vec_sum += vec_land[d, :, mine].astype(jnp.float32)
    vec_sum = vec_sum.reshape(own_rows, LANES)
    for k in range(1, n_dev):
        square_copy(k).wait()
    for d in range(n_dev):
        square += sq_land[d]
    norm = jnp.sqrt(jnp.sum(jnp.sum(square, axis=0, keepdims=True), axis=1, keepdims=True))
    coef = jnp.minimum(1.0, 1.0 / (norm + NORM_EPS))
    coef_out[...] = jnp.broadcast_to(coef, coef_out.shape)

    w_tiles = w_rows // 16
    w_blk = 16 * max(d for d in range(1, 9) if w_tiles % d == 0)

    def update(slot, part, t):
        @pl.loop(0, w_rows // w_blk)
        def _(i):
            at = pl.ds(pl.multiple_of(i * w_blk, 16), w_blk)
            grad, master, moment, second = (state_in[slot, k, part, at, :] for k in range(4))
            new = adam_update(grad, coef_out[0:1, :], master, moment, second, DECAY)[0]
            out = pl.ds(pl.multiple_of(part * half_rows + t * w_rows + i * w_blk, 16), w_blk)
            own_w[out, :] = new.astype(jnp.bfloat16)

    early = w_steps - sum(w_late)

    @pl.loop(0, w_steps + LAG + 2)
    def _(u):
        slot = lax.rem(u, 2)

        @pl.when(u + 1 < w_steps)
        def _():
            for copy in state_copies(u + 1, 1 - slot):
                copy.start()

        @pl.when(u < w_steps)
        def _():
            for copy in state_copies(u, slot):
                copy.wait()
            for part in range(2):
                update(slot, part, u)
                own_copy(part, part, u).start()

                @pl.when(u < early)
                def _():
                    own_copy(1 - part, part, u).start()

                own_copy(2, part, u).start()
                keep_copy(part, u).start()

        @pl.when(jnp.logical_and(u >= LAG, u < w_steps + LAG))
        def _():
            t = u - LAG
            for part in range(2):
                own_copy(part, part, t).wait_recv()
                forward(part, t).start()
                to_sib((x_dev, y_dev)[part], part, t).start()

            @pl.when(t < early)
            def _():
                for part in range(2):
                    own_copy(1 - part, part, t).wait_recv()
                    to_sib((y_dev, x_dev)[part], part, t).start()

        @pl.when(u >= LAG + 2)
        def _():
            t = u - LAG - 2
            for part in range(2):
                forward(part, t).wait_recv()
                to_sib(g_dev, part, t).start()

        @pl.when(u == 1)
        def _():
            new = adam_update(vec_sum, coef_out[0:1, :], pv[...], mv[...], sv[...], 0.0)
            for i in range(3):
                vec_new[i] = new[i]
            vec_w[me] = new[0]
            for k in range(1, n_dev):
                new_copy(k).start()

        @pl.when(u == w_steps - 1)
        def _():
            for group in range(2):
                for part in range(2):
                    late_copy(group, part).start()

    for k in range(1, n_dev):
        new_copy(k).wait()

    for t in (steps - 2, steps - 1):
        slot = t % 2
        for part in range(2):
            leaf_copy(t, slot, part).wait_send()
            direct_copy(t, slot, part).wait_send()
            four_copy(t, slot, part).wait_send()
    pltpu.make_async_remote_copy(
        src_ref=g.at[:, pl.ds(0, 4 * share)], dst_ref=sib_land, send_sem=sib_send, recv_sem=sib_recv.at[0, 0],
        device_id=(sib,), device_id_type=MESH).wait_send()
    for part in range(2):
        late_copy(0, part).wait()
        late_copy(1, part).wait()
        all_rows(w_steps + early, own_send.at[part], fsib_recv).wait_send()
        all_rows(w_steps, fwd_send.at[part], fsib_recv).wait_send()
    all_rows(2 * w_steps, own_send.at[2], own_sib_recv).wait()
    all_rows(4 * w_steps + 2 * early, fsib_send, fsib_recv).wait()
    pltpu.make_async_copy(own_w, gathered.at[pl.ds(0, share_rows), :], keep_sem).wait()


def step_call(g, gv, p_mat, m_mat, s_mat, pv, mv, sv, share, steps, w_steps, w_late):
    half = share // (2 * steps)
    rows = half // LANES
    share_rows = share // LANES
    w_rows = share_rows // (2 * w_steps)
    dma = pltpu.SemaphoreType.DMA
    f32, bf16 = jnp.float32, jnp.bfloat16
    own_rows = pv.shape[0]
    hbm = pl.BlockSpec(memory_space=pltpu.HBM)
    vmem = pl.BlockSpec(memory_space=pltpu.VMEM)
    return pl.pallas_call(
        functools.partial(step_kernel, share, half, steps, w_steps, w_late),
        out_shape=(jax.ShapeDtypeStruct((share_rows, LANES), f32),
                   jax.ShapeDtypeStruct((8 * share_rows, LANES), bf16),
                   jax.ShapeDtypeStruct((w_late[0] * w_rows, LANES), bf16),
                   jax.ShapeDtypeStruct((w_late[0] * w_rows, LANES), bf16),
                   jax.ShapeDtypeStruct((w_late[1] * w_rows, LANES), bf16),
                   jax.ShapeDtypeStruct((w_late[1] * w_rows, LANES), bf16),
                   jax.ShapeDtypeStruct((1, 4 * share), bf16),
                   jax.ShapeDtypeStruct((share_rows, LANES), f32),
                   jax.ShapeDtypeStruct((share_rows, LANES), f32),
                   jax.ShapeDtypeStruct((share_rows, LANES), f32),
                   jax.ShapeDtypeStruct((8, LANES), f32),
                   jax.ShapeDtypeStruct((3, own_rows, LANES), f32),
                   jax.ShapeDtypeStruct((8, own_rows, LANES), f32)),
        in_specs=[hbm, vmem, hbm, hbm, hbm, vmem, vmem, vmem],
        out_specs=(hbm,) * 10 + (vmem,) * 3,
        scratch_shapes=[
            pltpu.VMEM((2, 1, 8 * half), bf16),
            pltpu.VMEM((2, 1, 8 * half), bf16),
            pltpu.VMEM((2, 2 * rows, LANES), f32),
            pltpu.VMEM((2, 2 * rows, LANES), f32),
            pltpu.VMEM((2, 2 * rows, LANES), f32),
            pltpu.VMEM((2 * rows, LANES), f32),
            pltpu.VMEM((2, 2 * rows, LANES), f32),
            pltpu.VMEM((2, 2 * rows, LANES), f32),
            pltpu.VMEM((8, LANES), f32),
            pltpu.VMEM((8, 8, LANES), f32),
            pltpu.VMEM((8, 1, gv.shape[1]), bf16),
            dma(()), dma((4, steps)),
            dma((2, 2)), dma((2, steps)), dma((2, 2)), dma((2, steps)), dma((2, 2)), dma((2, steps)),
            dma((2, 6)), dma((2, 6)), dma((2,)), dma((2,)), dma((2,)),
            dma((7,)), dma((7,)), dma((7, 2)), dma((7, 2)), dma(()),
            pltpu.VMEM((2, 4, 2, w_rows, LANES), f32),
            pltpu.VMEM((share_rows, LANES), bf16),
            dma((2, 4, 2)), dma((3,)), dma((2, 2, w_steps)), dma(()), dma(()), dma((2, 2)),
            dma((2,)), dma((2, w_steps)), dma(()), dma(()),
        ],
        compiler_params=pltpu.CompilerParams(collective_id=0, has_side_effects=True, vmem_limit_bytes=60 * 2**20),
        name='reduce_update_gather',
    )(g, gv, p_mat, m_mat, s_mat, pv, mv, sv)


def update_kernel(coef, grad, master, moment, second, vec_new, vec_w, new_p, new_m, new_s, vec_p, vec_m, vec_s, w_vec,
                  rows):
    new_p[...], new_m[...], new_s[...] = adam_update(grad[...], coef[0:1, :], master[...], moment[...], second[...], DECAY)

    @pl.when(pl.program_id(0) == 0)
    def _():
        vec_p[...], vec_m[...], vec_s[...] = vec_new[0], vec_new[1], vec_new[2]
        n = vec_w.shape[1]
        for d in range(vec_w.shape[0]):
            rows[pl.ds(d * n, n), :] = vec_w[d]
        w_vec[...] = rows[...].astype(jnp.bfloat16)


def update_call(coef, grad, master, moment, second, vec_new, vec_w, block):
    n = grad.shape[0]
    own_rows = vec_new.shape[1]
    f32 = jnp.float32
    tile = pl.BlockSpec((block, LANES), lambda i: (i, 0))

    def whole(shape):
        return pl.BlockSpec(shape, lambda i: (0,) * len(shape))

    small = jax.ShapeDtypeStruct((own_rows, LANES), f32)
    return pl.pallas_call(
        update_kernel,
        grid=(n // block,),
        out_shape=(jax.ShapeDtypeStruct(grad.shape, f32),) * 3 + (small,) * 3 + (
            jax.ShapeDtypeStruct((8 * own_rows, LANES), jnp.bfloat16),),
        in_specs=[whole((8, LANES))] + [tile] * 4 + [whole(vec_new.shape), whole(vec_w.shape)],
        out_specs=(tile,) * 3 + (whole((own_rows, LANES)),) * 3 + (whole((8 * own_rows, LANES)),),
        scratch_shapes=[pltpu.VMEM((8 * own_rows, LANES), f32)],
        compiler_params=pltpu.CompilerParams(vmem_limit_bytes=40 * 2**20),
        cost_estimate=pl.CostEstimate(flops=n * LANES * 200, bytes_accessed=n * LANES * 28, transcendentals=0),
        name='update',
    )(coef, grad, master, moment, second, vec_new, vec_w)


def copy_kernel(moves, blocks, *refs):
    n_src = 1 + max(move[0] for move in moves(0))
    srcs, out, buf, in_sem, out_sem = refs[:n_src], refs[-4], refs[-3], refs[-2], refs[-1]
    me = lax.axis_index('fsdp')
    todo = []
    for which, src_row, dst_row, n in moves(me):
        size = n // blocks(n)
        for i in range(blocks(n)):
            todo.append((srcs[which], src_row + i * size, dst_row + i * size, size))
    slots = buf.shape[0]

    def take(k):
        src, src_row, _, size = todo[k]
        return pltpu.make_async_copy(src.at[pl.ds(pl.multiple_of(src_row, 16), size), :],
                                     buf.at[k % slots, pl.ds(0, size), :], in_sem.at[k % slots])

    def give(k):
        _, _, dst_row, size = todo[k]
        return pltpu.make_async_copy(buf.at[k % slots, pl.ds(0, size), :],
                                     out.at[pl.ds(pl.multiple_of(dst_row, 16), size), :], out_sem.at[k % slots])

    ahead = slots // 2
    for k in range(min(ahead, len(todo))):
        take(k).start()
    for k in range(len(todo)):
        take(k).wait()
        give(k).start()
        if k + ahead < len(todo):
            if k + ahead >= slots:
                give(k + ahead - slots).wait()
            take(k + ahead).start()
    for k in range(max(0, len(todo) - slots), len(todo)):
        give(k).wait()


def copy_call(moves, srcs, out_rows, into=None, slots=12, most=4160):
    def blocks(n):
        return next(d for d in range(1, n // 16 + 1) if (n // 16) % d == 0 and n // d <= most)

    hbm = pl.BlockSpec(memory_space=pltpu.HBM)
    args = list(srcs) + ([into] if into is not None else [])
    size = sum(move[3] for move in moves(0)) * LANES * 2
    return pl.pallas_call(
        functools.partial(copy_kernel, moves, blocks),
        out_shape=jax.ShapeDtypeStruct((out_rows, LANES), jnp.bfloat16),
        in_specs=[hbm] * len(args),
        out_specs=hbm,
        scratch_shapes=[pltpu.VMEM((slots, most, LANES), jnp.bfloat16),
                        pltpu.SemaphoreType.DMA((slots,)), pltpu.SemaphoreType.DMA((slots,))],
        input_output_aliases={len(srcs): 0} if into is not None else {},
        compiler_params=pltpu.CompilerParams(vmem_limit_bytes=32 * 2**20),
        cost_estimate=pl.CostEstimate(flops=size * 6, bytes_accessed=2 * size, transcendentals=0),
    )(*args)


def block_rows_of(n):
    return 16 * max(d for d in range(1, 190) if (n // 16) % d == 0)


STEPS = 28
W_STEPS = 26
W_LATE = (19, 6)
LAG = 3


def neighbours(me):
    core, x_pos, y_pos = lax.rem(me, 2), lax.rem(me // 2, 2), me // 4
    return me + 1 - 2 * core, me + 2 - 4 * x_pos, me + 4 - 8 * y_pos


def solution(mesh):
    hop_x = [(d, d ^ 2) for d in range(8)]
    hop_y = [(d, d ^ 4) for d in range(8)]
    hop_core = [(d, d ^ 1) for d in range(8)]

    def local_step(grad_mat, grad_vec, master_mat, moment_mat, second_mat, master_vec, moment_vec, second_vec):
        share = master_mat.shape[0]
        share_rows = share // LANES
        half_rows = share_rows // 2
        late, last = (n * (half_rows // W_STEPS) for n in W_LATE)
        early = half_rows - late - last
        own_rows = master_vec.shape[0] // LANES
        mats = [v.reshape(share_rows, LANES) for v in (master_mat, moment_mat, second_mat)]
        vecs = [v.reshape(own_rows, LANES) for v in (master_vec, moment_vec, second_vec)]
        total, gathered, late_a, late_b, last_a, last_b, _, _, _, _, coef, vec_new, vec_w = step_call(
            grad_mat, grad_vec, *mats, *vecs, share, STEPS, W_STEPS, W_LATE)

        late_x = lax.ppermute(late_b, 'fsdp', hop_x)
        late_y = lax.ppermute(late_a, 'fsdp', hop_y)
        last_x = lax.ppermute(last_b, 'fsdp', hop_x)
        last_y = lax.ppermute(last_a, 'fsdp', hop_y)

        def whole_moves(me):
            sib, x_dev, y_dev = neighbours(me)
            g_dev = x_dev + y_dev - me
            flip = sib - me
            return [(0, dev * share_rows, dev * share_rows, share_rows) for dev in (me, sib, g_dev, g_dev + flip)]

        def late_rows(x_dev, y_dev, first):
            return [(first, 0, x_dev * share_rows + half_rows + early, late),
                    (first + 1, 0, y_dev * share_rows + early, late)]

        def last_rows(x_dev, y_dev, first):
            return [(first, 0, x_dev * share_rows + half_rows + early + late, last),
                    (first + 1, 0, y_dev * share_rows + early + late, last)]

        def early_moves(me):
            sib, x_dev, y_dev = neighbours(me)
            flip = sib - me
            moves = []
            for dev in (x_dev, x_dev + flip):
                moves.append((0, dev * share_rows, dev * share_rows, half_rows + early))
            for dev in (y_dev, y_dev + flip):
                moves.append((0, dev * share_rows, dev * share_rows, early))
                moves.append((0, dev * share_rows + half_rows, dev * share_rows + half_rows, half_rows))
            return moves + late_rows(x_dev, y_dev, 1)

        def late_moves(me):
            sib, x_dev, y_dev = neighbours(me)
            flip = sib - me
            return last_rows(x_dev, y_dev, 0) + late_rows(x_dev + flip, y_dev + flip, 2)

        def last_moves(me):
            sib, x_dev, y_dev = neighbours(me)
            flip = sib - me
            return last_rows(x_dev + flip, y_dev + flip, 0)

        *new, weights_vec = update_call(coef, total, *mats, vec_new, vec_w, block_rows_of(share_rows))
        weights = copy_call(whole_moves, (gathered,), 8 * share_rows)
        late_x, late_y, weights, *new = lax.optimization_barrier((late_x, late_y, weights, *new))
        sib_late_x = lax.ppermute(late_x, 'fsdp', hop_core)
        sib_late_y = lax.ppermute(late_y, 'fsdp', hop_core)
        weights = copy_call(early_moves, (gathered, late_x, late_y), 8 * share_rows, into=weights)
        last_x, last_y, weights = lax.optimization_barrier((last_x, last_y, weights))
        sib_last_x = lax.ppermute(last_x, 'fsdp', hop_core)
        sib_last_y = lax.ppermute(last_y, 'fsdp', hop_core)
        weights = copy_call(late_moves, (last_x, last_y, sib_late_x, sib_late_y), 8 * share_rows,
                            into=weights)
        weights = copy_call(last_moves, (sib_last_x, sib_last_y), 8 * share_rows, into=weights)
        return tuple(v.reshape(-1) for v in (*new, weights, weights_vec))

    row_spec = P('fsdp', None)
    flat_spec = P('fsdp')
    whole_spec = P()
    return jax.shard_map(local_step, mesh=mesh,
                         in_specs=(row_spec, row_spec) + (flat_spec,) * 6,
                         out_specs=(flat_spec,) * 6 + (whole_spec, whole_spec),
                         check_vma=False)
```

```python
import functools

import jax
import jax.numpy as jnp
from jax import lax
from jax.experimental import pallas as pl
from jax.experimental.pallas import tpu as pltpu
from jax.sharding import PartitionSpec as P


STEP = 4
LEARN_RATE = 1e-3
BETA_ONE = 0.9
BETA_TWO = 0.999
ADAM_EPS = 1e-8
DECAY = 0.01
NORM_EPS = 1e-6
FIX_ONE = 1.0 - BETA_ONE ** STEP
FIX_TWO = 1.0 - BETA_TWO ** STEP

MESH = pl.DeviceIdType.MESH
LANES = 128
TILE = 1024


def adam_update(grad_sum, clip_coef, master, moment, second, decay):
    clip_grad = clip_coef * grad_sum
    new_moment = BETA_ONE * moment + (1.0 - BETA_ONE) * clip_grad
    new_second = BETA_TWO * second + (1.0 - BETA_TWO) * clip_grad * clip_grad
    step_dir = (new_moment * (LEARN_RATE / FIX_ONE)) / (jnp.sqrt(new_second * (1.0 / FIX_TWO)) + ADAM_EPS)
    new_master = master - (step_dir + (LEARN_RATE * decay) * master)
    return new_master, new_moment, new_second


def block_len(n, most):
    tiles = n // TILE
    return max(d for d in range(1, most // TILE + 1) if tiles % d == 0) * TILE


PIECES = {'diag': (0, 2), 'x_b': (2, 1), 'y_a': (3, 1), 'x_a': (4, 1), 'y_b': (5, 1), 'mine': (6, 2)}


def step_kernel(share, half, steps, w_steps, w_late, g, gv, p_mat, m_mat, s_mat, pv, mv, sv,
                total, gathered, late_a, late_b, last_a, last_b, sib_land, leaf_land, four_land, direct_land, coef_out, vec_new, vec_w,
                raw_own, raw_sib, leaf_st, direct_st, four_st, leaf_in, fin_in, out_st, acc, sq_land, vec_land,
                  sib_send, sib_recv, leaf_send, leaf_recv, four_send, four_recv, direct_send, direct_recv,
                  own_sem, sibin_sem, leafin_sem, fin_sem, out_sem, sq_send, sq_recv, vec_send, vec_recv, local_sem,
                state_in, own_w, state_sem, own_send, own_recv, own_sib_recv, keep_sem, late_sem,
                fwd_send, fwd_recv, fsib_send, fsib_recv, first_send, first_recv, vec_sum):
    me = lax.axis_index('fsdp')
    core = lax.rem(me, 2)
    x_pos = lax.rem(me // 2, 2)
    y_pos = me // 4
    sib = me + 1 - 2 * core
    x_dev = me + 2 - 4 * x_pos
    y_dev = me + 4 - 8 * y_pos
    g_dev = y_dev + 2 - 4 * x_pos
    sib_delta = 1 - 2 * core
    dests = (g_dev, x_dev, y_dev, me)
    rows = half // LANES
    n_dev = 8

    def sib_copy(j, t):
        src = pl.multiple_of((dests[j] + sib_delta) * share + t * 2 * half, TILE)
        dst = pl.multiple_of(j * share + t * 2 * half, TILE)
        return pltpu.make_async_remote_copy(
            src_ref=g.at[:, pl.ds(src, 2 * half)], dst_ref=sib_land.at[:, pl.ds(dst, 2 * half)],
            send_sem=sib_send, recv_sem=sib_recv.at[j, t], device_id=(sib,), device_id_type=MESH)

    def first_copy(part):
        src = pl.multiple_of((g_dev + sib_delta) * share + part * half, TILE)
        return pltpu.make_async_remote_copy(
            src_ref=g.at[:, pl.ds(src, half)], dst_ref=raw_sib.at[0, :, pl.ds(part * half, half)],
            send_sem=first_send.at[part], recv_sem=first_recv.at[part], device_id=(sib,), device_id_type=MESH)

    def raw_copy(piece, t, slot, which):
        place, width = PIECES[piece]
        j = {'diag': 0, 'x_b': 1, 'x_a': 1, 'y_a': 2, 'y_b': 2, 'mine': 3}[piece]
        skip = half if piece in ('x_b', 'y_b') else 0
        n = width * half
        here = pl.ds(place * half, n)
        index = list(PIECES).index(piece)
        src = pl.multiple_of(dests[j] * share + t * 2 * half + skip, TILE)
        land = pl.multiple_of(j * share + t * 2 * half + skip, TILE)
        if which == 0:
            return pltpu.make_async_copy(g.at[:, pl.ds(src, n)], raw_own.at[slot, :, here], own_sem.at[slot, index])
        return pltpu.make_async_copy(sib_land.at[:, pl.ds(land, n)], raw_sib.at[slot, :, here],
                                     sibin_sem.at[slot, index])

    def land_rows(t, part):
        return pl.ds(pl.multiple_of(t * 2 * rows + part * rows, 8), rows)

    def remote(stage, slot, part, land, t, send, recv, target):
        return pltpu.make_async_remote_copy(
            src_ref=stage.at[slot, pl.ds(part * rows, rows), :], dst_ref=land.at[land_rows(t, part), :],
            send_sem=send.at[slot, part], recv_sem=recv.at[part, t], device_id=(target,), device_id_type=MESH)

    def leaf_copy(t, slot, part):
        return remote(leaf_st, slot, part, leaf_land, t, leaf_send, leaf_recv, (y_dev, x_dev)[part])

    def direct_copy(t, slot, part):
        return remote(direct_st, slot, part, direct_land, t, direct_send, direct_recv, (y_dev, x_dev)[part])

    def four_copy(t, slot, part):
        return remote(four_st, slot, part, four_land, t, four_send, four_recv, (x_dev, y_dev)[part])

    def leaf_load(t, part):
        return pltpu.make_async_copy(leaf_land.at[land_rows(t, part), :], leaf_in.at[pl.ds(part * rows, rows), :],
                                     leafin_sem.at[part])

    def fin_load(which, t, part):
        return pltpu.make_async_copy((four_land, direct_land)[which].at[land_rows(t, part), :],
                                     fin_in.at[which, pl.ds(part * rows, rows), :], fin_sem.at[which, part])

    def out_copy(t, slot):
        both = pl.ds(pl.multiple_of(t * 2 * rows, 8), 2 * rows)
        return pltpu.make_async_copy(out_st.at[slot], total.at[both, :], out_sem.at[slot])

    blk = block_len(half, 16 * TILE)
    blk_rows = blk // LANES

    def pair(slot, place, i):
        at = pl.ds(pl.multiple_of(place * half + i * blk, TILE), blk)
        own = raw_own[slot, :, at].astype(jnp.float32).reshape(blk_rows, LANES)
        other = raw_sib[slot, :, at].astype(jnp.float32).reshape(blk_rows, LANES)
        return own + other

    def block_rows(i, part=0):
        return pl.ds(pl.multiple_of(part * rows + i * blk_rows, 8), blk_rows)

    def store_pair(slot, place, stage, part):
        @pl.loop(0, half // blk)
        def _(i):
            stage[slot, block_rows(i, part), :] = pair(slot, place, i)

    def wait_raw(piece, t, slot):
        for which in range(2):
            raw_copy(piece, t, slot, which).wait()

    own_rows = pv.shape[0]

    def row_part(dev):
        return gv.at[:, pl.ds(pl.multiple_of(dev * own_rows * LANES, LANES), own_rows * LANES)]

    def row_copy(k):
        target = lax.rem(me + k, n_dev)
        return pltpu.make_async_remote_copy(
            src_ref=row_part(target), dst_ref=vec_land.at[me], send_sem=vec_send.at[k - 1, 0],
            recv_sem=vec_recv.at[k - 1, 0], device_id=(target,), device_id_type=MESH)

    def new_copy(k):
        return pltpu.make_async_remote_copy(
            src_ref=vec_new.at[0], dst_ref=vec_w.at[me], send_sem=vec_send.at[k - 1, 1], recv_sem=vec_recv.at[k - 1, 1],
            device_id=(lax.rem(me + k, n_dev),), device_id_type=MESH)

    def send_sib(t):
        @pl.when(jnp.logical_and(t >= 1, t < steps))
        def _():
            sib_copy(0, t).start()

        @pl.when(t < steps)
        def _():
            for j in range(1, 3):
                sib_copy(j, t).start()

        @pl.when(t >= 1)
        def _():
            sib_copy(3, t - 1).start()

    def fetch(t, which):
        slot = lax.rem(t, 2)

        @pl.when(jnp.logical_and(t >= which, t < steps))
        def _():
            if which == 1:
                sib_copy(0, t).wait_recv()
            raw_copy('diag', t, slot, which).start()

        @pl.when(t < steps)
        def _():
            for j, piece in ((1, 'x_b'), (2, 'y_a')):
                if which == 1:
                    sib_copy(j, t).wait_recv()
                raw_copy(piece, t, slot, which).start()

        @pl.when(jnp.logical_and(t >= 1, t <= steps))
        def _():
            for piece in ('x_a', 'y_b'):
                raw_copy(piece, t - 1, slot, which).start()

        @pl.when(jnp.logical_and(t >= 2, t <= steps + 1))
        def _():
            if which == 1:
                sib_copy(3, t - 2).wait_recv()
            raw_copy('mine', t - 2, slot, which).start()

    barrier = pltpu.get_barrier_semaphore()
    for k in range(1, n_dev):
        pl.semaphore_signal(barrier, inc=1, device_id=(lax.rem(me + k, n_dev),), device_id_type=MESH)
    fetch(jnp.int32(0), 0)
    pl.semaphore_wait(barrier, n_dev - 1)
    for part in range(2):
        first_copy(part).start()
    send_sib(jnp.int32(0))
    acc[...] = jnp.zeros_like(acc)
    send_sib(jnp.int32(1))

    @pl.loop(0, steps + 2)
    def _(t):
        slot = lax.rem(t, 2)
        before = 1 - slot

        @pl.when(t + 2 <= steps)
        def _():
            send_sib(t + 2)

        fetch(t + 1, 0)

        @pl.when(t < steps)
        def _():
            raw_copy('diag', t, slot, 0).wait()

            @pl.when(t >= 1)
            def _():
                raw_copy('diag', t, slot, 1).wait()

            for part in range(2):
                @pl.when(t == 0)
                def _():
                    first_copy(part).wait_recv()

                @pl.when(t >= 2)
                def _():
                    leaf_copy(t - 2, slot, part).wait_send()

                store_pair(slot, part, leaf_st, part)
                leaf_copy(t, slot, part).start()

            @pl.when(t == 0)
            def _():
                fetch(t, 1)

            for part, piece, place in ((1, 'x_b', 2), (0, 'y_a', 3)):
                wait_raw(piece, t, slot)

                @pl.when(t >= 2)
                def _():
                    direct_copy(t - 2, slot, part).wait_send()

                store_pair(slot, place, direct_st, part)
                direct_copy(t, slot, part).start()

        fetch(t + 1, 1)

        @pl.when(t == 0)
        def _():
            for k in range(1, n_dev):
                row_copy(k).start()
            pltpu.make_async_copy(row_part(me), vec_land.at[me], local_sem).start()

        @pl.when(t == 3)
        def _():
            for k in range(1, n_dev):
                row_copy(k).wait()
            pltpu.make_async_copy(row_part(me), vec_land.at[me], local_sem).wait()
            part_sum = vec_land[0].astype(jnp.float32)
            for d in range(1, n_dev):
                part_sum += vec_land[d].astype(jnp.float32)
            part_sum = part_sum.reshape(own_rows, LANES)
            vec_sum[...] = part_sum
            acc[0:own_rows, :] += part_sum * part_sum

        @pl.when(jnp.logical_and(t >= 1, t <= steps))
        def _():
            for part in range(2):
                leaf_copy(t - 1, before, part).wait_recv()
                leaf_load(t - 1, part).start()
            for part, piece, place in ((0, 'x_a', 4), (1, 'y_b', 5)):
                wait_raw(piece, t - 1, slot)

                @pl.when(t >= 3)
                def _():
                    four_copy(t - 3, before, part).wait_send()

                leaf_load(t - 1, part).wait()

                @pl.loop(0, half // blk)
                def _(i):
                    at = block_rows(i, part)
                    four_st[before, at, :] = leaf_in[at, :] + pair(slot, place, i)

                four_copy(t - 1, before, part).start()

        @pl.when(t >= 2)
        def _():
            for part in range(2):
                direct_copy(t - 2, slot, part).wait_recv()
                fin_load(1, t - 2, part).start()
            wait_raw('mine', t - 2, slot)

            @pl.when(t >= 4)
            def _():
                out_copy(t - 4, slot).wait()

            for part in range(2):
                four_copy(t - 2, slot, part).wait_recv()
                fin_load(0, t - 2, part).start()
                fin_load(1, t - 2, part).wait()
                fin_load(0, t - 2, part).wait()

                @pl.loop(0, half // blk)
                def _(i):
                    at = block_rows(i, part)
                    whole = (fin_in[0, at, :] + fin_in[1, at, :]) + pair(slot, 6 + part, i)
                    out_st[slot, at, :] = whole
                    acc[...] += jnp.sum((whole * whole).reshape(blk_rows // 8, 8, LANES), axis=0)
            out_copy(t - 2, slot).start()

    def square_copy(k):
        target = lax.rem(me + k, n_dev)
        return pltpu.make_async_remote_copy(
            src_ref=acc, dst_ref=sq_land.at[me], send_sem=sq_send.at[k - 1], recv_sem=sq_recv.at[k - 1],
            device_id=(target,), device_id_type=MESH)

    for k in range(1, n_dev):
        square_copy(k).start()
    sq_land[me] = acc[...]
    for t in (steps - 2, steps - 1):
        out_copy(t, t % 2).wait()
    share_rows = share // LANES
    half_rows = share_rows // 2
    w_rows = half_rows // w_steps

    def inside(part, t, n=1):
        return pl.ds(pl.multiple_of(part * half_rows + t * w_rows, 16), n * w_rows)

    def place(dev, part, t):
        return pl.ds(pl.multiple_of(dev * share_rows + part * half_rows + t * w_rows, 16), w_rows)

    def state_copies(t, slot):
        return [pltpu.make_async_copy(src.at[inside(part, t), :], state_in.at[slot, i, part], state_sem.at[slot, i, part])
                for i, src in enumerate((total, p_mat, m_mat, s_mat)) for part in range(2)]

    def own_copy(to, part, t):
        target = (x_dev, y_dev, sib)[to]
        recv = own_sib_recv if to == 2 else own_recv.at[to, part, t]
        return pltpu.make_async_remote_copy(
            src_ref=own_w.at[inside(part, t), :], dst_ref=gathered.at[place(me, part, t), :],
            send_sem=own_send.at[to], recv_sem=recv, device_id=(target,), device_id_type=MESH)

    def keep_copy(part, t):
        return pltpu.make_async_copy(own_w.at[inside(part, t), :], gathered.at[place(me, part, t), :], keep_sem)

    def late_copy(group, part):
        start = w_steps - sum(w_late[group:])
        return pltpu.make_async_copy(own_w.at[inside(part, start, w_late[group]), :],
                                     ((late_a, late_b), (last_a, last_b))[group][part], late_sem.at[group, part])

    def forward(part, t):
        rows_at = place((x_dev, y_dev)[part], part, t)
        return pltpu.make_async_remote_copy(
            src_ref=gathered.at[rows_at, :], dst_ref=gathered.at[rows_at, :],
            send_sem=fwd_send.at[part], recv_sem=fwd_recv.at[part, t],
            device_id=((y_dev, x_dev)[part],), device_id_type=MESH)

    def to_sib(dev, part, t):
        rows_at = place(dev, part, t)
        return pltpu.make_async_remote_copy(
            src_ref=gathered.at[rows_at, :], dst_ref=gathered.at[rows_at, :],
            send_sem=fsib_send, recv_sem=fsib_recv, device_id=(sib,), device_id_type=MESH)

    def all_rows(n, send, recv):
        return pltpu.make_async_remote_copy(
            src_ref=gathered.at[pl.ds(0, n * w_rows), :], dst_ref=gathered.at[pl.ds(0, n * w_rows), :],
            send_sem=send, recv_sem=recv, device_id=(sib,), device_id_type=MESH)

    for copy in state_copies(0, 0):
        copy.start()

    square = jnp.zeros_like(acc)
    for k in range(1, n_dev):
        square_copy(k).wait()
    for d in range(n_dev):
        square += sq_land[d]
    norm = jnp.sqrt(jnp.sum(jnp.sum(square, axis=0, keepdims=True), axis=1, keepdims=True))
    coef = jnp.minimum(1.0, 1.0 / (norm + NORM_EPS))
    coef_out[...] = jnp.broadcast_to(coef, coef_out.shape)

    w_tiles = w_rows // 16
    w_blk = 16 * max(d for d in range(1, 9) if w_tiles % d == 0)

    def update(slot, part, t):
        @pl.loop(0, w_rows // w_blk)
        def _(i):
            at = pl.ds(pl.multiple_of(i * w_blk, 16), w_blk)
            grad, master, moment, second = (state_in[slot, k, part, at, :] for k in range(4))
            new = adam_update(grad, coef_out[0:1, :], master, moment, second, DECAY)[0]
            out = pl.ds(pl.multiple_of(part * half_rows + t * w_rows + i * w_blk, 16), w_blk)
            own_w[out, :] = new.astype(jnp.bfloat16)

    early = w_steps - sum(w_late)

    @pl.loop(0, w_steps + LAG + 2)
    def _(u):
        slot = lax.rem(u, 2)

        @pl.when(u + 1 < w_steps)
        def _():
            for copy in state_copies(u + 1, 1 - slot):
                copy.start()

        @pl.when(u < w_steps)
        def _():
            for copy in state_copies(u, slot):
                copy.wait()
            for part in range(2):
                update(slot, part, u)
                own_copy(part, part, u).start()

                @pl.when(u < early)
                def _():
                    own_copy(1 - part, part, u).start()

                own_copy(2, part, u).start()
                keep_copy(part, u).start()

        @pl.when(jnp.logical_and(u >= LAG, u < w_steps + LAG))
        def _():
            t = u - LAG
            for part in range(2):
                own_copy(part, part, t).wait_recv()
                forward(part, t).start()
                to_sib((x_dev, y_dev)[part], part, t).start()

            @pl.when(t < early)
            def _():
                for part in range(2):
                    own_copy(1 - part, part, t).wait_recv()
                    to_sib((y_dev, x_dev)[part], part, t).start()

        @pl.when(u >= LAG + 2)
        def _():
            t = u - LAG - 2
            for part in range(2):
                forward(part, t).wait_recv()
                to_sib(g_dev, part, t).start()

        @pl.when(u == 1)
        def _():
            new = adam_update(vec_sum[...], coef_out[0:1, :], pv[...], mv[...], sv[...], 0.0)
            for i in range(3):
                vec_new[i] = new[i]
            vec_w[me] = new[0]
            for k in range(1, n_dev):
                new_copy(k).start()

        @pl.when(u == w_steps - 1)
        def _():
            for group in range(2):
                for part in range(2):
                    late_copy(group, part).start()

    for k in range(1, n_dev):
        new_copy(k).wait()

    for t in (steps - 2, steps - 1):
        slot = t % 2
        for part in range(2):
            leaf_copy(t, slot, part).wait_send()
            direct_copy(t, slot, part).wait_send()
            four_copy(t, slot, part).wait_send()
    pltpu.make_async_remote_copy(
        src_ref=g.at[:, pl.ds(0, 4 * share - 2 * half)], dst_ref=sib_land.at[:, pl.ds(0, 4 * share - 2 * half)],
        send_sem=sib_send, recv_sem=sib_recv.at[0, 0], device_id=(sib,), device_id_type=MESH).wait_send()
    for part in range(2):
        first_copy(part).wait_send()
    for part in range(2):
        late_copy(0, part).wait()
        late_copy(1, part).wait()
        all_rows(w_steps + early, own_send.at[part], fsib_recv).wait_send()
        all_rows(w_steps, fwd_send.at[part], fsib_recv).wait_send()
    all_rows(2 * w_steps, own_send.at[2], own_sib_recv).wait()
    all_rows(4 * w_steps + 2 * early, fsib_send, fsib_recv).wait()
    pltpu.make_async_copy(own_w, gathered.at[pl.ds(0, share_rows), :], keep_sem).wait()


def step_call(g, gv, p_mat, m_mat, s_mat, pv, mv, sv, share, steps, w_steps, w_late):
    half = share // (2 * steps)
    rows = half // LANES
    share_rows = share // LANES
    w_rows = share_rows // (2 * w_steps)
    dma = pltpu.SemaphoreType.DMA
    f32, bf16 = jnp.float32, jnp.bfloat16
    own_rows = pv.shape[0]
    hbm = pl.BlockSpec(memory_space=pltpu.HBM)
    vmem = pl.BlockSpec(memory_space=pltpu.VMEM)
    return pl.pallas_call(
        functools.partial(step_kernel, share, half, steps, w_steps, w_late),
        out_shape=(jax.ShapeDtypeStruct((share_rows, LANES), f32),
                   jax.ShapeDtypeStruct((8 * share_rows, LANES), bf16),
                   jax.ShapeDtypeStruct((w_late[0] * w_rows, LANES), bf16),
                   jax.ShapeDtypeStruct((w_late[0] * w_rows, LANES), bf16),
                   jax.ShapeDtypeStruct((w_late[1] * w_rows, LANES), bf16),
                   jax.ShapeDtypeStruct((w_late[1] * w_rows, LANES), bf16),
                   jax.ShapeDtypeStruct((1, 4 * share), bf16),
                   jax.ShapeDtypeStruct((share_rows, LANES), f32),
                   jax.ShapeDtypeStruct((share_rows, LANES), f32),
                   jax.ShapeDtypeStruct((share_rows, LANES), f32),
                   jax.ShapeDtypeStruct((8, LANES), f32),
                   jax.ShapeDtypeStruct((3, own_rows, LANES), f32),
                   jax.ShapeDtypeStruct((8, own_rows, LANES), f32)),
        in_specs=[hbm, vmem, hbm, hbm, hbm, vmem, vmem, vmem],
        out_specs=(hbm,) * 10 + (vmem,) * 3,
        scratch_shapes=[
            pltpu.VMEM((2, 1, 8 * half), bf16),
            pltpu.VMEM((2, 1, 8 * half), bf16),
            pltpu.VMEM((2, 2 * rows, LANES), f32),
            pltpu.VMEM((2, 2 * rows, LANES), f32),
            pltpu.VMEM((2, 2 * rows, LANES), f32),
            pltpu.VMEM((2 * rows, LANES), f32),
            pltpu.VMEM((2, 2 * rows, LANES), f32),
            pltpu.VMEM((2, 2 * rows, LANES), f32),
            pltpu.VMEM((8, LANES), f32),
            pltpu.VMEM((8, 8, LANES), f32),
            pltpu.VMEM((8, 1, own_rows * LANES), bf16),
            dma(()), dma((4, steps)),
            dma((2, 2)), dma((2, steps)), dma((2, 2)), dma((2, steps)), dma((2, 2)), dma((2, steps)),
            dma((2, 6)), dma((2, 6)), dma((2,)), dma((2, 2)), dma((2,)),
            dma((7,)), dma((7,)), dma((7, 2)), dma((7, 2)), dma(()),
            pltpu.VMEM((2, 4, 2, w_rows, LANES), f32),
            pltpu.VMEM((share_rows, LANES), bf16),
            dma((2, 4, 2)), dma((3,)), dma((2, 2, w_steps)), dma(()), dma(()), dma((2, 2)),
            dma((2,)), dma((2, w_steps)), dma(()), dma(()), dma((2,)), dma((2,)),
            pltpu.VMEM((own_rows, LANES), f32),
        ],
        compiler_params=pltpu.CompilerParams(collective_id=0, has_side_effects=True, vmem_limit_bytes=60 * 2**20),
        name='reduce_update_gather',
    )(g, gv, p_mat, m_mat, s_mat, pv, mv, sv)


def update_kernel(coef, grad, master, moment, second, vec_new, vec_w, new_p, new_m, new_s, vec_p, vec_m, vec_s, w_vec,
                  rows):
    new_p[...], new_m[...], new_s[...] = adam_update(grad[...], coef[0:1, :], master[...], moment[...], second[...], DECAY)

    @pl.when(pl.program_id(0) == 0)
    def _():
        vec_p[...], vec_m[...], vec_s[...] = vec_new[0], vec_new[1], vec_new[2]
        n = vec_w.shape[1]
        for d in range(vec_w.shape[0]):
            rows[pl.ds(d * n, n), :] = vec_w[d]
        w_vec[...] = rows[...].astype(jnp.bfloat16)


def update_call(coef, grad, master, moment, second, vec_new, vec_w, block):
    n = grad.shape[0]
    own_rows = vec_new.shape[1]
    f32 = jnp.float32
    tile = pl.BlockSpec((block, LANES), lambda i: (i, 0))

    def whole(shape):
        return pl.BlockSpec(shape, lambda i: (0,) * len(shape))

    small = jax.ShapeDtypeStruct((own_rows, LANES), f32)
    return pl.pallas_call(
        update_kernel,
        grid=(n // block,),
        out_shape=(jax.ShapeDtypeStruct(grad.shape, f32),) * 3 + (small,) * 3 + (
            jax.ShapeDtypeStruct((8 * own_rows, LANES), jnp.bfloat16),),
        in_specs=[whole((8, LANES))] + [tile] * 4 + [whole(vec_new.shape), whole(vec_w.shape)],
        out_specs=(tile,) * 3 + (whole((own_rows, LANES)),) * 3 + (whole((8 * own_rows, LANES)),),
        scratch_shapes=[pltpu.VMEM((8 * own_rows, LANES), f32)],
        compiler_params=pltpu.CompilerParams(vmem_limit_bytes=40 * 2**20),
        cost_estimate=pl.CostEstimate(flops=n * LANES * 200, bytes_accessed=n * LANES * 28, transcendentals=0),
        name='update',
    )(coef, grad, master, moment, second, vec_new, vec_w)


def copy_kernel(moves, blocks, *refs):
    n_src = 1 + max(move[0] for move in moves(0))
    srcs, out, buf, in_sem, out_sem = refs[:n_src], refs[-4], refs[-3], refs[-2], refs[-1]
    me = lax.axis_index('fsdp')
    todo = []
    for which, src_row, dst_row, n in moves(me):
        size = n // blocks(n)
        for i in range(blocks(n)):
            todo.append((srcs[which], src_row + i * size, dst_row + i * size, size))
    slots = buf.shape[0]

    def take(k):
        src, src_row, _, size = todo[k]
        return pltpu.make_async_copy(src.at[pl.ds(pl.multiple_of(src_row, 16), size), :],
                                     buf.at[k % slots, pl.ds(0, size), :], in_sem.at[k % slots])

    def give(k):
        _, _, dst_row, size = todo[k]
        return pltpu.make_async_copy(buf.at[k % slots, pl.ds(0, size), :],
                                     out.at[pl.ds(pl.multiple_of(dst_row, 16), size), :], out_sem.at[k % slots])

    ahead = slots // 2
    for k in range(min(ahead, len(todo))):
        take(k).start()
    for k in range(len(todo)):
        take(k).wait()
        give(k).start()
        if k + ahead < len(todo):
            if k + ahead >= slots:
                give(k + ahead - slots).wait()
            take(k + ahead).start()
    for k in range(max(0, len(todo) - slots), len(todo)):
        give(k).wait()


def copy_call(moves, srcs, out_rows, into=None, slots=12, most=4160):
    def blocks(n):
        return next(d for d in range(1, n // 16 + 1) if (n // 16) % d == 0 and n // d <= most)

    hbm = pl.BlockSpec(memory_space=pltpu.HBM)
    args = list(srcs) + ([into] if into is not None else [])
    size = sum(move[3] for move in moves(0)) * LANES * 2
    return pl.pallas_call(
        functools.partial(copy_kernel, moves, blocks),
        out_shape=jax.ShapeDtypeStruct((out_rows, LANES), jnp.bfloat16),
        in_specs=[hbm] * len(args),
        out_specs=hbm,
        scratch_shapes=[pltpu.VMEM((slots, most, LANES), jnp.bfloat16),
                        pltpu.SemaphoreType.DMA((slots,)), pltpu.SemaphoreType.DMA((slots,))],
        input_output_aliases={len(srcs): 0} if into is not None else {},
        compiler_params=pltpu.CompilerParams(vmem_limit_bytes=32 * 2**20),
        cost_estimate=pl.CostEstimate(flops=size * 6, bytes_accessed=2 * size, transcendentals=0),
    )(*args)


def block_rows_of(n):
    return 16 * max(d for d in range(1, 190) if (n // 16) % d == 0)


STEPS = 28
W_STEPS = 26
W_LATE = (19, 6)
LAG = 3


def neighbours(me):
    core, x_pos, y_pos = lax.rem(me, 2), lax.rem(me // 2, 2), me // 4
    return me + 1 - 2 * core, me + 2 - 4 * x_pos, me + 4 - 8 * y_pos


def solution(mesh):
    hop_x = [(d, d ^ 2) for d in range(8)]
    hop_y = [(d, d ^ 4) for d in range(8)]
    hop_core = [(d, d ^ 1) for d in range(8)]

    def local_step(grad_mat, grad_vec, master_mat, moment_mat, second_mat, master_vec, moment_vec, second_vec):
        share = master_mat.shape[0]
        share_rows = share // LANES
        half_rows = share_rows // 2
        late, last = (n * (half_rows // W_STEPS) for n in W_LATE)
        early = half_rows - late - last
        own_rows = master_vec.shape[0] // LANES
        mats = [v.reshape(share_rows, LANES) for v in (master_mat, moment_mat, second_mat)]
        vecs = [v.reshape(own_rows, LANES) for v in (master_vec, moment_vec, second_vec)]
        total, gathered, late_a, late_b, last_a, last_b, _, _, _, _, coef, vec_new, vec_w = step_call(
            grad_mat, grad_vec, *mats, *vecs, share, STEPS, W_STEPS, W_LATE)

        late_x = lax.ppermute(late_b, 'fsdp', hop_x)
        late_y = lax.ppermute(late_a, 'fsdp', hop_y)
        last_x = lax.ppermute(last_b, 'fsdp', hop_x)
        last_y = lax.ppermute(last_a, 'fsdp', hop_y)

        def whole_moves(me):
            sib, x_dev, y_dev = neighbours(me)
            g_dev = x_dev + y_dev - me
            flip = sib - me
            return [(0, dev * share_rows, dev * share_rows, share_rows) for dev in (me, sib, g_dev, g_dev + flip)] + [
                (0, x_dev * share_rows, x_dev * share_rows, half_rows)]

        def late_rows(x_dev, y_dev, first):
            return [(first, 0, x_dev * share_rows + half_rows + early, late),
                    (first + 1, 0, y_dev * share_rows + early, late)]

        def last_rows(x_dev, y_dev, first):
            return [(first, 0, x_dev * share_rows + half_rows + early + late, last),
                    (first + 1, 0, y_dev * share_rows + early + late, last)]

        def early_moves(me):
            sib, x_dev, y_dev = neighbours(me)
            flip = sib - me
            moves = [(0, (x_dev + flip) * share_rows, (x_dev + flip) * share_rows, half_rows)]
            for dev in (x_dev, x_dev + flip):
                start = dev * share_rows + half_rows
                moves.append((0, start, start, early))
            for dev in (y_dev, y_dev + flip):
                start = dev * share_rows
                moves.append((0, start, start, early))
                moves.append((0, start + half_rows, start + half_rows, half_rows))
            return moves + late_rows(x_dev, y_dev, 1)

        def mid_moves(me):
            sib, x_dev, y_dev = neighbours(me)
            return late_rows(x_dev + sib - me, y_dev + sib - me, 0)

        def late_moves(me):
            _, x_dev, y_dev = neighbours(me)
            return last_rows(x_dev, y_dev, 0)

        def last_moves(me):
            sib, x_dev, y_dev = neighbours(me)
            flip = sib - me
            return last_rows(x_dev + flip, y_dev + flip, 0)

        *new, weights_vec = update_call(coef, total, *mats, vec_new, vec_w, block_rows_of(share_rows))
        weights = copy_call(whole_moves, (gathered,), 8 * share_rows)
        late_x, late_y, weights, *new = lax.optimization_barrier((late_x, late_y, weights, *new))
        sib_late_x = lax.ppermute(late_x, 'fsdp', hop_core)
        sib_late_y = lax.ppermute(late_y, 'fsdp', hop_core)
        weights = copy_call(early_moves, (gathered, late_x, late_y), 8 * share_rows, into=weights)
        weights = copy_call(mid_moves, (sib_late_x, sib_late_y), 8 * share_rows, into=weights)
        last_x, last_y, weights = lax.optimization_barrier((last_x, last_y, weights))
        sib_last_x = lax.ppermute(last_x, 'fsdp', hop_core)
        sib_last_y = lax.ppermute(last_y, 'fsdp', hop_core)
        weights = copy_call(late_moves, (last_x, last_y), 8 * share_rows, into=weights)
        weights = copy_call(last_moves, (sib_last_x, sib_last_y), 8 * share_rows, into=weights)
        return tuple(v.reshape(-1) for v in (*new, weights, weights_vec))

    row_spec = P('fsdp', None)
    flat_spec = P('fsdp')
    whole_spec = P()
    return jax.shard_map(local_step, mesh=mesh,
                         in_specs=(row_spec, row_spec) + (flat_spec,) * 6,
                         out_specs=(flat_spec,) * 6 + (whole_spec, whole_spec),
                         check_vma=False)
```

```python
import functools

import jax
import jax.numpy as jnp
from jax import lax
from jax.experimental import pallas as pl
from jax.experimental.pallas import tpu as pltpu
from jax.sharding import PartitionSpec as P


STEP = 4
LEARN_RATE = 1e-3
BETA_ONE = 0.9
BETA_TWO = 0.999
ADAM_EPS = 1e-8
DECAY = 0.01
NORM_EPS = 1e-6
FIX_ONE = 1.0 - BETA_ONE ** STEP
FIX_TWO = 1.0 - BETA_TWO ** STEP

MESH = pl.DeviceIdType.MESH
LANES = 128
TILE = 1024


def adam_update(grad_sum, clip_coef, master, moment, second, decay):
    clip_grad = clip_coef * grad_sum
    new_moment = BETA_ONE * moment + (1.0 - BETA_ONE) * clip_grad
    new_second = BETA_TWO * second + (1.0 - BETA_TWO) * clip_grad * clip_grad
    step_dir = (new_moment * (LEARN_RATE / FIX_ONE)) / (jnp.sqrt(new_second * (1.0 / FIX_TWO)) + ADAM_EPS)
    new_master = master - (step_dir + (LEARN_RATE * decay) * master)
    return new_master, new_moment, new_second


def block_len(n, most):
    tiles = n // TILE
    return max(d for d in range(1, most // TILE + 1) if tiles % d == 0) * TILE


PIECES = {'diag': (0, 2), 'x_b': (2, 1), 'y_a': (3, 1), 'x_a': (4, 1), 'y_b': (5, 1), 'mine': (6, 2)}


def step_kernel(share, half, steps, w_steps, w_late, g, gv, p_mat, m_mat, s_mat, pv, mv, sv,
                total, gathered, late_a, late_b, last_a, last_b, sib_land, leaf_land, four_land, direct_land, coef_out, vec_new, vec_w,
                raw_own, raw_sib, leaf_st, direct_st, four_st, leaf_in, fin_in, out_st, acc, sq_land, vec_land,
                  sib_send, sib_recv, leaf_send, leaf_recv, four_send, four_recv, direct_send, direct_recv,
                  own_sem, sibin_sem, leafin_sem, fin_sem, out_sem, sq_send, sq_recv, vec_send, vec_recv, local_sem,
                state_in, own_w, state_sem, own_send, own_recv, own_sib_recv, keep_sem, late_sem,
                fwd_send, fwd_recv, fsib_send, fsib_recv, first_send, first_recv, vec_sum):
    me = lax.axis_index('fsdp')
    core = lax.rem(me, 2)
    x_pos = lax.rem(me // 2, 2)
    y_pos = me // 4
    sib = me + 1 - 2 * core
    x_dev = me + 2 - 4 * x_pos
    y_dev = me + 4 - 8 * y_pos
    g_dev = y_dev + 2 - 4 * x_pos
    sib_delta = 1 - 2 * core
    dests = (g_dev, x_dev, y_dev, me)
    rows = half // LANES
    n_dev = 8

    def sib_copy(j, t):
        src = pl.multiple_of((dests[j] + sib_delta) * share + t * 2 * half, TILE)
        dst = pl.multiple_of(j * share + t * 2 * half, TILE)
        return pltpu.make_async_remote_copy(
            src_ref=g.at[:, pl.ds(src, 2 * half)], dst_ref=sib_land.at[:, pl.ds(dst, 2 * half)],
            send_sem=sib_send, recv_sem=sib_recv.at[j, t], device_id=(sib,), device_id_type=MESH)

    def first_copy(part):
        src = pl.multiple_of((g_dev + sib_delta) * share + part * half, TILE)
        return pltpu.make_async_remote_copy(
            src_ref=g.at[:, pl.ds(src, half)], dst_ref=raw_sib.at[0, :, pl.ds(part * half, half)],
            send_sem=first_send.at[part], recv_sem=first_recv.at[part], device_id=(sib,), device_id_type=MESH)

    def raw_copy(piece, t, slot, which):
        place, width = PIECES[piece]
        j = {'diag': 0, 'x_b': 1, 'x_a': 1, 'y_a': 2, 'y_b': 2, 'mine': 3}[piece]
        skip = half if piece in ('x_b', 'y_b') else 0
        n = width * half
        here = pl.ds(place * half, n)
        index = list(PIECES).index(piece)
        src = pl.multiple_of(dests[j] * share + t * 2 * half + skip, TILE)
        land = pl.multiple_of(j * share + t * 2 * half + skip, TILE)
        if which == 0:
            return pltpu.make_async_copy(g.at[:, pl.ds(src, n)], raw_own.at[slot, :, here], own_sem.at[slot, index])
        return pltpu.make_async_copy(sib_land.at[:, pl.ds(land, n)], raw_sib.at[slot, :, here],
                                     sibin_sem.at[slot, index])

    def land_rows(t, part):
        return pl.ds(pl.multiple_of(t * 2 * rows + part * rows, 8), rows)

    def remote(stage, slot, part, land, t, send, recv, target):
        return pltpu.make_async_remote_copy(
            src_ref=stage.at[slot, pl.ds(part * rows, rows), :], dst_ref=land.at[land_rows(t, part), :],
            send_sem=send.at[slot, part], recv_sem=recv.at[part, t], device_id=(target,), device_id_type=MESH)

    def leaf_copy(t, slot, part):
        return remote(leaf_st, slot, part, leaf_land, t, leaf_send, leaf_recv, (y_dev, x_dev)[part])

    def direct_copy(t, slot, part):
        return remote(direct_st, slot, part, direct_land, t, direct_send, direct_recv, (y_dev, x_dev)[part])

    def four_copy(t, slot, part):
        return remote(four_st, slot, part, four_land, t, four_send, four_recv, (x_dev, y_dev)[part])

    def leaf_load(t, part):
        return pltpu.make_async_copy(leaf_land.at[land_rows(t, part), :], leaf_in.at[pl.ds(part * rows, rows), :],
                                     leafin_sem.at[part])

    def fin_load(which, t, part):
        return pltpu.make_async_copy((four_land, direct_land)[which].at[land_rows(t, part), :],
                                     fin_in.at[which, pl.ds(part * rows, rows), :], fin_sem.at[which, part])

    def out_copy(t, slot):
        both = pl.ds(pl.multiple_of(t * 2 * rows, 8), 2 * rows)
        return pltpu.make_async_copy(out_st.at[slot], total.at[both, :], out_sem.at[slot])

    blk = block_len(half, 16 * TILE)
    blk_rows = blk // LANES

    def pair(slot, place, i):
        at = pl.ds(pl.multiple_of(place * half + i * blk, TILE), blk)
        own = raw_own[slot, :, at].astype(jnp.float32).reshape(blk_rows, LANES)
        other = raw_sib[slot, :, at].astype(jnp.float32).reshape(blk_rows, LANES)
        return own + other

    def block_rows(i, part=0):
        return pl.ds(pl.multiple_of(part * rows + i * blk_rows, 8), blk_rows)

    def store_pair(slot, place, stage, part):
        @pl.loop(0, half // blk)
        def _(i):
            stage[slot, block_rows(i, part), :] = pair(slot, place, i)

    def wait_raw(piece, t, slot):
        for which in range(2):
            raw_copy(piece, t, slot, which).wait()

    own_rows = pv.shape[0]

    def row_part(dev):
        return gv.at[:, pl.ds(pl.multiple_of(dev * own_rows * LANES, LANES), own_rows * LANES)]

    def row_copy(k):
        target = lax.rem(me + k, n_dev)
        return pltpu.make_async_remote_copy(
            src_ref=row_part(target), dst_ref=vec_land.at[me], send_sem=vec_send.at[k - 1, 0],
            recv_sem=vec_recv.at[k - 1, 0], device_id=(target,), device_id_type=MESH)

    def new_copy(k):
        return pltpu.make_async_remote_copy(
            src_ref=vec_new.at[0], dst_ref=vec_w.at[me], send_sem=vec_send.at[k - 1, 1], recv_sem=vec_recv.at[k - 1, 1],
            device_id=(lax.rem(me + k, n_dev),), device_id_type=MESH)

    def send_sib(t):
        @pl.when(jnp.logical_and(t >= 1, t < steps))
        def _():
            sib_copy(0, t).start()

        @pl.when(t < steps)
        def _():
            for j in range(1, 3):
                sib_copy(j, t).start()

        @pl.when(t >= 1)
        def _():
            sib_copy(3, t - 1).start()

    def fetch(t, which):
        slot = lax.rem(t, 2)

        @pl.when(jnp.logical_and(t >= which, t < steps))
        def _():
            if which == 1:
                sib_copy(0, t).wait_recv()
            raw_copy('diag', t, slot, which).start()

        @pl.when(t < steps)
        def _():
            for j, piece in ((1, 'x_b'), (2, 'y_a')):
                if which == 1:
                    sib_copy(j, t).wait_recv()
                raw_copy(piece, t, slot, which).start()

        @pl.when(jnp.logical_and(t >= 1, t <= steps))
        def _():
            for piece in ('x_a', 'y_b'):
                raw_copy(piece, t - 1, slot, which).start()

        @pl.when(jnp.logical_and(t >= 2, t <= steps + 1))
        def _():
            if which == 1:
                sib_copy(3, t - 2).wait_recv()
            raw_copy('mine', t - 2, slot, which).start()

    barrier = pltpu.get_barrier_semaphore()
    for k in range(1, n_dev):
        pl.semaphore_signal(barrier, inc=1, device_id=(lax.rem(me + k, n_dev),), device_id_type=MESH)
    fetch(jnp.int32(0), 0)
    pl.semaphore_wait(barrier, n_dev - 1)
    for part in range(2):
        first_copy(part).start()
    send_sib(jnp.int32(0))
    acc[...] = jnp.zeros_like(acc)
    send_sib(jnp.int32(1))

    @pl.loop(0, steps + 2)
    def _(t):
        slot = lax.rem(t, 2)
        before = 1 - slot

        @pl.when(t + 2 <= steps)
        def _():
            send_sib(t + 2)

        fetch(t + 1, 0)

        @pl.when(t < steps)
        def _():
            raw_copy('diag', t, slot, 0).wait()

            @pl.when(t >= 1)
            def _():
                raw_copy('diag', t, slot, 1).wait()

            for part in range(2):
                @pl.when(t == 0)
                def _():
                    first_copy(part).wait_recv()

                @pl.when(t >= 2)
                def _():
                    leaf_copy(t - 2, slot, part).wait_send()

                store_pair(slot, part, leaf_st, part)
                leaf_copy(t, slot, part).start()

            @pl.when(t == 0)
            def _():
                fetch(t, 1)

            for part, piece, place in ((1, 'x_b', 2), (0, 'y_a', 3)):
                wait_raw(piece, t, slot)

                @pl.when(t >= 2)
                def _():
                    direct_copy(t - 2, slot, part).wait_send()

                store_pair(slot, place, direct_st, part)
                direct_copy(t, slot, part).start()

        fetch(t + 1, 1)

        @pl.when(t == 0)
        def _():
            for k in range(1, n_dev):
                row_copy(k).start()
            pltpu.make_async_copy(row_part(me), vec_land.at[me], local_sem).start()

        @pl.when(t == 3)
        def _():
            for k in range(1, n_dev):
                row_copy(k).wait()
            pltpu.make_async_copy(row_part(me), vec_land.at[me], local_sem).wait()
            part_sum = vec_land[0].astype(jnp.float32)
            for d in range(1, n_dev):
                part_sum += vec_land[d].astype(jnp.float32)
            part_sum = part_sum.reshape(own_rows, LANES)
            vec_sum[...] = part_sum
            acc[0:own_rows, :] += part_sum * part_sum

        @pl.when(jnp.logical_and(t >= 1, t <= steps))
        def _():
            for part in range(2):
                leaf_copy(t - 1, before, part).wait_recv()
                leaf_load(t - 1, part).start()
            for part, piece, place in ((0, 'x_a', 4), (1, 'y_b', 5)):
                wait_raw(piece, t - 1, slot)

                @pl.when(t >= 3)
                def _():
                    four_copy(t - 3, before, part).wait_send()

                leaf_load(t - 1, part).wait()

                @pl.loop(0, half // blk)
                def _(i):
                    at = block_rows(i, part)
                    four_st[before, at, :] = leaf_in[at, :] + pair(slot, place, i)

                four_copy(t - 1, before, part).start()

        @pl.when(t >= 2)
        def _():
            for part in range(2):
                direct_copy(t - 2, slot, part).wait_recv()
                fin_load(1, t - 2, part).start()
            wait_raw('mine', t - 2, slot)

            @pl.when(t >= 4)
            def _():
                out_copy(t - 4, slot).wait()

            for part in range(2):
                four_copy(t - 2, slot, part).wait_recv()
                fin_load(0, t - 2, part).start()
                fin_load(1, t - 2, part).wait()
                fin_load(0, t - 2, part).wait()

                @pl.loop(0, half // blk)
                def _(i):
                    at = block_rows(i, part)
                    whole = (fin_in[0, at, :] + fin_in[1, at, :]) + pair(slot, 6 + part, i)
                    out_st[slot, at, :] = whole
                    acc[...] += jnp.sum((whole * whole).reshape(blk_rows // 8, 8, LANES), axis=0)
            out_copy(t - 2, slot).start()

    def square_copy(k):
        target = lax.rem(me + k, n_dev)
        return pltpu.make_async_remote_copy(
            src_ref=acc, dst_ref=sq_land.at[me], send_sem=sq_send.at[k - 1], recv_sem=sq_recv.at[k - 1],
            device_id=(target,), device_id_type=MESH)

    for k in range(1, n_dev):
        square_copy(k).start()
    sq_land[me] = acc[...]
    for t in (steps - 2, steps - 1):
        out_copy(t, t % 2).wait()
    share_rows = share // LANES
    half_rows = share_rows // 2
    w_rows = half_rows // w_steps

    def inside(part, t, n=1):
        return pl.ds(pl.multiple_of(part * half_rows + t * w_rows, 16), n * w_rows)

    def place(dev, part, t):
        return pl.ds(pl.multiple_of(dev * share_rows + part * half_rows + t * w_rows, 16), w_rows)

    def state_copies(t, slot):
        return [pltpu.make_async_copy(src.at[inside(part, t), :], state_in.at[slot, i, part], state_sem.at[slot, i, part])
                for i, src in enumerate((total, p_mat, m_mat, s_mat)) for part in range(2)]

    def own_copy(to, part, t):
        target = (x_dev, y_dev, sib)[to]
        recv = own_sib_recv if to == 2 else own_recv.at[to, part, t]
        return pltpu.make_async_remote_copy(
            src_ref=own_w.at[inside(part, t), :], dst_ref=gathered.at[place(me, part, t), :],
            send_sem=own_send.at[to], recv_sem=recv, device_id=(target,), device_id_type=MESH)

    def keep_copy(part, t):
        return pltpu.make_async_copy(own_w.at[inside(part, t), :], gathered.at[place(me, part, t), :], keep_sem)

    def late_copy(group, part):
        start = w_steps - sum(w_late[group:])
        return pltpu.make_async_copy(own_w.at[inside(part, start, w_late[group]), :],
                                     ((late_a, late_b), (last_a, last_b))[group][part], late_sem.at[group, part])

    def forward(part, t):
        rows_at = place((x_dev, y_dev)[part], part, t)
        return pltpu.make_async_remote_copy(
            src_ref=gathered.at[rows_at, :], dst_ref=gathered.at[rows_at, :],
            send_sem=fwd_send.at[part], recv_sem=fwd_recv.at[part, t],
            device_id=((y_dev, x_dev)[part],), device_id_type=MESH)

    def to_sib(dev, part, t):
        rows_at = place(dev, part, t)
        return pltpu.make_async_remote_copy(
            src_ref=gathered.at[rows_at, :], dst_ref=gathered.at[rows_at, :],
            send_sem=fsib_send, recv_sem=fsib_recv, device_id=(sib,), device_id_type=MESH)

    def all_rows(n, send, recv):
        return pltpu.make_async_remote_copy(
            src_ref=gathered.at[pl.ds(0, n * w_rows), :], dst_ref=gathered.at[pl.ds(0, n * w_rows), :],
            send_sem=send, recv_sem=recv, device_id=(sib,), device_id_type=MESH)

    for copy in state_copies(0, 0):
        copy.start()

    square = jnp.zeros_like(acc)
    for k in range(1, n_dev):
        square_copy(k).wait()
    for d in range(n_dev):
        square += sq_land[d]
    norm = jnp.sqrt(jnp.sum(jnp.sum(square, axis=0, keepdims=True), axis=1, keepdims=True))
    coef = jnp.minimum(1.0, 1.0 / (norm + NORM_EPS))
    coef_out[...] = jnp.broadcast_to(coef, coef_out.shape)

    w_tiles = w_rows // 16
    w_blk = 16 * max(d for d in range(1, 9) if w_tiles % d == 0)

    def update(slot, part, t):
        @pl.loop(0, w_rows // w_blk)
        def _(i):
            at = pl.ds(pl.multiple_of(i * w_blk, 16), w_blk)
            grad, master, moment, second = (state_in[slot, k, part, at, :] for k in range(4))
            new = adam_update(grad, coef_out[0:1, :], master, moment, second, DECAY)[0]
            out = pl.ds(pl.multiple_of(part * half_rows + t * w_rows + i * w_blk, 16), w_blk)
            own_w[out, :] = new.astype(jnp.bfloat16)

    early = w_steps - sum(w_late)

    @pl.loop(0, w_steps + LAG + 2)
    def _(u):
        slot = lax.rem(u, 2)

        @pl.when(u + 1 < w_steps)
        def _():
            for copy in state_copies(u + 1, 1 - slot):
                copy.start()

        @pl.when(u < w_steps)
        def _():
            for copy in state_copies(u, slot):
                copy.wait()
            for part in range(2):
                update(slot, part, u)
                own_copy(part, part, u).start()

                @pl.when(u < early)
                def _():
                    own_copy(1 - part, part, u).start()

                own_copy(2, part, u).start()
                keep_copy(part, u).start()

        @pl.when(jnp.logical_and(u >= LAG, u < w_steps + LAG))
        def _():
            t = u - LAG
            for part in range(2):
                own_copy(part, part, t).wait_recv()
                forward(part, t).start()
                to_sib((x_dev, y_dev)[part], part, t).start()

            @pl.when(t < early)
            def _():
                for part in range(2):
                    own_copy(1 - part, part, t).wait_recv()
                    to_sib((y_dev, x_dev)[part], part, t).start()

        @pl.when(u >= LAG + 2)
        def _():
            t = u - LAG - 2
            for part in range(2):
                forward(part, t).wait_recv()
                to_sib(g_dev, part, t).start()

        @pl.when(u == 1)
        def _():
            new = adam_update(vec_sum[...], coef_out[0:1, :], pv[...], mv[...], sv[...], 0.0)
            for i in range(3):
                vec_new[i] = new[i]
            vec_w[me] = new[0]
            for k in range(1, n_dev):
                new_copy(k).start()

        @pl.when(u == w_steps - 1)
        def _():
            for group in range(2):
                for part in range(2):
                    late_copy(group, part).start()

    for k in range(1, n_dev):
        new_copy(k).wait()

    for t in (steps - 2, steps - 1):
        slot = t % 2
        for part in range(2):
            leaf_copy(t, slot, part).wait_send()
            direct_copy(t, slot, part).wait_send()
            four_copy(t, slot, part).wait_send()
    pltpu.make_async_remote_copy(
        src_ref=g.at[:, pl.ds(0, 4 * share - 2 * half)], dst_ref=sib_land.at[:, pl.ds(0, 4 * share - 2 * half)],
        send_sem=sib_send, recv_sem=sib_recv.at[0, 0], device_id=(sib,), device_id_type=MESH).wait_send()
    for part in range(2):
        first_copy(part).wait_send()
    for part in range(2):
        late_copy(0, part).wait()
        late_copy(1, part).wait()
        all_rows(w_steps + early, own_send.at[part], fsib_recv).wait_send()
        all_rows(w_steps, fwd_send.at[part], fsib_recv).wait_send()
    all_rows(2 * w_steps, own_send.at[2], own_sib_recv).wait()
    all_rows(4 * w_steps + 2 * early, fsib_send, fsib_recv).wait()
    pltpu.make_async_copy(own_w, gathered.at[pl.ds(0, share_rows), :], keep_sem).wait()


def step_call(g, gv, p_mat, m_mat, s_mat, pv, mv, sv, share, steps, w_steps, w_late):
    half = share // (2 * steps)
    rows = half // LANES
    share_rows = share // LANES
    w_rows = share_rows // (2 * w_steps)
    dma = pltpu.SemaphoreType.DMA
    f32, bf16 = jnp.float32, jnp.bfloat16
    own_rows = pv.shape[0]
    hbm = pl.BlockSpec(memory_space=pltpu.HBM)
    vmem = pl.BlockSpec(memory_space=pltpu.VMEM)
    return pl.pallas_call(
        functools.partial(step_kernel, share, half, steps, w_steps, w_late),
        out_shape=(jax.ShapeDtypeStruct((share_rows, LANES), f32),
                   jax.ShapeDtypeStruct((8 * share_rows, LANES), bf16),
                   jax.ShapeDtypeStruct((w_late[0] * w_rows, LANES), bf16),
                   jax.ShapeDtypeStruct((w_late[0] * w_rows, LANES), bf16),
                   jax.ShapeDtypeStruct((w_late[1] * w_rows, LANES), bf16),
                   jax.ShapeDtypeStruct((w_late[1] * w_rows, LANES), bf16),
                   jax.ShapeDtypeStruct((1, 4 * share), bf16),
                   jax.ShapeDtypeStruct((share_rows, LANES), f32),
                   jax.ShapeDtypeStruct((share_rows, LANES), f32),
                   jax.ShapeDtypeStruct((share_rows, LANES), f32),
                   jax.ShapeDtypeStruct((8, LANES), f32),
                   jax.ShapeDtypeStruct((3, own_rows, LANES), f32),
                   jax.ShapeDtypeStruct((8, own_rows, LANES), f32)),
        in_specs=[hbm, vmem, hbm, hbm, hbm, vmem, vmem, vmem],
        out_specs=(hbm,) * 10 + (vmem,) * 3,
        scratch_shapes=[
            pltpu.VMEM((2, 1, 8 * half), bf16),
            pltpu.VMEM((2, 1, 8 * half), bf16),
            pltpu.VMEM((2, 2 * rows, LANES), f32),
            pltpu.VMEM((2, 2 * rows, LANES), f32),
            pltpu.VMEM((2, 2 * rows, LANES), f32),
            pltpu.VMEM((2 * rows, LANES), f32),
            pltpu.VMEM((2, 2 * rows, LANES), f32),
            pltpu.VMEM((2, 2 * rows, LANES), f32),
            pltpu.VMEM((8, LANES), f32),
            pltpu.VMEM((8, 8, LANES), f32),
            pltpu.VMEM((8, 1, own_rows * LANES), bf16),
            dma(()), dma((4, steps)),
            dma((2, 2)), dma((2, steps)), dma((2, 2)), dma((2, steps)), dma((2, 2)), dma((2, steps)),
            dma((2, 6)), dma((2, 6)), dma((2,)), dma((2, 2)), dma((2,)),
            dma((7,)), dma((7,)), dma((7, 2)), dma((7, 2)), dma(()),
            pltpu.VMEM((2, 4, 2, w_rows, LANES), f32),
            pltpu.VMEM((share_rows, LANES), bf16),
            dma((2, 4, 2)), dma((3,)), dma((2, 2, w_steps)), dma(()), dma(()), dma((2, 2)),
            dma((2,)), dma((2, w_steps)), dma(()), dma(()), dma((2,)), dma((2,)),
            pltpu.VMEM((own_rows, LANES), f32),
        ],
        compiler_params=pltpu.CompilerParams(collective_id=0, has_side_effects=True, vmem_limit_bytes=60 * 2**20),
        name='reduce_update_gather',
    )(g, gv, p_mat, m_mat, s_mat, pv, mv, sv)


def update_kernel(coef, grad, master, moment, second, vec_new, vec_w, new_p, new_m, new_s, vec_p, vec_m, vec_s, w_vec,
                  rows):
    new_p[...], new_m[...], new_s[...] = adam_update(grad[...], coef[0:1, :], master[...], moment[...], second[...], DECAY)

    @pl.when(pl.program_id(0) == 0)
    def _():
        vec_p[...], vec_m[...], vec_s[...] = vec_new[0], vec_new[1], vec_new[2]
        n = vec_w.shape[1]
        for d in range(vec_w.shape[0]):
            rows[pl.ds(d * n, n), :] = vec_w[d]
        w_vec[...] = rows[...].astype(jnp.bfloat16)


def update_call(coef, grad, master, moment, second, vec_new, vec_w, block):
    n = grad.shape[0]
    own_rows = vec_new.shape[1]
    f32 = jnp.float32
    tile = pl.BlockSpec((block, LANES), lambda i: (i, 0))

    def whole(shape):
        return pl.BlockSpec(shape, lambda i: (0,) * len(shape))

    small = jax.ShapeDtypeStruct((own_rows, LANES), f32)
    return pl.pallas_call(
        update_kernel,
        grid=(n // block,),
        out_shape=(jax.ShapeDtypeStruct(grad.shape, f32),) * 3 + (small,) * 3 + (
            jax.ShapeDtypeStruct((8 * own_rows, LANES), jnp.bfloat16),),
        in_specs=[whole((8, LANES))] + [tile] * 4 + [whole(vec_new.shape), whole(vec_w.shape)],
        out_specs=(tile,) * 3 + (whole((own_rows, LANES)),) * 3 + (whole((8 * own_rows, LANES)),),
        scratch_shapes=[pltpu.VMEM((8 * own_rows, LANES), f32)],
        compiler_params=pltpu.CompilerParams(vmem_limit_bytes=40 * 2**20),
        cost_estimate=pl.CostEstimate(flops=n * LANES * 200, bytes_accessed=n * LANES * 28, transcendentals=0),
        name='update',
    )(coef, grad, master, moment, second, vec_new, vec_w)


def copy_kernel(moves, blocks, *refs):
    n_src = 1 + max(move[0] for move in moves(0))
    srcs, out, buf, in_sem, out_sem = refs[:n_src], refs[-4], refs[-3], refs[-2], refs[-1]
    me = lax.axis_index('fsdp')
    todo = []
    for which, src_row, dst_row, n in moves(me):
        if n == 0:
            continue
        size = n // blocks(n)
        for i in range(blocks(n)):
            todo.append((srcs[which], src_row + i * size, dst_row + i * size, size))
    slots = buf.shape[0]

    def take(k):
        src, src_row, _, size = todo[k]
        return pltpu.make_async_copy(src.at[pl.ds(pl.multiple_of(src_row, 16), size), :],
                                     buf.at[k % slots, pl.ds(0, size), :], in_sem.at[k % slots])

    def give(k):
        _, _, dst_row, size = todo[k]
        return pltpu.make_async_copy(buf.at[k % slots, pl.ds(0, size), :],
                                     out.at[pl.ds(pl.multiple_of(dst_row, 16), size), :], out_sem.at[k % slots])

    ahead = slots // 2
    for k in range(min(ahead, len(todo))):
        take(k).start()
    for k in range(len(todo)):
        take(k).wait()
        give(k).start()
        if k + ahead < len(todo):
            if k + ahead >= slots:
                give(k + ahead - slots).wait()
            take(k + ahead).start()
    for k in range(max(0, len(todo) - slots), len(todo)):
        give(k).wait()


def copy_call(moves, srcs, out_rows, into=None, slots=6, most=14560):
    def blocks(n):
        return next(d for d in range(1, n // 16 + 1) if (n // 16) % d == 0 and n // d <= most)

    hbm = pl.BlockSpec(memory_space=pltpu.HBM)
    args = list(srcs) + ([into] if into is not None else [])
    size = sum(move[3] for move in moves(0)) * LANES * 2
    return pl.pallas_call(
        functools.partial(copy_kernel, moves, blocks),
        out_shape=jax.ShapeDtypeStruct((out_rows, LANES), jnp.bfloat16),
        in_specs=[hbm] * len(args),
        out_specs=hbm,
        scratch_shapes=[pltpu.VMEM((slots, most, LANES), jnp.bfloat16),
                        pltpu.SemaphoreType.DMA((slots,)), pltpu.SemaphoreType.DMA((slots,))],
        input_output_aliases={len(srcs): 0} if into is not None else {},
        compiler_params=pltpu.CompilerParams(vmem_limit_bytes=32 * 2**20),
        cost_estimate=pl.CostEstimate(flops=size * 6, bytes_accessed=2 * size, transcendentals=0),
    )(*args)


def place_kernel(moves, *refs):
    out, sems = refs[-2], refs[-1]
    copies = [pltpu.make_async_copy(refs[which], out.at[pl.ds(pl.multiple_of(dst_row, 16), n), :], sems.at[i])
              for i, (which, _, dst_row, n) in enumerate(moves(lax.axis_index('fsdp')))]
    for copy in copies:
        copy.start()
    for copy in copies:
        copy.wait()


def place_call(moves, srcs, into):
    hbm, vmem = pl.BlockSpec(memory_space=pltpu.HBM), pl.BlockSpec(memory_space=pltpu.VMEM)
    size = sum(move[3] for move in moves(0)) * LANES * 2
    return pl.pallas_call(
        functools.partial(place_kernel, moves),
        out_shape=jax.ShapeDtypeStruct(into.shape, into.dtype),
        in_specs=[vmem] * len(srcs) + [hbm],
        out_specs=hbm,
        scratch_shapes=[pltpu.SemaphoreType.DMA((len(srcs),))],
        input_output_aliases={len(srcs): 0},
        compiler_params=pltpu.CompilerParams(vmem_limit_bytes=16 * 2**20),
        cost_estimate=pl.CostEstimate(flops=size * 6, bytes_accessed=2 * size, transcendentals=0),
    )(*srcs, into)


def block_rows_of(n):
    return 16 * max(d for d in range(1, 190) if (n // 16) % d == 0)


STEPS = 28
W_STEPS = 26
W_LATE = (19, 6)
LAG = 3


def neighbours(me):
    core, x_pos, y_pos = lax.rem(me, 2), lax.rem(me // 2, 2), me // 4
    return me + 1 - 2 * core, me + 2 - 4 * x_pos, me + 4 - 8 * y_pos


def solution(mesh):
    hop_x = [(d, d ^ 2) for d in range(8)]
    hop_y = [(d, d ^ 4) for d in range(8)]
    hop_core = [(d, d ^ 1) for d in range(8)]

    def local_step(grad_mat, grad_vec, master_mat, moment_mat, second_mat, master_vec, moment_vec, second_vec):
        share = master_mat.shape[0]
        share_rows = share // LANES
        half_rows = share_rows // 2
        late, last = (n * (half_rows // W_STEPS) for n in W_LATE)
        early = half_rows - late - last
        own_rows = master_vec.shape[0] // LANES
        mats = [v.reshape(share_rows, LANES) for v in (master_mat, moment_mat, second_mat)]
        vecs = [v.reshape(own_rows, LANES) for v in (master_vec, moment_vec, second_vec)]
        total, gathered, late_a, late_b, last_a, last_b, _, _, _, _, coef, vec_new, vec_w = step_call(
            grad_mat, grad_vec, *mats, *vecs, share, STEPS, W_STEPS, W_LATE)

        late_x = lax.ppermute(late_b, 'fsdp', hop_x)
        late_y = lax.ppermute(late_a, 'fsdp', hop_y)
        last_x = lax.ppermute(last_b, 'fsdp', hop_x)
        last_y = lax.ppermute(last_a, 'fsdp', hop_y)

        def whole_moves(me):
            sib, x_dev, y_dev = neighbours(me)
            g_dev = x_dev + y_dev - me
            flip = sib - me
            return [(0, dev * share_rows, dev * share_rows, share_rows) for dev in (me, sib, g_dev, g_dev + flip)] + [
                (0, x_dev * share_rows, x_dev * share_rows, half_rows)]

        def late_rows(x_dev, y_dev, first):
            return [(first, 0, x_dev * share_rows + half_rows + early, late),
                    (first + 1, 0, y_dev * share_rows + early, late)]

        def last_rows(x_dev, y_dev, first):
            return [(first, 0, x_dev * share_rows + half_rows + early + late, last),
                    (first + 1, 0, y_dev * share_rows + early + late, last)]

        def early_moves(me):
            sib, x_dev, y_dev = neighbours(me)
            flip = sib - me
            moves = [(0, (x_dev + flip) * share_rows, (x_dev + flip) * share_rows, half_rows)]
            for dev in (x_dev, x_dev + flip):
                start = dev * share_rows + half_rows
                moves.append((0, start, start, early))
            for dev in (y_dev, y_dev + flip):
                start = dev * share_rows
                moves.append((0, start, start, early))
                moves.append((0, start + half_rows, start + half_rows, half_rows))
            return moves + late_rows(x_dev, y_dev, 1)

        def mid_moves(me):
            sib, x_dev, y_dev = neighbours(me)
            return late_rows(x_dev + sib - me, y_dev + sib - me, 0)

        def late_moves(me):
            _, x_dev, y_dev = neighbours(me)
            return last_rows(x_dev, y_dev, 0)

        def last_moves(me):
            sib, x_dev, y_dev = neighbours(me)
            flip = sib - me
            return last_rows(x_dev + flip, y_dev + flip, 0)

        *new, weights_vec = update_call(coef, total, *mats, vec_new, vec_w, block_rows_of(share_rows))
        weights = copy_call(whole_moves, (gathered,), 8 * share_rows)
        late_x, late_y, weights, *new = lax.optimization_barrier((late_x, late_y, weights, *new))
        sib_late_x = lax.ppermute(late_x, 'fsdp', hop_core)
        sib_late_y = lax.ppermute(late_y, 'fsdp', hop_core)
        weights = copy_call(early_moves, (gathered, late_x, late_y), 8 * share_rows, into=weights)
        weights = place_call(mid_moves, (sib_late_x, sib_late_y), weights)
        last_x, last_y, weights = lax.optimization_barrier((last_x, last_y, weights))
        sib_last_x = lax.ppermute(last_x, 'fsdp', hop_core)
        sib_last_y = lax.ppermute(last_y, 'fsdp', hop_core)
        weights = place_call(late_moves, (last_x, last_y), weights)
        weights = place_call(last_moves, (sib_last_x, sib_last_y), weights)
        return tuple(v.reshape(-1) for v in (*new, weights, weights_vec))

    row_spec = P('fsdp', None)
    flat_spec = P('fsdp')
    whole_spec = P()
    return jax.shard_map(local_step, mesh=mesh,
                         in_specs=(row_spec, row_spec) + (flat_spec,) * 6,
                         out_specs=(flat_spec,) * 6 + (whole_spec, whole_spec),
                         check_vma=False)
```

```python
import functools

import jax
import jax.numpy as jnp
from jax import lax
from jax.experimental import pallas as pl
from jax.experimental.pallas import tpu as pltpu
from jax.sharding import PartitionSpec as P


STEP = 4
LEARN_RATE = 1e-3
BETA_ONE = 0.9
BETA_TWO = 0.999
ADAM_EPS = 1e-8
DECAY = 0.01
NORM_EPS = 1e-6
FIX_ONE = 1.0 - BETA_ONE ** STEP
FIX_TWO = 1.0 - BETA_TWO ** STEP

MESH = pl.DeviceIdType.MESH
LANES = 128
TILE = 1024


def adam_update(grad_sum, clip_coef, master, moment, second, decay):
    clip_grad = clip_coef * grad_sum
    new_moment = BETA_ONE * moment + (1.0 - BETA_ONE) * clip_grad
    new_second = BETA_TWO * second + (1.0 - BETA_TWO) * clip_grad * clip_grad
    step_dir = (new_moment * (LEARN_RATE / FIX_ONE)) / (jnp.sqrt(new_second * (1.0 / FIX_TWO)) + ADAM_EPS)
    new_master = master - (step_dir + (LEARN_RATE * decay) * master)
    return new_master, new_moment, new_second


def block_len(n, most):
    tiles = n // TILE
    return max(d for d in range(1, most // TILE + 1) if tiles % d == 0) * TILE


PIECES = {'diag': (0, 2), 'x_b': (2, 1), 'y_a': (3, 1), 'x_a': (4, 1), 'y_b': (5, 1), 'mine': (6, 2)}


def step_kernel(share, half, steps, w_steps, w_late, g, gv, p_mat, m_mat, s_mat, pv, mv, sv,
                total, gathered, late_a, late_b, last_a, last_b, sib_land, leaf_land, four_land, direct_land, coef_out, vec_new, vec_w,
                raw_own, raw_sib, leaf_st, direct_st, four_st, leaf_in, fin_in, out_st, acc, sq_land, vec_land,
                  sib_send, sib_recv, leaf_send, leaf_recv, four_send, four_recv, direct_send, direct_recv,
                  own_sem, sibin_sem, leafin_sem, fin_sem, out_sem, sq_send, sq_recv, vec_send, vec_recv, local_sem,
                state_in, own_w, state_sem, own_send, own_recv, own_sib_recv, keep_sem, late_sem,
                fwd_send, fwd_recv, fsib_send, fsib_recv, first_send, first_recv, vec_sum):
    me = lax.axis_index('fsdp')
    core = lax.rem(me, 2)
    x_pos = lax.rem(me // 2, 2)
    y_pos = me // 4
    sib = me + 1 - 2 * core
    x_dev = me + 2 - 4 * x_pos
    y_dev = me + 4 - 8 * y_pos
    g_dev = y_dev + 2 - 4 * x_pos
    sib_delta = 1 - 2 * core
    dests = (g_dev, x_dev, y_dev, me)
    rows = half // LANES
    n_dev = 8

    def sib_copy(j, t):
        src = pl.multiple_of((dests[j] + sib_delta) * share + t * 2 * half, TILE)
        dst = pl.multiple_of(j * share + t * 2 * half, TILE)
        return pltpu.make_async_remote_copy(
            src_ref=g.at[:, pl.ds(src, 2 * half)], dst_ref=sib_land.at[:, pl.ds(dst, 2 * half)],
            send_sem=sib_send, recv_sem=sib_recv.at[j, t], device_id=(sib,), device_id_type=MESH)

    def first_copy(part):
        src = pl.multiple_of((g_dev + sib_delta) * share + part * half, TILE)
        return pltpu.make_async_remote_copy(
            src_ref=g.at[:, pl.ds(src, half)], dst_ref=raw_sib.at[0, :, pl.ds(part * half, half)],
            send_sem=first_send.at[part], recv_sem=first_recv.at[part], device_id=(sib,), device_id_type=MESH)

    def raw_copy(piece, t, slot, which):
        place, width = PIECES[piece]
        j = {'diag': 0, 'x_b': 1, 'x_a': 1, 'y_a': 2, 'y_b': 2, 'mine': 3}[piece]
        skip = half if piece in ('x_b', 'y_b') else 0
        n = width * half
        here = pl.ds(place * half, n)
        index = list(PIECES).index(piece)
        src = pl.multiple_of(dests[j] * share + t * 2 * half + skip, TILE)
        land = pl.multiple_of(j * share + t * 2 * half + skip, TILE)
        if which == 0:
            return pltpu.make_async_copy(g.at[:, pl.ds(src, n)], raw_own.at[slot, :, here], own_sem.at[slot, index])
        return pltpu.make_async_copy(sib_land.at[:, pl.ds(land, n)], raw_sib.at[slot, :, here],
                                     sibin_sem.at[slot, index])

    def land_rows(t, part):
        return pl.ds(pl.multiple_of(t * 2 * rows + part * rows, 8), rows)

    def remote(stage, slot, part, land, t, send, recv, target):
        return pltpu.make_async_remote_copy(
            src_ref=stage.at[slot, pl.ds(part * rows, rows), :], dst_ref=land.at[land_rows(t, part), :],
            send_sem=send.at[slot, part], recv_sem=recv.at[part, t], device_id=(target,), device_id_type=MESH)

    def leaf_copy(t, slot, part):
        return remote(leaf_st, slot, part, leaf_land, t, leaf_send, leaf_recv, (y_dev, x_dev)[part])

    def direct_copy(t, slot, part):
        return remote(direct_st, slot, part, direct_land, t, direct_send, direct_recv, (y_dev, x_dev)[part])

    def four_copy(t, slot, part):
        return remote(four_st, slot, part, four_land, t, four_send, four_recv, (x_dev, y_dev)[part])

    def both_rows(t):
        return pl.ds(pl.multiple_of(t * 2 * rows, 8), 2 * rows)

    def leaf_load(t):
        return pltpu.make_async_copy(leaf_land.at[both_rows(t), :], leaf_in, leafin_sem)

    def fin_load(which, t):
        return pltpu.make_async_copy((four_land, direct_land)[which].at[both_rows(t), :], fin_in.at[which],
                                     fin_sem.at[which])

    def out_copy(t, slot):
        both = pl.ds(pl.multiple_of(t * 2 * rows, 8), 2 * rows)
        return pltpu.make_async_copy(out_st.at[slot], total.at[both, :], out_sem.at[slot])

    blk = block_len(half, 16 * TILE)
    blk_rows = blk // LANES

    def pair(slot, place, i):
        at = pl.ds(pl.multiple_of(place * half + i * blk, TILE), blk)
        own = raw_own[slot, :, at].astype(jnp.float32).reshape(blk_rows, LANES)
        other = raw_sib[slot, :, at].astype(jnp.float32).reshape(blk_rows, LANES)
        return own + other

    def block_rows(i, part=0):
        return pl.ds(pl.multiple_of(part * rows + i * blk_rows, 8), blk_rows)

    def store_pair(slot, place, stage, part):
        @pl.loop(0, half // blk)
        def _(i):
            stage[slot, block_rows(i, part), :] = pair(slot, place, i)

    def wait_raw(piece, t, slot):
        for which in range(2):
            raw_copy(piece, t, slot, which).wait()

    own_rows = pv.shape[0]

    def row_part(dev):
        return gv.at[:, pl.ds(pl.multiple_of(dev * own_rows * LANES, LANES), own_rows * LANES)]

    def row_copy(k):
        target = lax.rem(me + k, n_dev)
        return pltpu.make_async_remote_copy(
            src_ref=row_part(target), dst_ref=vec_land.at[me], send_sem=vec_send.at[k - 1, 0],
            recv_sem=vec_recv.at[k - 1, 0], device_id=(target,), device_id_type=MESH)

    def new_copy(k):
        return pltpu.make_async_remote_copy(
            src_ref=vec_new.at[0], dst_ref=vec_w.at[me], send_sem=vec_send.at[k - 1, 1], recv_sem=vec_recv.at[k - 1, 1],
            device_id=(lax.rem(me + k, n_dev),), device_id_type=MESH)

    share_rows = share // LANES
    half_rows = share_rows // 2
    w_rows = half_rows // w_steps

    def inside(part, t, n=1):
        return pl.ds(pl.multiple_of(part * half_rows + t * w_rows, 16), n * w_rows)

    def place(dev, part, t):
        return pl.ds(pl.multiple_of(dev * share_rows + part * half_rows + t * w_rows, 16), w_rows)

    def state_copies(t, slot):
        return [pltpu.make_async_copy(src.at[inside(part, t), :], state_in.at[slot, i, part], state_sem.at[slot, i, part])
                for i, src in enumerate((total, p_mat, m_mat, s_mat)) for part in range(2)]

    def send_sib(t):
        @pl.when(jnp.logical_and(t >= 1, t < steps))
        def _():
            sib_copy(0, t).start()

        @pl.when(t < steps)
        def _():
            for j in range(1, 3):
                sib_copy(j, t).start()

        @pl.when(t >= 1)
        def _():
            sib_copy(3, t - 1).start()

    def fetch(t, which):
        slot = lax.rem(t, 2)

        @pl.when(jnp.logical_and(t >= which, t < steps))
        def _():
            if which == 1:
                sib_copy(0, t).wait_recv()
            raw_copy('diag', t, slot, which).start()

        @pl.when(t < steps)
        def _():
            for j, piece in ((1, 'x_b'), (2, 'y_a')):
                if which == 1:
                    sib_copy(j, t).wait_recv()
                raw_copy(piece, t, slot, which).start()

        @pl.when(jnp.logical_and(t >= 1, t <= steps))
        def _():
            for piece in ('x_a', 'y_b'):
                raw_copy(piece, t - 1, slot, which).start()

        @pl.when(jnp.logical_and(t >= 3, t <= steps + 2))
        def _():
            if which == 1:
                sib_copy(3, t - 3).wait_recv()
            raw_copy('mine', t - 3, slot, which).start()

    barrier = pltpu.get_barrier_semaphore()
    for k in range(1, n_dev):
        pl.semaphore_signal(barrier, inc=1, device_id=(lax.rem(me + k, n_dev),), device_id_type=MESH)
    fetch(jnp.int32(0), 0)
    pl.semaphore_wait(barrier, n_dev - 1)
    for part in range(2):
        first_copy(part).start()
    send_sib(jnp.int32(0))
    acc[...] = jnp.zeros_like(acc)
    send_sib(jnp.int32(1))

    @pl.loop(0, steps + 3)
    def _(t):
        slot = lax.rem(t, 2)
        before = 1 - slot

        @pl.when(t + 2 <= steps)
        def _():
            send_sib(t + 2)

        fetch(t + 1, 0)

        @pl.when(t < steps)
        def _():
            raw_copy('diag', t, slot, 0).wait()

            @pl.when(t >= 1)
            def _():
                raw_copy('diag', t, slot, 1).wait()

            for part in range(2):
                @pl.when(t == 0)
                def _():
                    first_copy(part).wait_recv()

                @pl.when(t >= 2)
                def _():
                    leaf_copy(t - 2, slot, part).wait_send()

                store_pair(slot, part, leaf_st, part)
                leaf_copy(t, slot, part).start()

            @pl.when(t == 0)
            def _():
                fetch(t, 1)

            for part, piece, place in ((1, 'x_b', 2), (0, 'y_a', 3)):
                wait_raw(piece, t, slot)

                @pl.when(t >= 2)
                def _():
                    direct_copy(t - 2, slot, part).wait_send()

                store_pair(slot, place, direct_st, part)
                direct_copy(t, slot, part).start()

        fetch(t + 1, 1)

        @pl.when(t == 0)
        def _():
            for k in range(1, n_dev):
                row_copy(k).start()
            pltpu.make_async_copy(row_part(me), vec_land.at[me], local_sem).start()

        @pl.when(t == 3)
        def _():
            for k in range(1, n_dev):
                row_copy(k).wait()
            pltpu.make_async_copy(row_part(me), vec_land.at[me], local_sem).wait()
            part_sum = vec_land[0].astype(jnp.float32)
            for d in range(1, n_dev):
                part_sum += vec_land[d].astype(jnp.float32)
            part_sum = part_sum.reshape(own_rows, LANES)
            vec_sum[...] = part_sum
            acc[0:own_rows, :] += part_sum * part_sum

        @pl.when(jnp.logical_and(t >= 1, t <= steps))
        def _():
            for part in range(2):
                leaf_copy(t - 1, before, part).wait_recv()
            leaf_load(t - 1).start()
            leaf_load(t - 1).wait()
            for part, piece, place in ((0, 'x_a', 4), (1, 'y_b', 5)):
                wait_raw(piece, t - 1, slot)

                @pl.when(t >= 3)
                def _():
                    four_copy(t - 3, before, part).wait_send()

                @pl.loop(0, half // blk)
                def _(i):
                    at = block_rows(i, part)
                    four_st[before, at, :] = leaf_in[at, :] + pair(slot, place, i)

                four_copy(t - 1, before, part).start()

        @pl.when(t == steps + 1)
        def _():
            for copy in state_copies(0, 0):
                copy.start()

        @pl.when(t >= 3)
        def _():
            wait_raw('mine', t - 3, slot)

            @pl.when(t >= 5)
            def _():
                out_copy(t - 5, slot).wait()

            for which in range(2):
                fin_load(which, t - 3).wait()

            @pl.loop(0, 2 * half // blk)
            def _(i):
                at = block_rows(i)
                whole = (fin_in[0, at, :] + fin_in[1, at, :]) + pair(slot, 6, i)
                out_st[slot, at, :] = whole
                acc[...] += jnp.sum((whole * whole).reshape(blk_rows // 8, 8, LANES), axis=0)

            out_copy(t - 3, slot).start()

        @pl.when(jnp.logical_and(t >= 2, t <= steps + 1))
        def _():
            for part in range(2):
                direct_copy(t - 2, slot, part).wait_recv()
                four_copy(t - 2, slot, part).wait_recv()
            for which in range(2):
                fin_load(which, t - 2).start()

    def square_copy(k):
        target = lax.rem(me + k, n_dev)
        return pltpu.make_async_remote_copy(
            src_ref=acc, dst_ref=sq_land.at[me], send_sem=sq_send.at[k - 1], recv_sem=sq_recv.at[k - 1],
            device_id=(target,), device_id_type=MESH)

    for k in range(1, n_dev):
        square_copy(k).start()
    sq_land[me] = acc[...]
    for t in (steps - 2, steps - 1):
        out_copy(t, 1 - t % 2).wait()

    def own_copy(to, part, t):
        target = (x_dev, y_dev, sib)[to]
        recv = own_sib_recv if to == 2 else own_recv.at[to, part, t]
        return pltpu.make_async_remote_copy(
            src_ref=own_w.at[inside(part, t), :], dst_ref=gathered.at[place(me, part, t), :],
            send_sem=own_send.at[to], recv_sem=recv, device_id=(target,), device_id_type=MESH)

    def keep_copy(part, t):
        return pltpu.make_async_copy(own_w.at[inside(part, t), :], gathered.at[place(me, part, t), :], keep_sem)

    def late_copy(group, part):
        start = w_steps - sum(w_late[group:])
        return pltpu.make_async_copy(own_w.at[inside(part, start, w_late[group]), :],
                                     ((late_a, late_b), (last_a, last_b))[group][part], late_sem.at[group, part])

    def forward(part, t):
        rows_at = place((x_dev, y_dev)[part], part, t)
        return pltpu.make_async_remote_copy(
            src_ref=gathered.at[rows_at, :], dst_ref=gathered.at[rows_at, :],
            send_sem=fwd_send.at[part], recv_sem=fwd_recv.at[part, t],
            device_id=((y_dev, x_dev)[part],), device_id_type=MESH)

    def to_sib(dev, part, t):
        rows_at = place(dev, part, t)
        return pltpu.make_async_remote_copy(
            src_ref=gathered.at[rows_at, :], dst_ref=gathered.at[rows_at, :],
            send_sem=fsib_send, recv_sem=fsib_recv, device_id=(sib,), device_id_type=MESH)

    def all_rows(n, send, recv):
        return pltpu.make_async_remote_copy(
            src_ref=gathered.at[pl.ds(0, n * w_rows), :], dst_ref=gathered.at[pl.ds(0, n * w_rows), :],
            send_sem=send, recv_sem=recv, device_id=(sib,), device_id_type=MESH)

    square = jnp.zeros_like(acc)
    for k in range(1, n_dev):
        square_copy(k).wait()
    for d in range(n_dev):
        square += sq_land[d]
    norm = jnp.sqrt(jnp.sum(jnp.sum(square, axis=0, keepdims=True), axis=1, keepdims=True))
    coef = jnp.minimum(1.0, 1.0 / (norm + NORM_EPS))
    coef_out[...] = jnp.broadcast_to(coef, coef_out.shape)

    w_tiles = w_rows // 16
    w_blk = 16 * max(d for d in range(1, 9) if w_tiles % d == 0)

    def update(slot, part, t):
        @pl.loop(0, w_rows // w_blk)
        def _(i):
            at = pl.ds(pl.multiple_of(i * w_blk, 16), w_blk)
            grad, master, moment, second = (state_in[slot, k, part, at, :] for k in range(4))
            new = adam_update(grad, coef_out[0:1, :], master, moment, second, DECAY)[0]
            out = pl.ds(pl.multiple_of(part * half_rows + t * w_rows + i * w_blk, 16), w_blk)
            own_w[out, :] = new.astype(jnp.bfloat16)

    early = w_steps - sum(w_late)

    @pl.loop(0, w_steps + LAG + 2)
    def _(u):
        slot = lax.rem(u, 2)

        @pl.when(u + 1 < w_steps)
        def _():
            for copy in state_copies(u + 1, 1 - slot):
                copy.start()

        @pl.when(u < w_steps)
        def _():
            for copy in state_copies(u, slot):
                copy.wait()
            for part in range(2):
                update(slot, part, u)
                own_copy(part, part, u).start()

                @pl.when(u < early)
                def _():
                    own_copy(1 - part, part, u).start()

                own_copy(2, part, u).start()
                keep_copy(part, u).start()

        @pl.when(jnp.logical_and(u >= LAG, u < w_steps + LAG))
        def _():
            t = u - LAG
            for part in range(2):
                own_copy(part, part, t).wait_recv()
                forward(part, t).start()
                to_sib((x_dev, y_dev)[part], part, t).start()

            @pl.when(t < early)
            def _():
                for part in range(2):
                    own_copy(1 - part, part, t).wait_recv()
                    to_sib((y_dev, x_dev)[part], part, t).start()

        @pl.when(u >= LAG + 2)
        def _():
            t = u - LAG - 2
            for part in range(2):
                forward(part, t).wait_recv()
                to_sib(g_dev, part, t).start()

        @pl.when(u == 1)
        def _():
            new = adam_update(vec_sum[...], coef_out[0:1, :], pv[...], mv[...], sv[...], 0.0)
            for i in range(3):
                vec_new[i] = new[i]
            vec_w[me] = new[0]
            for k in range(1, n_dev):
                new_copy(k).start()

        @pl.when(u == w_steps - 1)
        def _():
            for group in range(2):
                for part in range(2):
                    late_copy(group, part).start()

    for k in range(1, n_dev):
        new_copy(k).wait()

    for t in (steps - 2, steps - 1):
        slot = t % 2
        for part in range(2):
            leaf_copy(t, slot, part).wait_send()
            direct_copy(t, slot, part).wait_send()
            four_copy(t, slot, part).wait_send()
    pltpu.make_async_remote_copy(
        src_ref=g.at[:, pl.ds(0, 4 * share - 2 * half)], dst_ref=sib_land.at[:, pl.ds(0, 4 * share - 2 * half)],
        send_sem=sib_send, recv_sem=sib_recv.at[0, 0], device_id=(sib,), device_id_type=MESH).wait_send()
    for part in range(2):
        first_copy(part).wait_send()
    for part in range(2):
        late_copy(0, part).wait()
        late_copy(1, part).wait()
        all_rows(w_steps + early, own_send.at[part], fsib_recv).wait_send()
        all_rows(w_steps, fwd_send.at[part], fsib_recv).wait_send()
    all_rows(2 * w_steps, own_send.at[2], own_sib_recv).wait()
    all_rows(4 * w_steps + 2 * early, fsib_send, fsib_recv).wait()
    pltpu.make_async_copy(own_w, gathered.at[pl.ds(0, share_rows), :], keep_sem).wait()


def step_call(g, gv, p_mat, m_mat, s_mat, pv, mv, sv, share, steps, w_steps, w_late):
    half = share // (2 * steps)
    rows = half // LANES
    share_rows = share // LANES
    w_rows = share_rows // (2 * w_steps)
    dma = pltpu.SemaphoreType.DMA
    f32, bf16 = jnp.float32, jnp.bfloat16
    own_rows = pv.shape[0]
    hbm = pl.BlockSpec(memory_space=pltpu.HBM)
    vmem = pl.BlockSpec(memory_space=pltpu.VMEM)
    return pl.pallas_call(
        functools.partial(step_kernel, share, half, steps, w_steps, w_late),
        out_shape=(jax.ShapeDtypeStruct((share_rows, LANES), f32),
                   jax.ShapeDtypeStruct((8 * share_rows, LANES), bf16),
                   jax.ShapeDtypeStruct((w_late[0] * w_rows, LANES), bf16),
                   jax.ShapeDtypeStruct((w_late[0] * w_rows, LANES), bf16),
                   jax.ShapeDtypeStruct((w_late[1] * w_rows, LANES), bf16),
                   jax.ShapeDtypeStruct((w_late[1] * w_rows, LANES), bf16),
                   jax.ShapeDtypeStruct((1, 4 * share), bf16),
                   jax.ShapeDtypeStruct((share_rows, LANES), f32),
                   jax.ShapeDtypeStruct((share_rows, LANES), f32),
                   jax.ShapeDtypeStruct((share_rows, LANES), f32),
                   jax.ShapeDtypeStruct((8, LANES), f32),
                   jax.ShapeDtypeStruct((3, own_rows, LANES), f32),
                   jax.ShapeDtypeStruct((8, own_rows, LANES), f32)),
        in_specs=[hbm, vmem, hbm, hbm, hbm, vmem, vmem, vmem],
        out_specs=(hbm,) * 10 + (vmem,) * 3,
        scratch_shapes=[
            pltpu.VMEM((2, 1, 8 * half), bf16),
            pltpu.VMEM((2, 1, 8 * half), bf16),
            pltpu.VMEM((2, 2 * rows, LANES), f32),
            pltpu.VMEM((2, 2 * rows, LANES), f32),
            pltpu.VMEM((2, 2 * rows, LANES), f32),
            pltpu.VMEM((2 * rows, LANES), f32),
            pltpu.VMEM((2, 2 * rows, LANES), f32),
            pltpu.VMEM((2, 2 * rows, LANES), f32),
            pltpu.VMEM((8, LANES), f32),
            pltpu.VMEM((8, 8, LANES), f32),
            pltpu.VMEM((8, 1, own_rows * LANES), bf16),
            dma(()), dma((4, steps)),
            dma((2, 2)), dma((2, steps)), dma((2, 2)), dma((2, steps)), dma((2, 2)), dma((2, steps)),
            dma((2, 6)), dma((2, 6)), dma(()), dma((2,)), dma((2,)),
            dma((7,)), dma((7,)), dma((7, 2)), dma((7, 2)), dma(()),
            pltpu.VMEM((2, 4, 2, w_rows, LANES), f32),
            pltpu.VMEM((share_rows, LANES), bf16),
            dma((2, 4, 2)), dma((3,)), dma((2, 2, w_steps)), dma(()), dma(()), dma((2, 2)),
            dma((2,)), dma((2, w_steps)), dma(()), dma(()), dma((2,)), dma((2,)),
            pltpu.VMEM((own_rows, LANES), f32),
        ],
        compiler_params=pltpu.CompilerParams(collective_id=0, has_side_effects=True, vmem_limit_bytes=60 * 2**20),
        name='reduce_update_gather',
    )(g, gv, p_mat, m_mat, s_mat, pv, mv, sv)


def update_kernel(coef, grad, master, moment, second, vec_new, vec_w, new_p, new_m, new_s, vec_p, vec_m, vec_s, w_vec,
                  rows):
    new_p[...], new_m[...], new_s[...] = adam_update(grad[...], coef[0:1, :], master[...], moment[...], second[...], DECAY)

    @pl.when(pl.program_id(0) == 0)
    def _():
        vec_p[...], vec_m[...], vec_s[...] = vec_new[0], vec_new[1], vec_new[2]
        n = vec_w.shape[1]
        for d in range(vec_w.shape[0]):
            rows[pl.ds(d * n, n), :] = vec_w[d]
        w_vec[...] = rows[...].astype(jnp.bfloat16)


def update_call(coef, grad, master, moment, second, vec_new, vec_w, block):
    n = grad.shape[0]
    own_rows = vec_new.shape[1]
    f32 = jnp.float32
    tile = pl.BlockSpec((block, LANES), lambda i: (i, 0))

    def whole(shape):
        return pl.BlockSpec(shape, lambda i: (0,) * len(shape))

    small = jax.ShapeDtypeStruct((own_rows, LANES), f32)
    return pl.pallas_call(
        update_kernel,
        grid=(n // block,),
        out_shape=(jax.ShapeDtypeStruct(grad.shape, f32),) * 3 + (small,) * 3 + (
            jax.ShapeDtypeStruct((8 * own_rows, LANES), jnp.bfloat16),),
        in_specs=[whole((8, LANES))] + [tile] * 4 + [whole(vec_new.shape), whole(vec_w.shape)],
        out_specs=(tile,) * 3 + (whole((own_rows, LANES)),) * 3 + (whole((8 * own_rows, LANES)),),
        scratch_shapes=[pltpu.VMEM((8 * own_rows, LANES), f32)],
        compiler_params=pltpu.CompilerParams(vmem_limit_bytes=40 * 2**20),
        cost_estimate=pl.CostEstimate(flops=n * LANES * 200, bytes_accessed=n * LANES * 28, transcendentals=0),
        name='update',
    )(coef, grad, master, moment, second, vec_new, vec_w)


def copy_kernel(moves, blocks, *refs):
    n_src = 1 + max(move[0] for move in moves(0))
    srcs, out, buf, in_sem, out_sem = refs[:n_src], refs[-4], refs[-3], refs[-2], refs[-1]
    me = lax.axis_index('fsdp')
    todo = []
    for which, src_row, dst_row, n in moves(me):
        if n == 0:
            continue
        size = n // blocks(n)
        for i in range(blocks(n)):
            todo.append((srcs[which], src_row + i * size, dst_row + i * size, size))
    slots = buf.shape[0]

    def take(k):
        src, src_row, _, size = todo[k]
        return pltpu.make_async_copy(src.at[pl.ds(pl.multiple_of(src_row, 16), size), :],
                                     buf.at[k % slots, pl.ds(0, size), :], in_sem.at[k % slots])

    def give(k):
        _, _, dst_row, size = todo[k]
        return pltpu.make_async_copy(buf.at[k % slots, pl.ds(0, size), :],
                                     out.at[pl.ds(pl.multiple_of(dst_row, 16), size), :], out_sem.at[k % slots])

    ahead = slots // 2
    for k in range(min(ahead, len(todo))):
        take(k).start()
    for k in range(len(todo)):
        take(k).wait()
        give(k).start()
        if k + ahead < len(todo):
            if k + ahead >= slots:
                give(k + ahead - slots).wait()
            take(k + ahead).start()
    for k in range(max(0, len(todo) - slots), len(todo)):
        give(k).wait()


def copy_call(moves, srcs, out_rows, into=None, slots=6, most=14560):
    def blocks(n):
        return next(d for d in range(1, n // 16 + 1) if (n // 16) % d == 0 and n // d <= most)

    hbm = pl.BlockSpec(memory_space=pltpu.HBM)
    args = list(srcs) + ([into] if into is not None else [])
    size = sum(move[3] for move in moves(0)) * LANES * 2
    return pl.pallas_call(
        functools.partial(copy_kernel, moves, blocks),
        out_shape=jax.ShapeDtypeStruct((out_rows, LANES), jnp.bfloat16),
        in_specs=[hbm] * len(args),
        out_specs=hbm,
        scratch_shapes=[pltpu.VMEM((slots, most, LANES), jnp.bfloat16),
                        pltpu.SemaphoreType.DMA((slots,)), pltpu.SemaphoreType.DMA((slots,))],
        input_output_aliases={len(srcs): 0} if into is not None else {},
        compiler_params=pltpu.CompilerParams(vmem_limit_bytes=32 * 2**20),
        cost_estimate=pl.CostEstimate(flops=size * 6, bytes_accessed=2 * size, transcendentals=0),
    )(*args)


def place_kernel(moves, *refs):
    out, sems = refs[-2], refs[-1]
    copies = [pltpu.make_async_copy(refs[which], out.at[pl.ds(pl.multiple_of(dst_row, 16), n), :], sems.at[i])
              for i, (which, _, dst_row, n) in enumerate(moves(lax.axis_index('fsdp')))]
    for copy in copies:
        copy.start()
    for copy in copies:
        copy.wait()


def place_call(moves, srcs, into):
    hbm, vmem = pl.BlockSpec(memory_space=pltpu.HBM), pl.BlockSpec(memory_space=pltpu.VMEM)
    size = sum(move[3] for move in moves(0)) * LANES * 2
    return pl.pallas_call(
        functools.partial(place_kernel, moves),
        out_shape=jax.ShapeDtypeStruct(into.shape, into.dtype),
        in_specs=[vmem] * len(srcs) + [hbm],
        out_specs=hbm,
        scratch_shapes=[pltpu.SemaphoreType.DMA((len(srcs),))],
        input_output_aliases={len(srcs): 0},
        compiler_params=pltpu.CompilerParams(vmem_limit_bytes=16 * 2**20),
        cost_estimate=pl.CostEstimate(flops=size * 6, bytes_accessed=2 * size, transcendentals=0),
    )(*srcs, into)


def block_rows_of(n):
    return 8 * max(d for d in range(1, 460) if (n // 8) % d == 0)


STEPS = 20
W_STEPS = 26
W_LATE = (19, 6)
LAG = 3


def neighbours(me):
    core, x_pos, y_pos = lax.rem(me, 2), lax.rem(me // 2, 2), me // 4
    return me + 1 - 2 * core, me + 2 - 4 * x_pos, me + 4 - 8 * y_pos


def solution(mesh):
    hop_x = [(d, d ^ 2) for d in range(8)]
    hop_y = [(d, d ^ 4) for d in range(8)]
    hop_core = [(d, d ^ 1) for d in range(8)]

    def local_step(grad_mat, grad_vec, master_mat, moment_mat, second_mat, master_vec, moment_vec, second_vec):
        share = master_mat.shape[0]
        share_rows = share // LANES
        half_rows = share_rows // 2
        late, last = (n * (half_rows // W_STEPS) for n in W_LATE)
        early = half_rows - late - last
        own_rows = master_vec.shape[0] // LANES
        mats = [v.reshape(share_rows, LANES) for v in (master_mat, moment_mat, second_mat)]
        vecs = [v.reshape(own_rows, LANES) for v in (master_vec, moment_vec, second_vec)]
        total, gathered, late_a, late_b, last_a, last_b, _, _, _, _, coef, vec_new, vec_w = step_call(
            grad_mat, grad_vec, *mats, *vecs, share, STEPS, W_STEPS, W_LATE)

        late_x = lax.ppermute(late_b, 'fsdp', hop_x)
        late_y = lax.ppermute(late_a, 'fsdp', hop_y)
        last_x = lax.ppermute(last_b, 'fsdp', hop_x)
        last_y = lax.ppermute(last_a, 'fsdp', hop_y)

        def whole_moves(me):
            sib, x_dev, y_dev = neighbours(me)
            g_dev = x_dev + y_dev - me
            flip = sib - me
            return [(0, dev * share_rows, dev * share_rows, share_rows) for dev in (me, sib, g_dev, g_dev + flip)] + [
                (0, x_dev * share_rows, x_dev * share_rows, half_rows)]

        def late_rows(x_dev, y_dev, first):
            return [(first, 0, x_dev * share_rows + half_rows + early, late),
                    (first + 1, 0, y_dev * share_rows + early, late)]

        def last_rows(x_dev, y_dev, first):
            return [(first, 0, x_dev * share_rows + half_rows + early + late, last),
                    (first + 1, 0, y_dev * share_rows + early + late, last)]

        def early_moves(me):
            sib, x_dev, y_dev = neighbours(me)
            flip = sib - me
            moves = [(0, (x_dev + flip) * share_rows, (x_dev + flip) * share_rows, half_rows)]
            for dev in (x_dev, x_dev + flip):
                start = dev * share_rows + half_rows
                moves.append((0, start, start, early))
            for dev in (y_dev, y_dev + flip):
                start = dev * share_rows
                moves.append((0, start, start, early))
                moves.append((0, start + half_rows, start + half_rows, half_rows))
            return moves + late_rows(x_dev, y_dev, 1)

        def mid_moves(me):
            sib, x_dev, y_dev = neighbours(me)
            return late_rows(x_dev + sib - me, y_dev + sib - me, 0)

        def late_moves(me):
            _, x_dev, y_dev = neighbours(me)
            return last_rows(x_dev, y_dev, 0)

        def last_moves(me):
            sib, x_dev, y_dev = neighbours(me)
            flip = sib - me
            return last_rows(x_dev + flip, y_dev + flip, 0)

        *new, weights_vec = update_call(coef, total, *mats, vec_new, vec_w, block_rows_of(share_rows))
        weights = copy_call(whole_moves, (gathered,), 8 * share_rows)
        late_x, late_y, weights, *new = lax.optimization_barrier((late_x, late_y, weights, *new))
        sib_late_x = lax.ppermute(late_x, 'fsdp', hop_core)
        sib_late_y = lax.ppermute(late_y, 'fsdp', hop_core)
        weights = copy_call(early_moves, (gathered, late_x, late_y), 8 * share_rows, into=weights)
        weights = place_call(mid_moves, (sib_late_x, sib_late_y), weights)
        last_x, last_y, weights = lax.optimization_barrier((last_x, last_y, weights))
        sib_last_x = lax.ppermute(last_x, 'fsdp', hop_core)
        sib_last_y = lax.ppermute(last_y, 'fsdp', hop_core)
        weights = place_call(late_moves, (last_x, last_y), weights)
        weights = place_call(last_moves, (sib_last_x, sib_last_y), weights)
        return tuple(v.reshape(-1) for v in (*new, weights, weights_vec))

    row_spec = P('fsdp', None)
    flat_spec = P('fsdp')
    whole_spec = P()
    return jax.shard_map(local_step, mesh=mesh,
                         in_specs=(row_spec, row_spec) + (flat_spec,) * 6,
                         out_specs=(flat_spec,) * 6 + (whole_spec, whole_spec),
                         check_vma=False)
```
